32 devices in a mesh: sub: 2 (over x), row: 16 (over z, y, core).
Axes of the slice: x: 2, y: 2, z: 4, core: 2. Of those that a mesh axis runs over, the one named last changes fastest.
Arguments:
- diag_blocks: float32 [512, 128, 128], P(('sub', 'row')), parts along dimension 0, may hold values from -0.05 to 16, as said below
- coupling: float32 [512, 3, 128, 128], P(('sub', 'row')), parts along dimension 0, may hold values from -0.05 to 0.05
- offsets: int32 [512, 3], P(('sub', 'row')), parts along dimension 0, may hold values from 1 to 4, as said below
- mass: float32 [65536], P(('sub', 'row')), parts along dimension 0, may hold values from 0.5 to 2
- initial_modes: float32 [32, 65536], P(None, ('sub', 'row')), parts along dimension 1, may hold values from -6 to 6
Outputs:
- mass_density: float32 [65536], P(('sub', 'row')), parts along dimension 0
- energy_density: float32 [65536], P(('sub', 'row')), parts along dimension 0
The draws below stay inside these ranges and needn't reach their ends.
There are 2 independent parts, one for each index of `sub`. The reference program is written for one: setup_inputs(seed, part) draws one part's arguments, and reference() takes and returns one part's arrays. A program takes and returns all parts, laid end to end along the dimension named above; each array names one. Nothing has to cross between parts.
Inputs may be any that keep to these rules, and one draw needn't show every extreme that they name: `diag_blocks`: each block is symmetric; entries off a block's diagonal lie in -0.05 to 0.05, its diagonal entries in 1 to 16. The 3 offsets of a block row are distinct.
All inputs are finite; a program needn't handle non-finite values.
Results may differ from the reference program's by a relative error of at most 0.0003.
Values sent between devices are 32-bit elements; how exact they have to be, the bound alone decides.
No kernel may reach another device: no remote copies, remote signals or barrier semaphores. Data moves between devices by JAX's collectives and lax.ppermute only.
A program may use at most 128 MiB of HBM per device.

```python
import math
import jax
import jax.numpy as jnp
from jax import lax

BLK = 128
MODES = 32
SLOTS = 3
REACH = 4
ITERS = 3
PURIFY = 28
NBLK = 256
N = 32768


def draw_diag_blocks(key, part):
    key_off, key_diag = jax.random.split(key)
    shape = (NBLK, BLK, BLK)
    couplings = jax.random.uniform(key_off, shape, jnp.float32, -0.05, 0.05)
    diagonal = jnp.exp(jax.random.uniform(key_diag, (NBLK, BLK), jnp.float32, 0.0, jnp.log(10.0)))
    identity = jnp.eye(BLK, dtype=jnp.float32)
    symmetric = 0.5 * (couplings + jnp.swapaxes(couplings, 1, 2))
    return symmetric * (1.0 - identity)[None, :, :] + identity[None, :, :] * diagonal[:, :, None]


def draw_offsets(key, part):
    scores = jax.random.randint(key, (NBLK, REACH), 0, 1 << 20) * REACH + jnp.arange(REACH, dtype=jnp.int32)[None, :]
    ranking = jnp.argsort(scores, axis=1)
    return (ranking[:, :SLOTS] + 1).astype(jnp.int32)


def steps_of(key, extent, cuts, smallest, largest):
    gain, own = 1.0, jax.random.fold_in(key, 6)
    for axis_at, blocks in cuts:
        steps = jnp.exp(jax.random.uniform(jax.random.fold_in(own, axis_at), (blocks,), jnp.float32, smallest / len(cuts), largest / len(cuts)))
        gain = gain * jnp.repeat(steps, extent[axis_at] // blocks).reshape([-1 if axis == axis_at else 1 for axis in range(len(extent))])
    return gain


def gaussian(own_key, dims, deviation, limit, pieces=(), held_as=jnp.bfloat16):
    entries = jax.random.normal(own_key, dims, jnp.float32) * deviation
    if len(pieces) > 0:
        entries = steps_of(own_key, dims, pieces, -0.22, 0.18) * entries
    return jnp.clip(entries, min=-limit, max=limit).astype(held_as)


def setup_inputs(seed: int = 0, part: int = 0) -> dict:
    arg_keys = jax.random.split(jax.random.key(seed), 6)
    part_splits = jax.random.split(jax.random.fold_in(arg_keys[5], part), 6)
    diag_blocks = draw_diag_blocks(jax.random.fold_in(jax.random.fold_in(arg_keys[5], part), 71), part)
    coupling = jnp.clip(jax.random.uniform(part_splits[1], (NBLK, SLOTS, BLK, BLK), jnp.float32, -0.05, 0.05) * steps_of(part_splits[1], (NBLK, SLOTS, BLK, BLK), ((0, 16),), -0.4, 0.0), -0.05, 0.05)
    offsets = draw_offsets(jax.random.fold_in(jax.random.fold_in(arg_keys[5], part), 71), part)
    mass = jnp.clip(jnp.exp(math.log(2.0) - 1.3862944 * jax.random.uniform(part_splits[3], (N,), jnp.float32) ** steps_of(part_splits[3], (N,), ((0, 16),), -0.2, 0.2)), 0.5, 2.0)
    initial_modes = gaussian(part_splits[4], (MODES, N), 1.0, 6.0, ((1, 16),), jnp.float32)
    return {"diag_blocks": diag_blocks, "coupling": coupling, "offsets": offsets, "mass": mass, "initial_modes": initial_modes}


PRECISE = lax.Precision.HIGHEST

def stiffness_apply(vectors, diag_blocks, coupling, offsets):
    rowcount = vectors.shape[0]
    block_count = diag_blocks.shape[0]
    block_width = diag_blocks.shape[1]
    blocked = vectors.reshape(rowcount, block_count, block_width)
    result = jnp.einsum('nbk,bkj->nbj', blocked, diag_blocks, precision=PRECISE)
    targets = jnp.arange(block_count, dtype=jnp.int32)[:, None] - offsets
    present = (targets >= 0).astype(vectors.dtype)
    clipped = jnp.maximum(targets, 0).astype(jnp.int32)
    gathered = blocked[:, clipped, :] * present[None, :, :, None]
    result = result + jnp.einsum('nbsk,bsjk->nbj', gathered, coupling, precision=PRECISE)
    products = jnp.einsum('nbk,bskj->nbsj', blocked, coupling, precision=PRECISE) * present[None, :, :, None]
    result = result.at[:, clipped, :].add(products)
    return result.reshape(rowcount, block_count * block_width)

def purify(matrix, occupied, steps_count):
    order = matrix.shape[0]
    identity = jnp.eye(order, dtype=matrix.dtype)
    diagonal = jnp.diagonal(matrix)
    center = jnp.sum(diagonal) / order
    radius = lax.optimization_barrier(jnp.sum(jnp.abs(matrix), axis=1)) - jnp.abs(diagonal)
    highest = jnp.max(diagonal + radius)
    lowest = jnp.min(diagonal - radius)
    factor = jnp.minimum(occupied / jnp.maximum(highest - center, 1e-06), (order - occupied) / jnp.maximum(center - lowest, 1e-06))
    initial = factor / order * (center * identity - matrix) + occupied / order * identity

    def purify_step(index, density):
        square = jnp.dot(density, density, precision=PRECISE)
        cube = jnp.dot(square, density, precision=PRECISE)
        numerator = jnp.trace(square - cube)
        denominator = jnp.trace(density - square)
        safe_denominator = jnp.where(jnp.abs(denominator) > 1e-12, denominator, 1.0)
        ratio = jnp.clip(numerator / safe_denominator, 0.0, 1.0)
        upward = ((1.0 + ratio) * square - cube) / jnp.maximum(ratio, 0.5)
        downward = ((1.0 - 2.0 * ratio) * density + (1.0 + ratio) * square - cube) / jnp.maximum(1.0 - ratio, 0.5)
        return jnp.where(ratio >= 0.5, upward, downward)
    return lax.fori_loop(0, steps_count, purify_step, initial)

def ritz_basis(gram_stiff, gram_mass, modes_wanted, steps_count):
    order = gram_stiff.shape[0]
    gram_stiff = 0.5 * (gram_stiff + gram_stiff.T)
    gram_mass = 0.5 * (gram_mass + gram_mass.T)
    scaling = lax.rsqrt(jnp.diagonal(gram_mass) + 1e-06)
    stiff_scaled = scaling[:, None] * gram_stiff * scaling[None, :]
    mass_scaled = scaling[:, None] * gram_mass * scaling[None, :]
    factor_low = jnp.linalg.cholesky(mass_scaled)
    identity = jnp.eye(order, dtype=gram_stiff.dtype)
    inverse_low = lax.linalg.triangular_solve(factor_low, identity, left_side=True, lower=True)
    reduced = jnp.dot(jnp.dot(inverse_low, stiff_scaled, precision=PRECISE), inverse_low.T, precision=PRECISE)
    reduced = 0.5 * (reduced + reduced.T)
    if order > modes_wanted:
        projector = purify(reduced, modes_wanted, steps_count)
        columns = projector[:, :modes_wanted]
    else:
        columns = identity
    correlation = jnp.dot(columns.T, columns, precision=PRECISE)
    correlation_low = jnp.linalg.cholesky(correlation)
    orthonormal = lax.linalg.triangular_solve(correlation_low, columns.T, left_side=True, lower=True).T
    coefficients = scaling[:, None] * jnp.dot(inverse_low.T, orthonormal, precision=PRECISE)
    projected = jnp.dot(jnp.dot(orthonormal.T, reduced, precision=PRECISE), orthonormal, precision=PRECISE)
    return (coefficients, 0.5 * (projected + projected.T))

def reference(diag_blocks, coupling, offsets, mass, initial_modes):
    stiff_diag = jnp.diagonal(diag_blocks, axis1=1, axis2=2).reshape(-1)

    def gram_pair(basis, stiff_basis):
        gram_stiff = jnp.dot(basis, stiff_basis.T, precision=PRECISE)
        gram_mass = jnp.dot(basis * mass[None, :], basis.T, precision=PRECISE)
        return (gram_stiff, gram_mass)
    stiff_initial = stiffness_apply(initial_modes, diag_blocks, coupling, offsets)
    gram_stiff, gram_mass = gram_pair(initial_modes, stiff_initial)
    coefficients, projected = ritz_basis(gram_stiff, gram_mass, MODES, PURIFY)
    modes_now = jnp.dot(coefficients.T, initial_modes, precision=PRECISE)
    stiff_modes = jnp.dot(coefficients.T, stiff_initial, precision=PRECISE)
    directions = None
    stiff_directions = None
    for iteration in range(ITERS):
        residual = stiff_modes - jnp.dot(projected, modes_now * mass[None, :], precision=PRECISE)
        precond = residual / stiff_diag[None, :]
        stiff_precond = stiffness_apply(precond, diag_blocks, coupling, offsets)
        if directions is None:
            basis = jnp.concatenate([modes_now, precond], axis=0)
            stiff_basis = jnp.concatenate([stiff_modes, stiff_precond], axis=0)
        else:
            basis = jnp.concatenate([modes_now, precond, directions], axis=0)
            stiff_basis = jnp.concatenate([stiff_modes, stiff_precond, stiff_directions], axis=0)
        gram_stiff, gram_mass = gram_pair(basis, stiff_basis)
        coefficients, projected = ritz_basis(gram_stiff, gram_mass, MODES, PURIFY)
        directions = jnp.dot(coefficients[MODES:].T, basis[MODES:], precision=PRECISE)
        stiff_directions = jnp.dot(coefficients[MODES:].T, stiff_basis[MODES:], precision=PRECISE)
        modes_now = jnp.dot(coefficients.T, basis, precision=PRECISE)
        stiff_modes = jnp.dot(coefficients.T, stiff_basis, precision=PRECISE)
    weight = modes_now.shape[1] / MODES
    mass_density = weight * mass * lax.optimization_barrier(jnp.sum(modes_now * modes_now, axis=0))
    energy_density = weight * lax.optimization_barrier(jnp.sum(modes_now * stiff_modes, axis=0))
    return (mass_density, energy_density)
```

```python
import functools

import jax
import jax.numpy as jnp
from jax import lax
from jax.experimental import pallas as pl
from jax.experimental.pallas import tpu as pltpu
from jax.sharding import PartitionSpec as P

MODES = 32
REACH = 4
ITERS = 3
PURIFY = 28


PRECISE = lax.Precision.HIGHEST


def from_behind(value, axis, steps):
    count = lax.axis_size(axis)
    initial, last = (max(0, -steps), min(count, count - steps))
    return lax.ppermute(value, axis, [(source, source + steps) for source in range(initial, last)])


def one_hot_table(positions, extent):
    return (positions[..., None] == jnp.arange(extent, dtype=jnp.int32)).astype(jnp.float32)


def stiffness_apply(vectors, diag_blocks, coupling, offsets):
    rowcount = vectors.shape[0]
    block_count = diag_blocks.shape[0]
    block_width = diag_blocks.shape[1]
    blocked = vectors.reshape(rowcount, block_count, block_width)
    result = jnp.einsum("nbk,bkj->nbj", blocked, diag_blocks, precision=PRECISE)
    positions = jnp.arange(block_count, dtype=jnp.int32)[:, None] - offsets + REACH
    products = jnp.einsum("nbk,bskj->nbsj", blocked, coupling, precision=PRECISE)
    lower_part = from_behind(vectors[:, (block_count - REACH) * block_width :], "row", 1)
    extent = block_count + REACH
    extended = jnp.concatenate([lower_part, vectors], axis=1).reshape(rowcount, extent, block_width)
    selector = one_hot_table(positions, extent)
    gathered = jnp.einsum("bse,nek->nbsk", selector, extended, precision=PRECISE)
    result = result + jnp.einsum("nbsk,bsjk->nbj", gathered, coupling, precision=PRECISE)
    spread = jnp.einsum("bse,nbsj->nej", selector, products, precision=PRECISE)
    returned = from_behind(spread[:, :REACH].reshape(rowcount, REACH * block_width), "row", -1)
    result = result + spread[:, REACH:]
    result = result.at[:, block_count - REACH :].add(returned.reshape(rowcount, REACH, block_width))
    return result.reshape(rowcount, block_count * block_width)


LANES = 128
F32 = jnp.float32
BF16 = jnp.bfloat16


def pieces(x, count):
    out = []
    for index in range(count):
        part = x.astype(BF16)
        out.append(part)
        if index + 1 < count:
            x = x - part.astype(F32)
    return out


def dot_nn(a, b):
    return lax.dot_general(a, b, (((1,), (0,)), ((), ())), preferred_element_type=F32)


def dot_nt(a, b):
    return lax.dot_general(a, b, (((1,), (1,)), ((), ())), preferred_element_type=F32)


def pad_rows(x):
    short = LANES - x.shape[0]
    return x if short == 0 else jnp.concatenate([x, jnp.zeros((short, x.shape[1]), x.dtype)], axis=0)


def mul_nn(a, b, count):
    rows = a.shape[0]
    left = pieces(a, count)
    right = [pad_rows(part) for part in pieces(b, count)]
    out = dot_nn(jnp.concatenate(left, axis=0), jnp.concatenate(right[:2], axis=1))
    total = out[:rows, :LANES] + (out[:rows, LANES:] + out[rows : 2 * rows, :LANES])
    if count == 3:
        total = total + (out[rows : 2 * rows, LANES:] + (out[2 * rows :, :LANES] + dot_nn(left[0], right[2])))
    return total


def mul_nt(a, b, count):
    left = pieces(a, count)
    right = [pad_rows(part) for part in pieces(b, count)]
    total = None
    for i in range(count):
        for j in range(count - i):
            term = dot_nt(left[i], right[j])
            total = term if total is None else total + term
    return total


def lane_of(shape):
    return lax.broadcasted_iota(jnp.int32, shape, 1)


def row_of(shape):
    return lax.broadcasted_iota(jnp.int32, shape, 0)


def eliminate(matrix, other):
    order = matrix.shape[0]
    tiles = order // 8
    a = [matrix[8 * i : 8 * i + 8] for i in range(tiles)]
    e = [other[8 * i : 8 * i + 8] for i in range(tiles)]
    sub = row_of((8, LANES))
    scales = []
    for k in range(order):
        kt, ks = k // 8, k % 8
        row_a = jnp.broadcast_to(a[kt][ks : ks + 1, :], (8, LANES))
        row_e = jnp.broadcast_to(e[kt][ks : ks + 1, :], (8, LANES))
        column = [jnp.broadcast_to(a[i][:, k : k + 1], (8, LANES)) for i in range(kt, tiles)]
        pivot = jnp.broadcast_to(column[0][ks : ks + 1, :], (8, LANES))
        inverse = 1.0 / pivot
        for i in range(kt, tiles):
            ratio = column[i - kt] * inverse
            if i == kt:
                ratio = jnp.where(sub > ks, ratio, 0.0)
            a[i] = a[i] - ratio * row_a
            e[i] = e[i] - ratio * row_e
        e[kt] = jnp.where(sub == ks, e[kt] * lax.rsqrt(pivot), e[kt])
    return jnp.concatenate(e, axis=0)


def total_of(x):
    return jnp.sum(jnp.sum(x, axis=0, keepdims=True), axis=1, keepdims=True)


def purify(c, wanted, steps, eye, valid):
    order = c.shape[0]
    diagonal = jnp.sum(jnp.where(eye, c, 0.0), axis=0, keepdims=True)
    center = jnp.sum(diagonal, axis=1, keepdims=True) / order
    radius = jnp.sum(jnp.where(eye, 0.0, jnp.abs(c)), axis=0, keepdims=True)
    highest = jnp.max(jnp.where(valid, diagonal + radius, -jnp.inf), axis=1, keepdims=True)
    lowest = jnp.min(jnp.where(valid, diagonal - radius, jnp.inf), axis=1, keepdims=True)
    factor = jnp.minimum(
        wanted / jnp.maximum(highest - center, 1e-06),
        (order - wanted) / jnp.maximum(center - lowest, 1e-06),
    )
    ones = jnp.where(eye, 1.0, 0.0)
    density = factor / order * (center * ones - c) + wanted / order * ones

    def step(index, density):
        square = mul_nn(density, density, 2)
        cube = mul_nn(square, density, 2)
        below = total_of(jnp.where(eye, density, 0.0) - density * density)
        above = total_of(density * (density - square))
        safe = jnp.where(jnp.abs(below) > 1e-12, below, 1.0)
        ratio = jnp.clip(above / safe, 0.0, 1.0)
        high = ratio >= 0.5
        scale = 1.0 / jnp.where(high, jnp.maximum(ratio, 0.5), jnp.maximum(1.0 - ratio, 0.5))
        first = jnp.where(high, 0.0, 1.0 - 2.0 * ratio) * scale
        second = (1.0 + ratio) * scale
        return first * density + second * square - scale * cube

    return lax.fori_loop(0, steps, step, density)


def ritz_math(gram_stiff, gram_mass, wanted, steps):
    order = gram_stiff.shape[0]
    shape = (order, LANES)
    eye = lane_of(shape) == row_of(shape)
    valid = lane_of((1, LANES)) < order
    gram_stiff = 0.5 * (gram_stiff + pad_rows(gram_stiff).T[:order])
    gram_mass = 0.5 * (gram_mass + pad_rows(gram_mass).T[:order])
    picked = jnp.where(eye, gram_mass, 0.0)
    scale_col = lax.rsqrt(jnp.sum(picked, axis=1, keepdims=True) + 1e-06)
    scale_row = lax.rsqrt(jnp.sum(picked, axis=0, keepdims=True) + 1e-06)
    stiff = scale_col * gram_stiff * scale_row
    mass = scale_col * gram_mass * scale_row
    inverse_low = eliminate(mass, jnp.where(eye, 1.0, 0.0))
    reduced = mul_nt(mul_nn(inverse_low, stiff, 3), inverse_low, 3)
    reduced = 0.5 * (reduced + pad_rows(reduced).T[:order])
    if order > wanted:
        columns = purify(reduced, wanted, steps, eye, valid)[:wanted]
        correlation = mul_nt(columns, columns, 3)
        columns = eliminate(correlation, columns)
        coefficients = mul_nn(columns, inverse_low, 3) * scale_row
        projected = mul_nt(mul_nn(columns, reduced, 3), columns, 3)
        projected = 0.5 * (projected + pad_rows(projected).T[:wanted])
    else:
        coefficients = inverse_low * scale_row
        projected = reduced
    return coefficients, projected


def ritz_kernel(wanted, steps, a_ref, b_ref, g_ref, h_ref):
    g, h = ritz_math(a_ref[...], b_ref[...], wanted, steps)
    g_ref[...] = g
    h_ref[...] = h


def ritz(a, b, wanted, steps):
    return pl.pallas_call(
        functools.partial(ritz_kernel, wanted, steps),
        out_shape=[jax.ShapeDtypeStruct((wanted, LANES), F32)] * 2,
        in_specs=[pl.BlockSpec(memory_space=pltpu.VMEM)] * 2,
        out_specs=[pl.BlockSpec(memory_space=pltpu.VMEM)] * 2,
        compiler_params=pltpu.CompilerParams(vmem_limit_bytes=16 << 20),
    )(a, b)


def exchange_sum(value, axis):
    count = lax.axis_size(axis)
    if count & (count - 1):
        return lax.psum(value, axis)
    stride = 1
    while stride < count:
        masks = [stride, 2 * stride, 3 * stride] if 4 * stride <= count else [stride]
        parts = [
            lax.ppermute(value, axis, [(source, source ^ mask) for source in range(count)])
            for mask in masks
        ]
        value = value + parts[0] if len(parts) == 1 else (value + parts[0]) + (parts[1] + parts[2])
        stride *= 1 << len(masks).bit_length()
    return value


def local(diag_blocks, coupling, offsets, mass, initial_modes):
    stiff_diag = jnp.diagonal(diag_blocks, axis1=1, axis2=2).reshape(-1)

    def gram_pair(basis, stiff_basis):
        local_stiff = jnp.dot(basis, stiff_basis.T, precision=PRECISE)
        local_mass = jnp.dot(basis * mass[None, :], basis.T, precision=PRECISE)
        both = exchange_sum(jnp.stack([local_stiff, local_mass]), "row")
        spare = LANES - basis.shape[0]
        both = jnp.pad(both, ((0, 0), (0, 0), (0, spare)))
        return both[0], both[1]

    stiff_initial = stiffness_apply(initial_modes, diag_blocks, coupling, offsets)
    gram_stiff, gram_mass = gram_pair(initial_modes, stiff_initial)
    coefficients, projected = ritz(gram_stiff, gram_mass, MODES, PURIFY)
    coefficients, projected = coefficients[:, :MODES], projected[:, :MODES]
    modes_now = jnp.dot(coefficients, initial_modes, precision=PRECISE)
    stiff_modes = jnp.dot(coefficients, stiff_initial, precision=PRECISE)
    directions = None
    stiff_directions = None
    for iteration in range(ITERS):
        residual = stiff_modes - jnp.dot(projected, modes_now * mass[None, :], precision=PRECISE)
        precond = residual / stiff_diag[None, :]
        stiff_precond = stiffness_apply(precond, diag_blocks, coupling, offsets)
        if directions is None:
            basis = jnp.concatenate([modes_now, precond], axis=0)
            stiff_basis = jnp.concatenate([stiff_modes, stiff_precond], axis=0)
        else:
            basis = jnp.concatenate([modes_now, precond, directions], axis=0)
            stiff_basis = jnp.concatenate([stiff_modes, stiff_precond, stiff_directions], axis=0)
        gram_stiff, gram_mass = gram_pair(basis, stiff_basis)
        coefficients, projected = ritz(gram_stiff, gram_mass, MODES, PURIFY)
        order = basis.shape[0]
        coefficients, projected = coefficients[:, :order], projected[:, :MODES]
        directions = jnp.dot(coefficients[:, MODES:], basis[MODES:], precision=PRECISE)
        stiff_directions = jnp.dot(coefficients[:, MODES:], stiff_basis[MODES:], precision=PRECISE)
        modes_now = jnp.dot(coefficients, basis, precision=PRECISE)
        stiff_modes = jnp.dot(coefficients, stiff_basis, precision=PRECISE)
    weight = mass.shape[0] * lax.axis_size("row") / MODES
    mass_density = weight * mass * jnp.sum(modes_now * modes_now, axis=0)
    energy_density = weight * jnp.sum(modes_now * stiff_modes, axis=0)
    return (mass_density, energy_density)


def solution(mesh):
    placed = (
        P(("sub", "row"), None, None),
        P(("sub", "row"), None, None, None),
        P(("sub", "row"), None),
        P(("sub", "row")),
        P(None, ("sub", "row")),
    )
    return jax.shard_map(
        local,
        mesh=mesh,
        in_specs=placed,
        out_specs=(P(("sub", "row")), P(("sub", "row"))),
        check_vma=False,
    )
```

```python
import functools

import jax
import jax.numpy as jnp
from jax import lax
from jax.experimental import pallas as pl
from jax.experimental.pallas import tpu as pltpu
from jax.sharding import PartitionSpec as P

MODES = 32
REACH = 4
ITERS = 3
PURIFY = 28
LANES = 128
F32 = jnp.float32
BF16 = jnp.bfloat16


def pieces(value, count):
    parts = []
    for index in range(count):
        part = value.astype(BF16)
        parts.append(part)
        if index + 1 < count:
            value = value - part.astype(F32)
    return parts


def dot_nn(left, right):
    return lax.dot_general(left, right, (((1,), (0,)), ((), ())), preferred_element_type=F32)


def dot_nt(left, right):
    return lax.dot_general(left, right, (((1,), (1,)), ((), ())), preferred_element_type=F32)


def pad_rows(value):
    short = LANES - value.shape[0]
    if short == 0:
        return value
    return jnp.concatenate([value, jnp.zeros((short, value.shape[1]), value.dtype)], axis=0)


def transposed(value):
    return pad_rows(value).T[: value.shape[0]]


def fold(out):
    rows, width = out.shape[0] // 2, out.shape[1] // 2
    return out[:rows, :width] + (out[:rows, width:] + out[rows:, :width])


def mul_nn(left, right, count):
    rows = left.shape[0]
    left = pieces(left, count)
    right = [pad_rows(part) for part in pieces(right, count)]
    out = dot_nn(jnp.concatenate(left, axis=0), jnp.concatenate(right[:2], axis=1))
    total = fold(out[: 2 * rows])
    if count == 3:
        total = total + (
            out[rows : 2 * rows, LANES:] + (out[2 * rows :, :LANES] + dot_nn(left[0], right[2]))
        )
    return total


def mul_nt(left, right, count):
    left = pieces(left, count)
    right = [pad_rows(part) for part in pieces(right, count)]
    total = None
    for i in range(count):
        for j in range(count - i):
            term = dot_nt(left[i], right[j])
            total = term if total is None else total + term
    return total


def lane_of(shape):
    return lax.broadcasted_iota(jnp.int32, shape, 1)


def row_of(shape):
    return lax.broadcasted_iota(jnp.int32, shape, 0)


def eye_of(rows, lead=0):
    shape = (rows, LANES)
    return lane_of(shape) == row_of(shape) + lead


def eliminate(matrix, other, lead):
    order = matrix.shape[0]
    tiles = order // 8
    a = [matrix[8 * i : 8 * i + 8] for i in range(tiles)]
    e = [other[8 * i : 8 * i + 8] for i in range(tiles)]
    sub = row_of((8, LANES))
    for k in range(order):
        kt, ks = k // 8, k % 8
        row_a = jnp.broadcast_to(a[kt][ks : ks + 1, :], (8, LANES))
        row_e = jnp.broadcast_to(e[kt][ks : ks + 1, :], (8, LANES))
        at = lead + k
        column = [jnp.broadcast_to(a[i][:, at : at + 1], (8, LANES)) for i in range(kt, tiles)]
        pivot = jnp.broadcast_to(column[0][ks : ks + 1, :], (8, LANES))
        inverse = 1.0 / pivot
        for i in range(kt, tiles):
            ratio = column[i - kt] * inverse
            if i == kt:
                ratio = jnp.where(sub > ks, ratio, 0.0)
            a[i] = a[i] - ratio * row_a
            e[i] = e[i] - ratio * row_e
        e[kt] = jnp.where(sub == ks, e[kt] * lax.rsqrt(pivot), e[kt])
    return jnp.concatenate(e, axis=0)


def total_of(value):
    return jnp.sum(jnp.sum(value, axis=0, keepdims=True), axis=1, keepdims=True)


def purify(matrix, wanted, steps):
    order = matrix.shape[0]
    eye = eye_of(order)
    valid = lane_of((1, LANES)) < order
    diagonal = jnp.sum(jnp.where(eye, matrix, 0.0), axis=0, keepdims=True)
    center = jnp.sum(diagonal, axis=1, keepdims=True) / order
    radius = jnp.sum(jnp.where(eye, 0.0, jnp.abs(matrix)), axis=0, keepdims=True)
    highest = jnp.max(jnp.where(valid, diagonal + radius, -jnp.inf), axis=1, keepdims=True)
    lowest = jnp.min(jnp.where(valid, diagonal - radius, jnp.inf), axis=1, keepdims=True)
    factor = jnp.minimum(
        wanted / jnp.maximum(highest - center, 1e-06),
        (order - wanted) / jnp.maximum(center - lowest, 1e-06),
    )
    ones = jnp.where(eye, 1.0, 0.0)
    initial = factor / order * (center * ones - matrix) + wanted / order * ones

    def purify_step(index, density):
        square = mul_nn(density, density, 2)
        cube = mul_nn(square, density, 2)
        below = total_of(jnp.where(eye, density, 0.0) - density * density)
        above = total_of(density * (density - square))
        safe = jnp.where(jnp.abs(below) > 1e-12, below, 1.0)
        ratio = jnp.clip(above / safe, 0.0, 1.0)
        high = ratio >= 0.5
        scale = 1.0 / jnp.where(high, jnp.maximum(ratio, 0.5), jnp.maximum(1.0 - ratio, 0.5))
        first = jnp.where(high, 0.0, 1.0 - 2.0 * ratio) * scale
        second = (1.0 + ratio) * scale
        return first * density + second * square - scale * cube

    return lax.fori_loop(0, steps, purify_step, initial)


def ritz(half_stiff, half_mass, wanted, steps, last):
    order = half_stiff.shape[0]
    eye = eye_of(order)
    gram_stiff = half_stiff + transposed(half_stiff)
    gram_mass = half_mass + transposed(half_mass)
    picked = jnp.where(eye, gram_mass, 0.0)
    scale_col = lax.rsqrt(jnp.sum(picked, axis=1, keepdims=True) + 1e-06)
    scale_row = lax.rsqrt(jnp.sum(picked, axis=0, keepdims=True) + 1e-06)
    stiff = scale_col * gram_stiff * scale_row
    mass = scale_col * gram_mass * scale_row
    ones = jnp.where(eye, 1.0, 0.0)
    if order == wanted:
        inverse_low = eliminate(mass, ones, 0)
    else:
        known = lane_of((1, LANES)) < wanted
        pivots = jnp.where(known, jnp.sum(jnp.where(eye, mass, 0.0), axis=0, keepdims=True), 1.0)
        ratio = jnp.where(known, mass[wanted:], 0.0) / pivots
        rest = jnp.where(known, 0.0, mass[wanted:] - mul_nn(ratio, mass[:wanted], 3))
        inverse_low = jnp.concatenate(
            [ones[:wanted] * lax.rsqrt(pivots), eliminate(rest, ones[wanted:] - ratio, wanted)], axis=0
        )
    reduced = mul_nt(mul_nn(inverse_low, stiff, 3), inverse_low, 3)
    reduced = 0.5 * (reduced + transposed(reduced))
    if order == wanted:
        return inverse_low * scale_row, reduced, gram_stiff, gram_mass
    columns = purify(reduced, wanted, steps)[:wanted]
    columns = eliminate(mul_nt(columns, columns, 3), columns, 0)
    coefficients = mul_nn(columns, inverse_low, 3) * scale_row
    if last:
        return coefficients, None, gram_stiff, gram_mass
    projected = mul_nt(mul_nn(columns, reduced, 3), columns, 3)
    return coefficients, 0.5 * (projected + transposed(projected)), gram_stiff, gram_mass


def halves_next(coefficients, projected, gram_stiff, gram_mass):
    order = gram_stiff.shape[0]
    wanted = coefficients.shape[0]
    lane = lane_of((wanted, LANES))
    first = lane < wanted
    stiff_top = jnp.where(first, 0.5 * projected, 0.0)
    mass_top = jnp.where(eye_of(wanted), 0.5, 0.0)
    blank = jnp.zeros((wanted, LANES), F32)
    if order == wanted:
        return jnp.concatenate([stiff_top, blank], axis=0), jnp.concatenate([mass_top, blank], axis=0)
    later = jnp.where(first, 0.0, coefficients)
    both = jnp.concatenate([mul_nn(later, gram_stiff, 3), mul_nn(later, gram_mass, 3)], axis=0)
    crossed = mul_nt(both, jnp.concatenate([coefficients, later], axis=0), 3)
    moved = pltpu.roll(crossed, wanted, 1)
    lane = lane_of((2 * wanted, LANES))
    tail = jnp.where((lane >= 2 * wanted) & (lane < 3 * wanted), 0.5 * moved, 0.0)
    crossed = jnp.where(lane < wanted, crossed, tail)
    return (
        jnp.concatenate([stiff_top, blank, crossed[:wanted]], axis=0),
        jnp.concatenate([mass_top, blank, crossed[wanted:]], axis=0),
    )


def odd_lanes(rows):
    return (lane_of((rows, LANES)) // MODES) % 2 == 1


def pack_gram(gram):
    rows = gram.shape[0]
    gram = jnp.where(odd_lanes(rows), gram, 0.0)
    if rows <= 2 * MODES:
        return gram
    top = gram[:MODES] + pltpu.roll(gram[2 * MODES :], MODES, 1)
    return jnp.concatenate([top, gram[MODES : 2 * MODES]], axis=0)


def unpack_gram(packed, order):
    if order > 2 * MODES:
        packed = jnp.concatenate([packed, pltpu.roll(packed[:MODES], LANES - MODES, 1)], axis=0)
    return jnp.where(odd_lanes(order), packed, 0.0)


def halves_now(parts, known, order):
    total = parts[0][...]
    for part in parts[1:]:
        total = total + part[...]
    total = unpack_gram(total, order)
    if order == MODES:
        first = lane_of((MODES, LANES)) < MODES
        stiff = jnp.where(first, 0.5 * pltpu.roll(total, LANES - MODES, 1), 0.0)
        mass = jnp.where(first, 0.5 * pltpu.roll(total, MODES, 1), 0.0)
        return stiff, mass
    row = row_of((order, LANES))
    lane = lane_of((order, LANES))
    total = total * jnp.where((row >= MODES) & (row < 2 * MODES), 0.5, 1.0)
    inside = (lane >= MODES) & (lane < 2 * MODES)
    stiff = known[0][...] + jnp.where(inside, total, 0.0)
    mass = known[1][...] + jnp.where(inside, pltpu.roll(total, LANES // 2, 1), 0.0)
    return stiff, mass


def stiffness_apply(split_ref, out_ref, diag_ref, coupling_ref, offsets_ref):
    count, slots, width = coupling_ref.shape[0], coupling_ref.shape[1], coupling_ref.shape[2]
    diagonal = lax.broadcasted_iota(jnp.int32, (width, width), 0) == lax.broadcasted_iota(
        jnp.int32, (width, width), 1
    )

    def block_step(block, carry):
        here = pl.ds(pl.multiple_of((block + REACH) * width, width), width)
        mine = split_ref[:, here]
        pair = pieces(jnp.where(diagonal, 0.0, diag_ref[block]), 2)
        own = fold(dot_nn(mine, jnp.concatenate(pair, axis=1)))
        spread = []
        for slot in range(slots):
            back = block + REACH - offsets_ref[block, slot]
            there = pl.ds(pl.multiple_of(back * width, width), width)
            pair = pieces(coupling_ref[block, slot], 2)
            own = own + fold(dot_nt(split_ref[:, there], jnp.concatenate(pair, axis=0)))
            spread.append((there, fold(dot_nn(mine, jnp.concatenate(pair, axis=1)))))
        out_ref[:, here] += own
        for there, product in spread:
            out_ref[:, there] += product
        return carry

    lax.fori_loop(0, count, block_step, 0)


def split_store(split_ref, at, value):
    rows = value.shape[0]
    high, low = pieces(value, 2)
    split_ref[:rows, at] = high
    split_ref[rows:, at] = low


def gram_of(basis_refs, vectors_ref, stiff_ref, mass):
    halo = stiff_ref.shape[1] - mass.shape[1]
    weighted = jnp.concatenate(
        [jnp.zeros((MODES, halo), F32), vectors_ref[:, halo:] * mass], axis=1
    )
    stiff_high, stiff_low = pieces(stiff_ref[...], 2)
    mass_high, mass_low = pieces(weighted, 2)
    right = jnp.concatenate([stiff_low, stiff_high, mass_low, mass_high], axis=0)
    basis = [pieces(ref[...], 2) for ref in basis_refs]
    left = jnp.concatenate([pair[0] for pair in basis] + [pair[1] for pair in basis], axis=0)
    out = dot_nt(left, right)
    rows = left.shape[0] // 2
    return pack_gram(out[:rows] + pltpu.roll(out[:rows], MODES, 1) + out[rows:])


def first_kernel(
    modes_ref, edge_ref, mass_ref, diag_ref, coupling_ref, offsets_ref,
    basis_ref, stiff_ref, gram_ref, inverse_ref, split_ref,
):
    halo = edge_ref.shape[1]
    count, width = diag_ref.shape[0], diag_ref.shape[1]
    basis_ref[:, :halo] = edge_ref[...]
    basis_ref[:, halo:] = modes_ref[...]
    split_store(split_ref, slice(None), basis_ref[...])
    stiff_ref[:, :halo] = jnp.zeros((MODES, halo), F32)
    diagonal = lax.broadcasted_iota(jnp.int32, (width, width), 0) == lax.broadcasted_iota(
        jnp.int32, (width, width), 1
    )
    for block in range(count):
        at = slice(block * width, (block + 1) * width)
        picked = jnp.sum(jnp.where(diagonal, diag_ref[block], 0.0), axis=0, keepdims=True)
        inverse_ref[:, at] = 1.0 / picked
        stiff_ref[:, halo + block * width : halo + (block + 1) * width] = modes_ref[:, at] * picked
    stiffness_apply(split_ref, stiff_ref, diag_ref, coupling_ref, offsets_ref)
    gram_ref[...] = gram_of([basis_ref], basis_ref, stiff_ref, mass_ref[...])


def combine(left, right):
    high, low = pieces(right, 2)
    pair = jnp.concatenate(pieces(left, 2), axis=0)
    rows = left.shape[0]
    out = dot_nn(pair, high)
    return out[:rows] + (out[rows:] + dot_nn(left.astype(BF16), low))


def middle_kernel(order, parts_count, *refs):
    refs = list(refs)
    take = lambda count: [refs.pop(0) for _ in range(count)]
    parts = take(parts_count)
    known = take(2) if order > MODES else []
    blocks = order // MODES
    basis = take(blocks)
    stiff = take(blocks)
    ahead_ref, behind_ref, mass_ref, inverse_ref, diag_ref, coupling_ref, offsets_ref = take(7)
    out_blocks = min(blocks + 1, 3)
    basis_out = take(out_blocks)
    stiff_out = take(out_blocks)
    gram_ref, half_stiff_ref, half_mass_ref = take(3)
    (split_ref,) = take(1)

    coefficients, projected, gram_stiff, gram_mass = ritz(
        *halves_now(parts, known, order), MODES, PURIFY, False
    )
    halves = halves_next(coefficients, projected, gram_stiff, gram_mass)
    half_stiff_ref[...] = halves[0]
    half_mass_ref[...] = halves[1]
    halo = ahead_ref.shape[1]
    extent = mass_ref.shape[1]
    mixing = coefficients[:, :order]
    if order > MODES:
        later = jnp.where(lane_of((MODES, LANES)) < MODES, 0.0, coefficients)
        mixing = jnp.concatenate([mixing, later[:, :order]], axis=0)
    newest = 0 if order == MODES else 1
    for start in range(0, extent, halo):
        at = slice(start, start + halo)
        current = [ref[:, at] for ref in stiff]
        if start == 0:
            current[newest] = current[newest] + ahead_ref[...]
        if start + halo == extent:
            current[newest] = current[newest] + behind_ref[...]
        vectors = combine(mixing, jnp.concatenate([ref[:, at] for ref in basis], axis=0))
        images = combine(mixing, jnp.concatenate(current, axis=0))
        mass = mass_ref[:, at]
        inverse = inverse_ref[:, at]
        modes, stiff_modes = vectors[:MODES], images[:MODES]
        basis_out[0][:, at] = modes
        stiff_out[0][:, at] = stiff_modes
        if order > MODES:
            basis_out[2][:, at] = vectors[MODES:]
            stiff_out[2][:, at] = images[MODES:]
        residual = stiff_modes - combine(projected[:, :MODES], modes * mass)
        precond = residual * inverse
        basis_out[1][:, at] = precond
        split_store(split_ref, at, precond)
        if start == 0:
            stiff_out[1][:, at] = jnp.zeros((MODES, halo), F32)
        else:
            stiff_out[1][:, at] = jnp.where(inverse > 0.0, residual, 0.0)
    stiffness_apply(split_ref, stiff_out[1], diag_ref, coupling_ref, offsets_ref)
    gram_ref[...] = gram_of(basis_out, basis_out[1], stiff_out[1], mass_ref[:, halo:])


def last_kernel(order, parts_count, weight, *refs):
    refs = list(refs)
    take = lambda count: [refs.pop(0) for _ in range(count)]
    parts = take(parts_count)
    known = take(2)
    blocks = order // MODES
    basis = take(blocks)
    stiff = take(blocks)
    behind_ref, mass_ref = take(2)
    mass_out, energy_out = take(2)
    coefficients = ritz(*halves_now(parts, known, order), MODES, PURIFY, True)[0]
    halo = behind_ref.shape[1]
    extent = mass_ref.shape[1]
    mixing = coefficients[:, :order]
    for start in range(halo, extent, halo):
        at = slice(start, start + halo)
        to = slice(start - halo, start)
        current = [ref[:, at] for ref in stiff]
        if start + halo == extent:
            current[1] = current[1] + behind_ref[...]
        vectors = combine(mixing, jnp.concatenate([ref[:, at] for ref in basis], axis=0))
        images = combine(mixing, jnp.concatenate(current, axis=0))
        mass_out[:, to] = weight * mass_ref[:, at] * jnp.sum(vectors * vectors, axis=0, keepdims=True)
        energy_out[:, to] = weight * jnp.sum(vectors * images, axis=0, keepdims=True)


def call(kernel, args, outs, scratch, flops):
    smem = [arg.dtype == jnp.int32 for arg in args]
    return pl.pallas_call(
        kernel,
        out_shape=[jax.ShapeDtypeStruct(shape, F32) for shape in outs],
        in_specs=[pl.BlockSpec(memory_space=pltpu.SMEM if flag else pltpu.VMEM) for flag in smem],
        out_specs=[pl.BlockSpec(memory_space=pltpu.VMEM)] * len(outs),
        scratch_shapes=scratch,
        compiler_params=pltpu.CompilerParams(vmem_limit_bytes=24 << 20),
        cost_estimate=pl.CostEstimate(flops=flops, bytes_accessed=1 << 20, transcendentals=0),
    )(*args)


def shifted(value, axis, steps):
    count = lax.axis_size(axis)
    return lax.ppermute(
        value, axis, [(at, at + steps) for at in range(max(0, -steps), min(count, count - steps))]
    )


def sum_parts(value, axis):
    count = lax.axis_size(axis)
    if count & (count - 1):
        return [lax.psum(value, axis)]
    parts = [value]
    stride = 1
    while stride < count:
        if len(parts) > 1:
            value = parts[0] + parts[1] if len(parts) == 2 else (parts[0] + parts[1]) + (parts[2] + parts[3])
        masks = [stride, 2 * stride, 3 * stride] if 4 * stride <= count else [stride]
        parts = [value] + [
            lax.ppermute(value, axis, [(at, at ^ mask) for at in range(count)]) for mask in masks
        ]
        stride *= 1 << len(masks).bit_length()
    return parts


def local(diag_blocks, coupling, offsets, mass, initial_modes):
    count, width = diag_blocks.shape[0], diag_blocks.shape[1]
    own = count * width
    halo = REACH * width
    extent = own + halo
    split = [pltpu.VMEM((2 * MODES, extent), BF16)]
    matrices = [diag_blocks, coupling, offsets]
    mass = mass.reshape(1, own)
    edge = shifted(initial_modes[:, own - halo :], "row", 1)
    vectors, stiff, gram, inverse = call(
        first_kernel,
        [initial_modes, edge, mass, *matrices],
        [(MODES, extent), (MODES, extent), (MODES, LANES), (1, own)],
        split,
        1 << 30,
    )
    rows = jnp.concatenate([mass[:, own - halo :], inverse[:, own - halo :]], axis=0)
    rows = shifted(rows, "row", 1)
    mass_wide = jnp.concatenate([rows[:1], mass], axis=1)
    inverse_wide = jnp.concatenate([rows[1:], inverse], axis=1)
    basis, images, known = [vectors], [stiff], []
    for iteration in range(ITERS):
        parts = sum_parts(gram, "row")
        newest = images[min(len(images) - 1, 1)]
        ahead = shifted(newest[:, own:], "row", 1)
        behind = shifted(newest[:, :halo], "row", -1)
        order = MODES * len(basis)
        out_blocks = min(len(basis) + 1, 3)
        wide = [(MODES, extent)] * out_blocks
        packed = (min(out_blocks, 2) * MODES, LANES)
        halves = [(out_blocks * MODES, LANES)] * 2
        outs = call(
            functools.partial(middle_kernel, order, len(parts)),
            [*parts, *known, *basis, *images, ahead, behind, mass_wide, inverse_wide, *matrices],
            [*wide, *wide, packed, *halves],
            split,
            1 << 31,
        )
        basis = outs[:out_blocks]
        images = outs[out_blocks : 2 * out_blocks]
        gram = outs[2 * out_blocks]
        known = outs[2 * out_blocks + 1 :]
    parts = sum_parts(gram, "row")
    behind = shifted(images[1][:, :halo], "row", -1)
    weight = own * lax.axis_size("row") / MODES
    outs = call(
        functools.partial(last_kernel, MODES * len(basis), len(parts), weight),
        [*parts, *known, *basis, *images, behind, mass_wide],
        [(1, own), (1, own)],
        [],
        1 << 31,
    )
    return outs[0].reshape(own), outs[1].reshape(own)


def solution(mesh):
    placed = (
        P(("sub", "row"), None, None),
        P(("sub", "row"), None, None, None),
        P(("sub", "row"), None),
        P(("sub", "row")),
        P(None, ("sub", "row")),
    )
    return jax.shard_map(
        local,
        mesh=mesh,
        in_specs=placed,
        out_specs=(P(("sub", "row")), P(("sub", "row"))),
        check_vma=False,
    )
```

```python
import functools

import jax
import jax.numpy as jnp
from jax import lax
from jax.experimental import pallas as pl
from jax.experimental.pallas import tpu as pltpu
from jax.sharding import PartitionSpec as P

MODES = 32
REACH = 4
ITERS = 3
PURIFY = 28
LANES = 128
SETTLED = 1e-8
F32 = jnp.float32
BF16 = jnp.bfloat16


def pieces(value, count):
    parts = []
    for index in range(count):
        part = value.astype(BF16)
        parts.append(part)
        if index + 1 < count:
            value = value - part.astype(F32)
    return parts


def dot_nn(left, right):
    return lax.dot_general(left, right, (((1,), (0,)), ((), ())), preferred_element_type=F32)


def dot_nt(left, right):
    return lax.dot_general(left, right, (((1,), (1,)), ((), ())), preferred_element_type=F32)


def pad_rows(value):
    short = LANES - value.shape[0]
    if short == 0:
        return value
    return jnp.concatenate([value, jnp.zeros((short, value.shape[1]), value.dtype)], axis=0)


def transposed(value):
    return pad_rows(value).T[: value.shape[0]]


def fold(out):
    rows, width = out.shape[0] // 2, out.shape[1] // 2
    out = out[:rows] + out[rows:]
    return out[:, :width] + out[:, width:]


def mul_nn(left, right, count):
    rows = left.shape[0]
    left = pieces(left, count)
    right = [pad_rows(part) for part in pieces(right, count)]
    out = dot_nn(jnp.concatenate(left, axis=0), jnp.concatenate(right[:2], axis=1))
    total = fold(out[: 2 * rows])
    if count == 3:
        total = total + (
            out[2 * rows :, :LANES] + dot_nn(left[0], right[2])
        )
    return total


def mul_nt(left, right, count):
    left = pieces(left, count)
    right = [pad_rows(part) for part in pieces(right, count)]
    total = None
    for i in range(count):
        for j in range(count - i):
            term = dot_nt(left[i], right[j])
            total = term if total is None else total + term
    return total


def lane_of(shape):
    return lax.broadcasted_iota(jnp.int32, shape, 1)


def row_of(shape):
    return lax.broadcasted_iota(jnp.int32, shape, 0)


def eye_of(rows, lead=0):
    shape = (rows, LANES)
    return lane_of(shape) == row_of(shape) + lead


def eliminate(matrix, other, lead):
    order = matrix.shape[0]
    tiles = order // 8
    a = [matrix[8 * i : 8 * i + 8] for i in range(tiles)]
    e = [other[8 * i : 8 * i + 8] for i in range(tiles)]
    sub = row_of((8, LANES))
    for kt in range(tiles):
        below = range(kt, tiles)
        columns = [
            {
                i: jnp.broadcast_to(a[i][:, lead + 8 * kt + k : lead + 8 * kt + k + 1], (8, LANES))
                for i in below
            }
            for k in range(8)
        ]
        for k in range(8):
            head = lambda tile: jnp.broadcast_to(tile[k : k + 1, :], (8, LANES))
            pivot = head(columns[k][kt])
            inverse = 1.0 / pivot
            ratios = {i: columns[k][i] * inverse for i in below}
            ratios[kt] = jnp.where(sub > k, ratios[kt], 0.0)
            for later in range(k + 1, 8):
                top = head(columns[later][kt])
                for i in below:
                    columns[later][i] = columns[later][i] - ratios[i] * top
            row_a, row_e = head(a[kt]), head(e[kt])
            for i in below:
                a[i] = a[i] - ratios[i] * row_a
                e[i] = e[i] - ratios[i] * row_e
            e[kt] = jnp.where(sub == k, e[kt] * lax.rsqrt(pivot), e[kt])
    return jnp.concatenate(e, axis=0)


def total_of(value):
    return jnp.sum(jnp.sum(value, axis=0, keepdims=True), axis=1, keepdims=True)


def purify(matrix, wanted, steps):
    order = matrix.shape[0]
    eye = eye_of(order)
    valid = lane_of((1, LANES)) < order
    diagonal = jnp.sum(jnp.where(eye, matrix, 0.0), axis=0, keepdims=True)
    center = jnp.sum(diagonal, axis=1, keepdims=True) / order
    radius = jnp.sum(jnp.where(eye, 0.0, jnp.abs(matrix)), axis=0, keepdims=True)
    highest = jnp.max(jnp.where(valid, diagonal + radius, -jnp.inf), axis=1, keepdims=True)
    lowest = jnp.min(jnp.where(valid, diagonal - radius, jnp.inf), axis=1, keepdims=True)
    factor = jnp.minimum(
        wanted / jnp.maximum(highest - center, 1e-06),
        (order - wanted) / jnp.maximum(center - lowest, 1e-06),
    )
    ones = jnp.where(eye, 1.0, 0.0)
    initial = factor / order * (center * ones - matrix) + wanted / order * ones

    def purify_step(density):
        square = mul_nn(density, density, 2)
        cube = mul_nn(square, density, 2)
        gap = density - square
        below = total_of(jnp.where(eye, density, 0.0) - density * density)
        above = total_of(density * gap)
        change = total_of(gap * gap)
        safe = jnp.where(jnp.abs(below) > 1e-12, below, 1.0)
        ratio = jnp.clip(above / safe, 0.0, 1.0)
        high = ratio >= 0.5
        scale = 1.0 / jnp.where(high, jnp.maximum(ratio, 0.5), jnp.maximum(1.0 - ratio, 0.5))
        first = jnp.where(high, 0.0, 1.0 - 2.0 * ratio) * scale
        second = (1.0 + ratio) * scale
        return first * density + second * square - scale * cube, change

    def advance(carry):
        index, _, density = carry
        density, change = purify_step(density)
        return index + 1, change[0, 0], density

    def unsettled(carry):
        return (carry[0] < steps) & (carry[1] > SETTLED)

    return lax.while_loop(unsettled, advance, (0, jnp.float32(1.0), initial))[2]


def ritz(half_stiff, half_mass, wanted, steps, last):
    order = half_stiff.shape[0]
    eye = eye_of(order)
    gram_stiff = half_stiff + transposed(half_stiff)
    gram_mass = half_mass + transposed(half_mass)
    picked = jnp.where(eye, gram_mass, 0.0)
    scale_col = lax.rsqrt(jnp.sum(picked, axis=1, keepdims=True) + 1e-06)
    scale_row = lax.rsqrt(jnp.sum(picked, axis=0, keepdims=True) + 1e-06)
    stiff = scale_col * gram_stiff * scale_row
    mass = scale_col * gram_mass * scale_row
    ones = jnp.where(eye, 1.0, 0.0)
    if order == wanted:
        inverse_low = eliminate(mass, ones, 0)
    else:
        known = lane_of((1, LANES)) < wanted
        pivots = jnp.where(known, jnp.sum(jnp.where(eye, mass, 0.0), axis=0, keepdims=True), 1.0)
        ratio = jnp.where(known, mass[wanted:], 0.0) / pivots
        rest = jnp.where(known, 0.0, mass[wanted:] - mul_nn(ratio, mass[:wanted], 3))
        inverse_low = jnp.concatenate(
            [ones[:wanted] * lax.rsqrt(pivots), eliminate(rest, ones[wanted:] - ratio, wanted)], axis=0
        )
    reduced = mul_nt(mul_nn(inverse_low, stiff, 3), inverse_low, 3)
    reduced = 0.5 * (reduced + transposed(reduced))
    if order == wanted:
        return inverse_low * scale_row, reduced, gram_stiff, gram_mass
    columns = purify(reduced, wanted, steps)[:wanted]
    columns = eliminate(mul_nt(columns, columns, 3), columns, 0)
    coefficients = mul_nn(columns, inverse_low, 3) * scale_row
    if last:
        return coefficients, None, gram_stiff, gram_mass
    projected = mul_nt(mul_nn(columns, reduced, 3), columns, 3)
    return coefficients, 0.5 * (projected + transposed(projected)), gram_stiff, gram_mass


def halves_next(coefficients, projected, gram_stiff, gram_mass):
    order = gram_stiff.shape[0]
    wanted = coefficients.shape[0]
    lane = lane_of((wanted, LANES))
    first = lane < wanted
    stiff_top = jnp.where(first, 0.5 * projected, 0.0)
    mass_top = jnp.where(eye_of(wanted), 0.5, 0.0)
    blank = jnp.zeros((wanted, LANES), F32)
    if order == wanted:
        return jnp.concatenate([stiff_top, blank], axis=0), jnp.concatenate([mass_top, blank], axis=0)
    later = jnp.where(first, 0.0, coefficients)
    both = jnp.concatenate([mul_nn(later, gram_stiff, 3), mul_nn(later, gram_mass, 3)], axis=0)
    crossed = mul_nt(both, jnp.concatenate([coefficients, later], axis=0), 3)
    moved = pltpu.roll(crossed, wanted, 1)
    lane = lane_of((2 * wanted, LANES))
    tail = jnp.where((lane >= 2 * wanted) & (lane < 3 * wanted), 0.5 * moved, 0.0)
    crossed = jnp.where(lane < wanted, crossed, tail)
    return (
        jnp.concatenate([stiff_top, blank, crossed[:wanted]], axis=0),
        jnp.concatenate([mass_top, blank, crossed[wanted:]], axis=0),
    )


def odd_lanes(rows):
    return (lane_of((rows, LANES)) // MODES) % 2 == 1


def pack_gram(gram):
    rows = gram.shape[0]
    gram = jnp.where(odd_lanes(rows), gram, 0.0)
    if rows <= 2 * MODES:
        return gram
    top = gram[:MODES] + pltpu.roll(gram[2 * MODES :], MODES, 1)
    return jnp.concatenate([top, gram[MODES : 2 * MODES]], axis=0)


def unpack_gram(packed, order):
    if order > 2 * MODES:
        packed = jnp.concatenate([packed, pltpu.roll(packed[:MODES], LANES - MODES, 1)], axis=0)
    return jnp.where(odd_lanes(order), packed, 0.0)


def halves_now(parts, known, order):
    total = parts[0][...]
    for part in parts[1:]:
        total = total + part[...]
    total = unpack_gram(total, order)
    if order == MODES:
        first = lane_of((MODES, LANES)) < MODES
        stiff = jnp.where(first, 0.5 * pltpu.roll(total, LANES - MODES, 1), 0.0)
        mass = jnp.where(first, 0.5 * pltpu.roll(total, MODES, 1), 0.0)
        return stiff, mass
    row = row_of((order, LANES))
    lane = lane_of((order, LANES))
    total = total * jnp.where((row >= MODES) & (row < 2 * MODES), 0.5, 1.0)
    inside = (lane >= MODES) & (lane < 2 * MODES)
    stiff = known[0][...] + jnp.where(inside, total, 0.0)
    mass = known[1][...] + jnp.where(inside, pltpu.roll(total, LANES // 2, 1), 0.0)
    return stiff, mass


def stiffness_apply(split_ref, out_ref, diag_ref, coupling_ref, offsets_ref):
    count, slots, width = coupling_ref.shape[0], coupling_ref.shape[1], coupling_ref.shape[2]
    diagonal = lax.broadcasted_iota(jnp.int32, (width, width), 0) == lax.broadcasted_iota(
        jnp.int32, (width, width), 1
    )

    def block_step(block, carry):
        here = pl.ds(pl.multiple_of((block + REACH) * width, width), width)
        mine = split_ref[:, here]
        pair = pieces(jnp.where(diagonal, 0.0, diag_ref[block]), 2)
        own = fold(dot_nn(mine, jnp.concatenate(pair, axis=1)))
        spread = []
        for slot in range(slots):
            back = block + REACH - offsets_ref[block, slot]
            there = pl.ds(pl.multiple_of(back * width, width), width)
            pair = pieces(coupling_ref[block, slot], 2)
            own = own + fold(dot_nt(split_ref[:, there], jnp.concatenate(pair, axis=0)))
            spread.append((there, fold(dot_nn(mine, jnp.concatenate(pair, axis=1)))))
        out_ref[:, here] += own
        for there, product in spread:
            out_ref[:, there] += product
        return carry

    lax.fori_loop(0, count, block_step, 0)


def split_store(split_ref, at, value):
    rows = value.shape[0]
    high, low = pieces(value, 2)
    split_ref[:rows, at] = high
    split_ref[rows:, at] = low


def gram_of(basis_refs, vectors_ref, stiff_ref, mass):
    halo = stiff_ref.shape[1] - mass.shape[1]
    weighted = jnp.concatenate(
        [jnp.zeros((MODES, halo), F32), vectors_ref[:, halo:] * mass], axis=1
    )
    stiff_high, stiff_low = pieces(stiff_ref[...], 2)
    mass_high, mass_low = pieces(weighted, 2)
    right = jnp.concatenate([stiff_low, stiff_high, mass_low, mass_high], axis=0)
    basis = [pieces(ref[...], 2) for ref in basis_refs]
    left = jnp.concatenate([pair[0] for pair in basis] + [pair[1] for pair in basis], axis=0)
    out = dot_nt(left, right)
    rows = left.shape[0] // 2
    out = out[:rows] + out[rows:]
    return pack_gram(out + pltpu.roll(out, MODES, 1))


def first_kernel(
    modes_ref, edge_ref, mass_ref, diag_ref, coupling_ref, offsets_ref,
    basis_ref, stiff_ref, gram_ref, inverse_ref, split_ref,
):
    halo = edge_ref.shape[1]
    count, width = diag_ref.shape[0], diag_ref.shape[1]
    basis_ref[:, :halo] = edge_ref[...]
    basis_ref[:, halo:] = modes_ref[...]
    split_store(split_ref, slice(None), basis_ref[...])
    stiff_ref[:, :halo] = jnp.zeros((MODES, halo), F32)
    diagonal = lax.broadcasted_iota(jnp.int32, (width, width), 0) == lax.broadcasted_iota(
        jnp.int32, (width, width), 1
    )
    for block in range(count):
        at = slice(block * width, (block + 1) * width)
        picked = jnp.sum(jnp.where(diagonal, diag_ref[block], 0.0), axis=0, keepdims=True)
        inverse_ref[:, at] = 1.0 / picked
        stiff_ref[:, halo + block * width : halo + (block + 1) * width] = modes_ref[:, at] * picked
    stiffness_apply(split_ref, stiff_ref, diag_ref, coupling_ref, offsets_ref)
    gram_ref[...] = gram_of([basis_ref], basis_ref, stiff_ref, mass_ref[...])


def combine(left, right):
    high, low = pieces(right, 2)
    pair = jnp.concatenate(pieces(left, 2), axis=0)
    rows = left.shape[0]
    out = dot_nn(pair, high)
    return out[:rows] + (out[rows:] + dot_nn(left.astype(BF16), low))


def middle_kernel(order, parts_count, *refs):
    refs = list(refs)
    take = lambda count: [refs.pop(0) for _ in range(count)]
    parts = take(parts_count)
    known = take(2) if order > MODES else []
    blocks = order // MODES
    basis = take(blocks)
    stiff = take(blocks)
    ahead_ref, behind_ref, mass_ref, inverse_ref, diag_ref, coupling_ref, offsets_ref = take(7)
    out_blocks = min(blocks + 1, 3)
    basis_out = take(out_blocks)
    stiff_out = take(out_blocks)
    gram_ref, half_stiff_ref, half_mass_ref = take(3)
    (split_ref,) = take(1)

    coefficients, projected, gram_stiff, gram_mass = ritz(
        *halves_now(parts, known, order), MODES, PURIFY, False
    )
    halves = halves_next(coefficients, projected, gram_stiff, gram_mass)
    half_stiff_ref[...] = halves[0]
    half_mass_ref[...] = halves[1]
    halo = ahead_ref.shape[1]
    extent = mass_ref.shape[1]
    mixing = coefficients[:, :order]
    if order > MODES:
        later = jnp.where(lane_of((MODES, LANES)) < MODES, 0.0, coefficients)
        mixing = jnp.concatenate([mixing, later[:, :order]], axis=0)
    newest = 0 if order == MODES else 1
    for start in range(0, extent, halo):
        at = slice(start, start + halo)
        current = [ref[:, at] for ref in stiff]
        if start == 0:
            current[newest] = current[newest] + ahead_ref[...]
        if start + halo == extent:
            current[newest] = current[newest] + behind_ref[...]
        vectors = combine(mixing, jnp.concatenate([ref[:, at] for ref in basis], axis=0))
        images = combine(mixing, jnp.concatenate(current, axis=0))
        mass = mass_ref[:, at]
        inverse = inverse_ref[:, at]
        modes, stiff_modes = vectors[:MODES], images[:MODES]
        basis_out[0][:, at] = modes
        stiff_out[0][:, at] = stiff_modes
        if order > MODES:
            basis_out[2][:, at] = vectors[MODES:]
            stiff_out[2][:, at] = images[MODES:]
        residual = stiff_modes - combine(projected[:, :MODES], modes * mass)
        precond = residual * inverse
        basis_out[1][:, at] = precond
        split_store(split_ref, at, precond)
        if start == 0:
            stiff_out[1][:, at] = jnp.zeros((MODES, halo), F32)
        else:
            stiff_out[1][:, at] = residual
    stiffness_apply(split_ref, stiff_out[1], diag_ref, coupling_ref, offsets_ref)
    gram_ref[...] = gram_of(basis_out, basis_out[1], stiff_out[1], mass_ref[:, halo:])


def last_kernel(order, parts_count, weight, *refs):
    refs = list(refs)
    take = lambda count: [refs.pop(0) for _ in range(count)]
    parts = take(parts_count)
    known = take(2)
    blocks = order // MODES
    basis = take(blocks)
    stiff = take(blocks)
    behind_ref, mass_ref = take(2)
    mass_out, energy_out = take(2)
    coefficients = ritz(*halves_now(parts, known, order), MODES, PURIFY, True)[0]
    halo = behind_ref.shape[1]
    extent = mass_ref.shape[1]
    mixing = coefficients[:, :order]
    for start in range(halo, extent, halo):
        at = slice(start, start + halo)
        to = slice(start - halo, start)
        current = [ref[:, at] for ref in stiff]
        if start + halo == extent:
            current[1] = current[1] + behind_ref[...]
        vectors = combine(mixing, jnp.concatenate([ref[:, at] for ref in basis], axis=0))
        images = combine(mixing, jnp.concatenate(current, axis=0))
        mass_out[:, to] = weight * mass_ref[:, at] * jnp.sum(vectors * vectors, axis=0, keepdims=True)
        energy_out[:, to] = weight * jnp.sum(vectors * images, axis=0, keepdims=True)


def call(kernel, args, outs, scratch, flops):
    smem = [arg.dtype == jnp.int32 for arg in args]
    return pl.pallas_call(
        kernel,
        out_shape=[jax.ShapeDtypeStruct(shape, F32) for shape in outs],
        in_specs=[pl.BlockSpec(memory_space=pltpu.SMEM if flag else pltpu.VMEM) for flag in smem],
        out_specs=[pl.BlockSpec(memory_space=pltpu.VMEM)] * len(outs),
        scratch_shapes=scratch,
        compiler_params=pltpu.CompilerParams(vmem_limit_bytes=24 << 20),
        cost_estimate=pl.CostEstimate(flops=flops, bytes_accessed=1 << 20, transcendentals=0),
    )(*args)


def shifted(value, axis, steps):
    count = lax.axis_size(axis)
    return lax.ppermute(
        value, axis, [(at, at + steps) for at in range(max(0, -steps), min(count, count - steps))]
    )


def sum_parts(value, axis):
    count = lax.axis_size(axis)
    if count & (count - 1):
        return [lax.psum(value, axis)]
    parts = [value]
    stride = 1
    while stride < count:
        if len(parts) > 1:
            value = parts[0] + parts[1] if len(parts) == 2 else (parts[0] + parts[1]) + (parts[2] + parts[3])
        masks = [stride, 2 * stride, 3 * stride] if 4 * stride <= count else [stride]
        parts = [value] + [
            lax.ppermute(value, axis, [(at, at ^ mask) for at in range(count)]) for mask in masks
        ]
        stride *= 1 << len(masks).bit_length()
    return parts


def local(diag_blocks, coupling, offsets, mass, initial_modes):
    count, width = diag_blocks.shape[0], diag_blocks.shape[1]
    own = count * width
    halo = REACH * width
    extent = own + halo
    split = [pltpu.VMEM((2 * MODES, extent), BF16)]
    matrices = [diag_blocks, coupling, offsets]
    mass = mass.reshape(1, own)
    edge = shifted(initial_modes[:, own - halo :], "row", 1)
    vectors, stiff, gram, inverse = call(
        first_kernel,
        [initial_modes, edge, mass, *matrices],
        [(MODES, extent), (MODES, extent), (MODES, LANES), (1, own)],
        split,
        1 << 30,
    )
    rows = jnp.concatenate([mass[:, own - halo :], inverse[:, own - halo :]], axis=0)
    rows = shifted(rows, "row", 1)
    mass_wide = jnp.concatenate([rows[:1], mass], axis=1)
    inverse_wide = jnp.concatenate([rows[1:], inverse], axis=1)
    basis, images, known = [vectors], [stiff], []
    for iteration in range(ITERS):
        parts = sum_parts(gram, "row")
        newest = images[min(len(images) - 1, 1)]
        ahead = shifted(newest[:, own:], "row", 1)
        behind = shifted(newest[:, :halo], "row", -1)
        order = MODES * len(basis)
        out_blocks = min(len(basis) + 1, 3)
        wide = [(MODES, extent)] * out_blocks
        packed = (min(out_blocks, 2) * MODES, LANES)
        halves = [(out_blocks * MODES, LANES)] * 2
        outs = call(
            functools.partial(middle_kernel, order, len(parts)),
            [*parts, *known, *basis, *images, ahead, behind, mass_wide, inverse_wide, *matrices],
            [*wide, *wide, packed, *halves],
            split,
            1 << 31,
        )
        basis = outs[:out_blocks]
        images = outs[out_blocks : 2 * out_blocks]
        gram = outs[2 * out_blocks]
        known = outs[2 * out_blocks + 1 :]
    parts = sum_parts(gram, "row")
    behind = shifted(images[1][:, :halo], "row", -1)
    weight = own * lax.axis_size("row") / MODES
    outs = call(
        functools.partial(last_kernel, MODES * len(basis), len(parts), weight),
        [*parts, *known, *basis, *images, behind, mass_wide],
        [(1, own), (1, own)],
        [],
        1 << 31,
    )
    return outs[0].reshape(own), outs[1].reshape(own)


def solution(mesh):
    placed = (
        P(("sub", "row"), None, None),
        P(("sub", "row"), None, None, None),
        P(("sub", "row"), None),
        P(("sub", "row")),
        P(None, ("sub", "row")),
    )
    return jax.shard_map(
        local,
        mesh=mesh,
        in_specs=placed,
        out_specs=(P(("sub", "row")), P(("sub", "row"))),
        check_vma=False,
    )
```

```python
import functools

import jax
import jax.numpy as jnp
from jax import lax
from jax.experimental import pallas as pl
from jax.experimental.pallas import tpu as pltpu
from jax.sharding import PartitionSpec as P

MODES = 32
REACH = 4
ITERS = 3
PURIFY = 28
LANES = 128
SETTLED = 1e-8
F32 = jnp.float32
BF16 = jnp.bfloat16


def pieces(value, count):
    parts = []
    for index in range(count):
        part = value.astype(BF16)
        parts.append(part)
        if index + 1 < count:
            value = value - part.astype(F32)
    return parts


def dot_nn(left, right):
    return lax.dot_general(left, right, (((1,), (0,)), ((), ())), preferred_element_type=F32)


def dot_nt(left, right):
    return lax.dot_general(left, right, (((1,), (1,)), ((), ())), preferred_element_type=F32)


def pad_rows(value):
    short = LANES - value.shape[0]
    if short == 0:
        return value
    return jnp.concatenate([value, jnp.zeros((short, value.shape[1]), value.dtype)], axis=0)


def transposed(value):
    return pad_rows(value).T[: value.shape[0]]


def fold(out):
    rows, width = out.shape[0] // 2, out.shape[1] // 2
    out = out[:rows] + out[rows:]
    return out[:, :width] + out[:, width:]


def mul_nn(left, right, count):
    rows = left.shape[0]
    left = pieces(left, count)
    right = [pad_rows(part) for part in pieces(right, count)]
    out = dot_nn(jnp.concatenate(left, axis=0), jnp.concatenate(right[:2], axis=1))
    total = fold(out[: 2 * rows])
    if count == 3:
        total = total + (
            out[2 * rows :, :LANES] + dot_nn(left[0], right[2])
        )
    return total


def mul_nt(left, right, count):
    left = pieces(left, count)
    right = [pad_rows(part) for part in pieces(right, count)]
    total = None
    for i in range(count):
        for j in range(count - i):
            term = dot_nt(left[i], right[j])
            total = term if total is None else total + term
    return total


def lane_of(shape):
    return lax.broadcasted_iota(jnp.int32, shape, 1)


def row_of(shape):
    return lax.broadcasted_iota(jnp.int32, shape, 0)


def eye_of(rows, lead=0):
    shape = (rows, LANES)
    return lane_of(shape) == row_of(shape) + lead


def eliminate(matrix, other, lead):
    order = matrix.shape[0]
    tiles = order // 8
    a = [matrix[8 * i : 8 * i + 8] for i in range(tiles)]
    e = [other[8 * i : 8 * i + 8] for i in range(tiles)]
    sub = row_of((8, LANES))
    for kt in range(tiles):
        below = range(kt, tiles)
        columns = [
            {
                i: jnp.broadcast_to(a[i][:, lead + 8 * kt + k : lead + 8 * kt + k + 1], (8, LANES))
                for i in below
            }
            for k in range(8)
        ]
        for k in range(8):
            head = lambda tile: jnp.broadcast_to(tile[k : k + 1, :], (8, LANES))
            pivot = head(columns[k][kt])
            inverse = 1.0 / pivot
            ratios = {i: columns[k][i] * inverse for i in below}
            ratios[kt] = jnp.where(sub > k, ratios[kt], 0.0)
            for later in range(k + 1, 8):
                top = head(columns[later][kt])
                for i in below:
                    columns[later][i] = columns[later][i] - ratios[i] * top
            row_a, row_e = head(a[kt]), head(e[kt])
            for i in below:
                a[i] = a[i] - ratios[i] * row_a
                e[i] = e[i] - ratios[i] * row_e
            e[kt] = jnp.where(sub == k, e[kt] * lax.rsqrt(pivot), e[kt])
    return jnp.concatenate(e, axis=0)


def total_of(value):
    return jnp.sum(jnp.sum(value, axis=0, keepdims=True), axis=1, keepdims=True)


def purify(matrix, wanted, steps):
    order = matrix.shape[0]
    eye = eye_of(order)
    valid = lane_of((1, LANES)) < order
    diagonal = jnp.sum(jnp.where(eye, matrix, 0.0), axis=0, keepdims=True)
    center = jnp.sum(diagonal, axis=1, keepdims=True) / order
    radius = jnp.sum(jnp.where(eye, 0.0, jnp.abs(matrix)), axis=0, keepdims=True)
    highest = jnp.max(jnp.where(valid, diagonal + radius, -jnp.inf), axis=1, keepdims=True)
    lowest = jnp.min(jnp.where(valid, diagonal - radius, jnp.inf), axis=1, keepdims=True)
    factor = jnp.minimum(
        wanted / jnp.maximum(highest - center, 1e-06),
        (order - wanted) / jnp.maximum(center - lowest, 1e-06),
    )
    ones = jnp.where(eye, 1.0, 0.0)
    initial = factor / order * (center * ones - matrix) + wanted / order * ones

    def purify_step(density):
        square = mul_nn(density, density, 2)
        cube = mul_nn(square, density, 2)
        gap = density - square
        below = total_of(jnp.where(eye, density, 0.0) - density * density)
        above = total_of(density * gap)
        change = total_of(gap * gap)
        safe = jnp.where(jnp.abs(below) > 1e-12, below, 1.0)
        ratio = jnp.clip(above / safe, 0.0, 1.0)
        high = ratio >= 0.5
        scale = 1.0 / jnp.where(high, jnp.maximum(ratio, 0.5), jnp.maximum(1.0 - ratio, 0.5))
        first = jnp.where(high, 0.0, 1.0 - 2.0 * ratio) * scale
        second = (1.0 + ratio) * scale
        return first * density + second * square - scale * cube, change

    def advance(carry):
        index, _, density = carry
        density, change = purify_step(density)
        return index + 1, change[0, 0], density

    def unsettled(carry):
        return (carry[0] < steps) & (carry[1] > SETTLED)

    return lax.while_loop(unsettled, advance, (0, jnp.float32(1.0), initial))[2]


def ritz(half_stiff, half_mass, wanted, steps, last):
    order = half_stiff.shape[0]
    eye = eye_of(order)
    gram_stiff = half_stiff + transposed(half_stiff)
    gram_mass = half_mass + transposed(half_mass)
    picked = jnp.where(eye, gram_mass, 0.0)
    scale_col = lax.rsqrt(jnp.sum(picked, axis=1, keepdims=True) + 1e-06)
    scale_row = lax.rsqrt(jnp.sum(picked, axis=0, keepdims=True) + 1e-06)
    stiff = scale_col * gram_stiff * scale_row
    mass = scale_col * gram_mass * scale_row
    ones = jnp.where(eye, 1.0, 0.0)
    if order == wanted:
        inverse_low = eliminate(mass, ones, 0)
    else:
        known = lane_of((1, LANES)) < wanted
        pivots = jnp.where(known, jnp.sum(jnp.where(eye, mass, 0.0), axis=0, keepdims=True), 1.0)
        ratio = jnp.where(known, mass[wanted:], 0.0) / pivots
        rest = jnp.where(known, 0.0, mass[wanted:] - mul_nn(ratio, mass[:wanted], 3))
        inverse_low = jnp.concatenate(
            [ones[:wanted] * lax.rsqrt(pivots), eliminate(rest, ones[wanted:] - ratio, wanted)], axis=0
        )
    reduced = mul_nt(mul_nn(inverse_low, stiff, 3), inverse_low, 3)
    reduced = 0.5 * (reduced + transposed(reduced))
    if order == wanted:
        return inverse_low * scale_row, reduced, gram_stiff, gram_mass
    columns = purify(reduced, wanted, steps)[:wanted]
    columns = eliminate(mul_nt(columns, columns, 3), columns, 0)
    coefficients = mul_nn(columns, inverse_low, 3) * scale_row
    if last:
        return coefficients, None, gram_stiff, gram_mass
    projected = mul_nt(mul_nn(columns, reduced, 3), columns, 3)
    return coefficients, 0.5 * (projected + transposed(projected)), gram_stiff, gram_mass


def halves_next(coefficients, projected, gram_stiff, gram_mass):
    order = gram_stiff.shape[0]
    wanted = coefficients.shape[0]
    lane = lane_of((wanted, LANES))
    first = lane < wanted
    stiff_top = jnp.where(first, 0.5 * projected, 0.0)
    mass_top = jnp.where(eye_of(wanted), 0.5, 0.0)
    blank = jnp.zeros((wanted, LANES), F32)
    if order == wanted:
        return jnp.concatenate([stiff_top, blank], axis=0), jnp.concatenate([mass_top, blank], axis=0)
    later = jnp.where(first, 0.0, coefficients)
    both = jnp.concatenate([mul_nn(later, gram_stiff, 3), mul_nn(later, gram_mass, 3)], axis=0)
    crossed = mul_nt(both, jnp.concatenate([coefficients, later], axis=0), 3)
    moved = pltpu.roll(crossed, wanted, 1)
    lane = lane_of((2 * wanted, LANES))
    tail = jnp.where((lane >= 2 * wanted) & (lane < 3 * wanted), 0.5 * moved, 0.0)
    crossed = jnp.where(lane < wanted, crossed, tail)
    return (
        jnp.concatenate([stiff_top, blank, crossed[:wanted]], axis=0),
        jnp.concatenate([mass_top, blank, crossed[wanted:]], axis=0),
    )


def odd_lanes(rows):
    return (lane_of((rows, LANES)) // MODES) % 2 == 1


def pack_gram(gram):
    rows = gram.shape[0]
    gram = jnp.where(odd_lanes(rows), gram, 0.0)
    if rows <= 2 * MODES:
        return gram
    top = gram[:MODES] + pltpu.roll(gram[2 * MODES :], MODES, 1)
    return jnp.concatenate([top, gram[MODES : 2 * MODES]], axis=0)


def unpack_gram(packed, order):
    if order > 2 * MODES:
        packed = jnp.concatenate([packed, pltpu.roll(packed[:MODES], LANES - MODES, 1)], axis=0)
    return jnp.where(odd_lanes(order), packed, 0.0)


def halves_now(parts, known, order):
    total = parts[0][...]
    for part in parts[1:]:
        total = total + part[...]
    total = unpack_gram(total, order)
    if order == MODES:
        first = lane_of((MODES, LANES)) < MODES
        stiff = jnp.where(first, 0.5 * pltpu.roll(total, LANES - MODES, 1), 0.0)
        mass = jnp.where(first, 0.5 * pltpu.roll(total, MODES, 1), 0.0)
        return stiff, mass
    row = row_of((order, LANES))
    lane = lane_of((order, LANES))
    total = total * jnp.where((row >= MODES) & (row < 2 * MODES), 0.5, 1.0)
    inside = (lane >= MODES) & (lane < 2 * MODES)
    stiff = known[0][...] + jnp.where(inside, total, 0.0)
    mass = known[1][...] + jnp.where(inside, pltpu.roll(total, LANES // 2, 1), 0.0)
    return stiff, mass


def stiffness_apply(split_ref, out_ref, offsets_ref, first, last, pairs_of):
    width = split_ref.shape[1] // (offsets_ref.shape[0] + REACH)
    slots = offsets_ref.shape[1]

    def block_step(block, carry):
        here = pl.ds(pl.multiple_of((block + REACH) * width, width), width)
        mine = split_ref[:, here]
        pairs = pairs_of(block)
        own = fold(dot_nn(mine, jnp.concatenate(pairs[0], axis=1)))
        spread = []
        for slot in range(slots):
            back = block + REACH - offsets_ref[block, slot]
            there = pl.ds(pl.multiple_of(back * width, width), width)
            pair = pairs[slot + 1]
            own = own + fold(dot_nt(split_ref[:, there], jnp.concatenate(pair, axis=0)))
            spread.append((there, fold(dot_nn(mine, jnp.concatenate(pair, axis=1)))))
        out_ref[:, here] += own
        for there, product in spread:
            out_ref[:, there] += product
        return carry

    lax.fori_loop(first, last, block_step, 0)


def loaded_pairs(pairs_ref):
    slots = pairs_ref.shape[1]
    return lambda block: [[pairs_ref[block, slot, 0], pairs_ref[block, slot, 1]] for slot in range(slots)]


def stacked(value, width):
    count = value.shape[1] // width
    return jnp.concatenate([value[:, width * i : width * (i + 1)] for i in range(count)], axis=0)


def unstacked(value, count):
    rows = value.shape[0] // count
    return jnp.concatenate([value[rows * i : rows * (i + 1)] for i in range(count)], axis=1)


def send_edges(gram, behind, ahead, even, gram_ref, near_ref, far_ref):
    behind, ahead = stacked(behind, LANES), stacked(ahead, LANES)
    rows = gram.shape[0]
    gram_ref[...] = gram
    near_ref[:rows, :] = gram
    near_ref[rows:, :] = jnp.where(even, ahead, behind)
    far_ref[...] = jnp.where(even, behind, ahead)


def received_edges(near_ref, far_ref, even):
    far = far_ref[...]
    near = near_ref[near_ref.shape[0] - far.shape[0] :, :]
    ahead, behind = jnp.where(even, far, near), jnp.where(even, near, far)
    return unstacked(ahead, REACH), unstacked(behind, REACH)


def split_store(split_ref, at, value):
    rows = value.shape[0]
    high, low = pieces(value, 2)
    split_ref[:rows, at] = high
    split_ref[rows:, at] = low


def gram_of(basis_refs, vectors_ref, stiff_ref, mass):
    halo = stiff_ref.shape[1] - mass.shape[1]
    weighted = jnp.concatenate(
        [jnp.zeros((MODES, halo), F32), vectors_ref[:, halo:] * mass], axis=1
    )
    stiff_high, stiff_low = pieces(stiff_ref[...], 2)
    mass_high, mass_low = pieces(weighted, 2)
    right = jnp.concatenate([stiff_low, stiff_high, mass_low, mass_high], axis=0)
    basis = [pieces(ref[...], 2) for ref in basis_refs]
    left = jnp.concatenate([pair[0] for pair in basis] + [pair[1] for pair in basis], axis=0)
    out = dot_nt(left, right)
    rows = left.shape[0] // 2
    out = out[:rows] + out[rows:]
    return pack_gram(out + pltpu.roll(out, MODES, 1))


def first_kernel(
    modes_hbm, diag_hbm, coupling_hbm, edge_ref, mass_ref, parity_ref, offsets_ref,
    basis_ref, stiff_ref, gram_ref, near_ref, far_ref, inverse_ref, mass_wide_ref, pairs_ref,
    split_ref, modes_ref, diag_ref, coupling_ref, semaphores,
):
    halo = edge_ref.shape[1]
    count, width = diag_ref.shape[0], diag_ref.shape[1]
    groups = semaphores.shape[0] // 2
    size = count // groups
    copies = [pltpu.make_async_copy(modes_hbm, modes_ref, semaphores.at[2 * groups])]
    for group in range(groups):
        at = pl.ds(group * size, size)
        copies.append(pltpu.make_async_copy(diag_hbm.at[at], diag_ref.at[at], semaphores.at[2 * group]))
        copies.append(
            pltpu.make_async_copy(coupling_hbm.at[at], coupling_ref.at[at], semaphores.at[2 * group + 1])
        )
    for copy in copies:
        copy.start()
    diagonal = lax.broadcasted_iota(jnp.int32, (width, width), 0) == lax.broadcasted_iota(
        jnp.int32, (width, width), 1
    )

    def pairs_of(block):
        values = [jnp.where(diagonal, 0.0, diag_ref[block])]
        values += [coupling_ref[block, slot] for slot in range(coupling_ref.shape[1])]
        pairs = [pieces(value, 2) for value in values]
        for index, pair in enumerate(pairs):
            pairs_ref[block, index, 0] = pair[0]
            pairs_ref[block, index, 1] = pair[1]
        return pairs

    copies[0].wait()
    basis_ref[:, :halo] = edge_ref[:MODES]
    basis_ref[:, halo:] = modes_ref[...]
    split_store(split_ref, slice(None), basis_ref[...])
    mass_wide_ref[:, :halo] = edge_ref[MODES : MODES + 1]
    mass_wide_ref[:, halo:] = mass_ref[...]
    stiff_ref[...] = jnp.zeros(stiff_ref.shape, F32)
    for group in range(groups):
        copies[2 * group + 1].wait()
        copies[2 * group + 2].wait()
        for block in range(group * size, (group + 1) * size):
            at = slice(block * width, (block + 1) * width)
            picked = jnp.sum(jnp.where(diagonal, diag_ref[block], 0.0), axis=0, keepdims=True)
            inverse_ref[:, at] = 1.0 / picked
            stiff_ref[:, halo + block * width : halo + (block + 1) * width] += modes_ref[:, at] * picked
        stiffness_apply(split_ref, stiff_ref, offsets_ref, group * size, (group + 1) * size, pairs_of)
    gram = gram_of([basis_ref], basis_ref, stiff_ref, mass_ref[...])
    extra = edge_ref.shape[0] - MODES
    tail = jnp.broadcast_to(inverse_ref[:, inverse_ref.shape[1] - halo :], (extra, halo))
    behind = jnp.concatenate([stiff_ref[:, :halo], tail], axis=0)
    ahead = jnp.concatenate([stiff_ref[:, stiff_ref.shape[1] - halo :], tail], axis=0)
    send_edges(gram, behind, ahead, parity_ref[0] == 0, gram_ref, near_ref, far_ref)


def combine(left, right):
    high, low = pieces(right, 2)
    pair = jnp.concatenate(pieces(left, 2), axis=0)
    rows = left.shape[0]
    out = dot_nn(pair, high)
    return out[:rows] + (out[rows:] + dot_nn(left.astype(BF16), low))


def middle_kernel(order, parts_count, *refs):
    refs = list(refs)
    take = lambda count: [refs.pop(0) for _ in range(count)]
    parts = take(parts_count)
    known = take(2) if order > MODES else []
    blocks = order // MODES
    basis = take(blocks)
    stiff = take(blocks)
    near_in, far_in, mass_ref, inverse_in, pairs_ref, parity_ref, offsets_ref = take(7)
    out_blocks = min(blocks + 1, 3)
    basis_out = take(out_blocks)
    stiff_out = take(out_blocks)
    gram_ref, near_ref, far_ref, half_stiff_ref, half_mass_ref = take(5)
    inverse_ref = take(1)[0] if order == MODES else inverse_in
    (split_ref,) = take(1)

    even = parity_ref[0] == 0
    coefficients, projected, gram_stiff, gram_mass = ritz(
        *halves_now(parts, known, order), MODES, PURIFY, False
    )
    halves = halves_next(coefficients, projected, gram_stiff, gram_mass)
    half_stiff_ref[...] = halves[0]
    half_mass_ref[...] = halves[1]
    ahead, behind = received_edges(near_in, far_in, even)
    halo = ahead.shape[1]
    extent = mass_ref.shape[1]
    if order == MODES:
        inverse_ref[:, :halo] = ahead[MODES : MODES + 1]
        inverse_ref[:, halo:] = inverse_in[...]
    mixing = coefficients[:, :order]
    if order > MODES:
        later = jnp.where(lane_of((MODES, LANES)) < MODES, 0.0, coefficients)
        mixing = jnp.concatenate([mixing, later[:, :order]], axis=0)
    newest = 0 if order == MODES else 1
    for start in range(0, extent, halo):
        at = slice(start, start + halo)
        current = [ref[:, at] for ref in stiff]
        if start == 0:
            current[newest] = current[newest] + ahead[:MODES]
        if start + halo == extent:
            current[newest] = current[newest] + behind[:MODES]
        vectors = combine(mixing, jnp.concatenate([ref[:, at] for ref in basis], axis=0))
        images = combine(mixing, jnp.concatenate(current, axis=0))
        modes, stiff_modes = vectors[:MODES], images[:MODES]
        basis_out[0][:, at] = modes
        stiff_out[0][:, at] = stiff_modes
        if order > MODES:
            basis_out[2][:, at] = vectors[MODES:]
            stiff_out[2][:, at] = images[MODES:]
        residual = stiff_modes - combine(projected[:, :MODES], modes * mass_ref[:, at])
        precond = residual * inverse_ref[:, at]
        basis_out[1][:, at] = precond
        split_store(split_ref, at, precond)
        stiff_out[1][:, at] = jnp.zeros((MODES, halo), F32) if start == 0 else residual
    stiffness_apply(split_ref, stiff_out[1], offsets_ref, 0, offsets_ref.shape[0], loaded_pairs(pairs_ref))
    gram = gram_of(basis_out, basis_out[1], stiff_out[1], mass_ref[:, halo:])
    newest = stiff_out[1]
    send_edges(gram, newest[:, :halo], newest[:, extent - halo :], even, gram_ref, near_ref, far_ref)


def last_kernel(order, parts_count, weight, *refs):
    refs = list(refs)
    take = lambda count: [refs.pop(0) for _ in range(count)]
    parts = take(parts_count)
    known = take(2)
    blocks = order // MODES
    basis = take(blocks)
    stiff = take(blocks)
    near_in, far_in, mass_ref, parity_ref = take(4)
    mass_out, energy_out = take(2)
    coefficients = ritz(*halves_now(parts, known, order), MODES, PURIFY, True)[0]
    behind = received_edges(near_in, far_in, parity_ref[0] == 0)[1]
    halo = behind.shape[1]
    extent = mass_ref.shape[1]
    mixing = coefficients[:, :order]
    for start in range(halo, extent, halo):
        at = slice(start, start + halo)
        to = slice(start - halo, start)
        current = [ref[:, at] for ref in stiff]
        if start + halo == extent:
            current[1] = current[1] + behind
        vectors = combine(mixing, jnp.concatenate([ref[:, at] for ref in basis], axis=0))
        images = combine(mixing, jnp.concatenate(current, axis=0))
        mass_out[:, to] = weight * mass_ref[:, at] * jnp.sum(vectors * vectors, axis=0, keepdims=True)
        energy_out[:, to] = weight * jnp.sum(vectors * images, axis=0, keepdims=True)


def call(kernel, args, outs, scratch, flops, spaces=()):
    spaces = list(spaces) + [pltpu.VMEM] * (len(args) - len(spaces))
    spaces = [pltpu.SMEM if arg.dtype == jnp.int32 else space for arg, space in zip(args, spaces)]
    return pl.pallas_call(
        kernel,
        out_shape=[
            jax.ShapeDtypeStruct(shape, BF16 if len(shape) > 2 else F32) for shape in outs
        ],
        in_specs=[pl.BlockSpec(memory_space=space) for space in spaces],
        out_specs=[pl.BlockSpec(memory_space=pltpu.VMEM)] * len(outs),
        scratch_shapes=scratch,
        compiler_params=pltpu.CompilerParams(vmem_limit_bytes=24 << 20),
        cost_estimate=pl.CostEstimate(flops=flops, bytes_accessed=1 << 20, transcendentals=0),
    )(*args)


def exchange(gram, near, far, axis):
    count = lax.axis_size(axis)
    across = lambda value, mask: lax.ppermute(
        value, axis, [(at, at ^ mask) for at in range(count) if at ^ mask < count]
    )
    near = across(near, 1)
    if count & (count - 1):
        parts = [lax.psum(gram, axis)]
    else:
        parts, stride = [gram], 1
        while stride < count:
            if len(parts) > 1:
                gram = sum(parts[1:], parts[0])
            masks = [stride, 2 * stride, 3 * stride] if 4 * stride <= count else [stride]
            parts = [gram] + [
                near[: gram.shape[0]] if mask == 1 else across(gram, mask) for mask in masks
            ]
            stride *= 1 << len(masks).bit_length()
    hops = [(at, at + 1 if at % 2 else at - 1) for at in range(count)]
    far = lax.ppermute(far, axis, [hop for hop in hops if 0 <= hop[1] < count])
    return parts, near, far


def local(diag_blocks, coupling, offsets, mass, initial_modes):
    count, width = diag_blocks.shape[0], diag_blocks.shape[1]
    slots = coupling.shape[1]
    own = count * width
    halo = REACH * width
    extent = own + halo
    split = [pltpu.VMEM((2 * MODES, extent), BF16)]
    parity = (lax.axis_index("row") % 2).astype(jnp.int32).reshape(1)
    mass = mass.reshape(1, own)
    spare = 8
    edge = jnp.concatenate(
        [initial_modes[:, own - halo :], jnp.broadcast_to(mass[:, own - halo :], (spare, halo))], axis=0
    )
    ranks = lax.axis_size("row")
    edge = lax.ppermute(edge, "row", [(at, at + 1) for at in range(ranks - 1)])
    edge_rows = REACH * (MODES + spare)
    groups = 4 if count % 4 == 0 else 1
    vectors, stiff, gram, near, far, inverse, mass_wide, pairs = call(
        first_kernel,
        [initial_modes, diag_blocks, coupling, edge, mass, parity, offsets],
        [
            (MODES, extent), (MODES, extent), (MODES, LANES), (MODES + edge_rows, LANES),
            (edge_rows, LANES), (1, own), (1, extent), (count, slots + 1, 2, width, width),
        ],
        split
        + [
            pltpu.VMEM((MODES, own), F32),
            pltpu.VMEM((count, width, width), F32),
            pltpu.VMEM((count, slots, width, width), F32),
            pltpu.SemaphoreType.DMA((2 * groups + 1,)),
        ],
        1 << 30,
        [pl.ANY] * 3,
    )
    edge_rows = REACH * MODES
    basis, images, known = [vectors], [stiff], []
    for iteration in range(ITERS):
        parts, near, far = exchange(gram, near, far, "row")
        order = MODES * len(basis)
        out_blocks = min(len(basis) + 1, 3)
        wide = [(MODES, extent)] * out_blocks
        packed = min(out_blocks, 2) * MODES
        halves = [(out_blocks * MODES, LANES)] * 2
        outs = call(
            functools.partial(middle_kernel, order, len(parts)),
            [*parts, *known, *basis, *images, near, far, mass_wide, inverse, pairs, parity, offsets],
            [
                *wide, *wide, (packed, LANES), (packed + edge_rows, LANES), (edge_rows, LANES), *halves,
                *([(1, extent)] if order == MODES else []),
            ],
            split,
            1 << 31,
        )
        basis = outs[:out_blocks]
        images = outs[out_blocks : 2 * out_blocks]
        gram, near, far = outs[2 * out_blocks : 2 * out_blocks + 3]
        known = outs[2 * out_blocks + 3 : 2 * out_blocks + 5]
        if order == MODES:
            inverse = outs[-1]
    parts, near, far = exchange(gram, near, far, "row")
    weight = own * ranks / MODES
    outs = call(
        functools.partial(last_kernel, MODES * len(basis), len(parts), weight),
        [*parts, *known, *basis, *images, near, far, mass_wide, parity],
        [(1, own), (1, own)],
        [],
        1 << 31,
    )
    return outs[0].reshape(own), outs[1].reshape(own)


def solution(mesh):
    placed = (
        P(("sub", "row"), None, None),
        P(("sub", "row"), None, None, None),
        P(("sub", "row"), None),
        P(("sub", "row")),
        P(None, ("sub", "row")),
    )
    return jax.shard_map(
        local,
        mesh=mesh,
        in_specs=placed,
        out_specs=(P(("sub", "row")), P(("sub", "row"))),
        check_vma=False,
    )
```

```python
import functools

import jax
import jax.numpy as jnp
from jax import lax
from jax.experimental import pallas as pl
from jax.experimental.pallas import tpu as pltpu
from jax.sharding import PartitionSpec as P

MODES = 32
REACH = 4
ITERS = 3
PURIFY = 28
LANES = 128
SETTLED = 1e-8
F32 = jnp.float32
BF16 = jnp.bfloat16


def pieces(value, count):
    parts = []
    for index in range(count):
        part = value.astype(BF16)
        parts.append(part)
        if index + 1 < count:
            value = value - part.astype(F32)
    return parts


def dot_nn(left, right):
    return lax.dot_general(left, right, (((1,), (0,)), ((), ())), preferred_element_type=F32)


def dot_nt(left, right):
    return lax.dot_general(left, right, (((1,), (1,)), ((), ())), preferred_element_type=F32)


def pad_rows(value):
    short = LANES - value.shape[0]
    if short == 0:
        return value
    return jnp.concatenate([value, jnp.zeros((short, value.shape[1]), value.dtype)], axis=0)


def transposed(value):
    return pad_rows(value).T[: value.shape[0]]


def fold(out):
    rows, width = out.shape[0] // 2, out.shape[1] // 2
    out = out[:rows] + out[rows:]
    return out[:, :width] + out[:, width:]


def mul_nn(left, right, count):
    rows = left.shape[0]
    left = pieces(left, count)
    right = [pad_rows(part) for part in pieces(right, count)]
    out = dot_nn(jnp.concatenate(left, axis=0), jnp.concatenate(right[:2], axis=1))
    total = fold(out[: 2 * rows])
    if count == 3:
        total = total + (
            out[2 * rows :, :LANES] + dot_nn(left[0], right[2])
        )
    return total


def mul_nt(left, right, count):
    left = pieces(left, count)
    right = [pad_rows(part) for part in pieces(right, count)]
    total = None
    for i in range(count):
        for j in range(count - i):
            term = dot_nt(left[i], right[j])
            total = term if total is None else total + term
    return total


def lane_of(shape):
    return lax.broadcasted_iota(jnp.int32, shape, 1)


def row_of(shape):
    return lax.broadcasted_iota(jnp.int32, shape, 0)


def eye_of(rows, lead=0):
    shape = (rows, LANES)
    return lane_of(shape) == row_of(shape) + lead


def eliminate(matrix, other, lead):
    order = matrix.shape[0]
    tiles = order // 8
    a = [matrix[8 * i : 8 * i + 8] for i in range(tiles)]
    e = [other[8 * i : 8 * i + 8] for i in range(tiles)]
    sub = row_of((8, LANES))
    for kt in range(tiles):
        below = range(kt, tiles)
        columns = [
            {
                i: jnp.broadcast_to(a[i][:, lead + 8 * kt + k : lead + 8 * kt + k + 1], (8, LANES))
                for i in below
            }
            for k in range(8)
        ]
        for k in range(8):
            head = lambda tile: jnp.broadcast_to(tile[k : k + 1, :], (8, LANES))
            pivot = head(columns[k][kt])
            inverse = 1.0 / pivot
            ratios = {i: columns[k][i] * inverse for i in below}
            ratios[kt] = jnp.where(sub > k, ratios[kt], 0.0)
            for later in range(k + 1, 8):
                top = head(columns[later][kt])
                for i in below:
                    columns[later][i] = columns[later][i] - ratios[i] * top
            row_a, row_e = head(a[kt]), head(e[kt])
            for i in below:
                a[i] = a[i] - ratios[i] * row_a
                e[i] = e[i] - ratios[i] * row_e
            e[kt] = jnp.where(sub == k, e[kt] * lax.rsqrt(pivot), e[kt])
    return jnp.concatenate(e, axis=0)


def total_of(value):
    return jnp.sum(jnp.sum(value, axis=0, keepdims=True), axis=1, keepdims=True)


def purify(matrix, wanted, steps):
    order = matrix.shape[0]
    eye = eye_of(order)
    valid = lane_of((1, LANES)) < order
    diagonal = jnp.sum(jnp.where(eye, matrix, 0.0), axis=0, keepdims=True)
    center = jnp.sum(diagonal, axis=1, keepdims=True) / order
    radius = jnp.sum(jnp.where(eye, 0.0, jnp.abs(matrix)), axis=0, keepdims=True)
    highest = jnp.max(jnp.where(valid, diagonal + radius, -jnp.inf), axis=1, keepdims=True)
    lowest = jnp.min(jnp.where(valid, diagonal - radius, jnp.inf), axis=1, keepdims=True)
    factor = jnp.minimum(
        wanted / jnp.maximum(highest - center, 1e-06),
        (order - wanted) / jnp.maximum(center - lowest, 1e-06),
    )
    ones = jnp.where(eye, 1.0, 0.0)
    initial = factor / order * (center * ones - matrix) + wanted / order * ones

    def purify_step(density):
        square = mul_nn(density, density, 2)
        cube = mul_nn(square, density, 2)
        gap = density - square
        below = total_of(jnp.where(eye, density, 0.0) - density * density)
        above = total_of(density * gap)
        change = total_of(gap * gap)
        safe = jnp.where(jnp.abs(below) > 1e-12, below, 1.0)
        ratio = jnp.clip(above / safe, 0.0, 1.0)
        high = ratio >= 0.5
        scale = 1.0 / jnp.where(high, jnp.maximum(ratio, 0.5), jnp.maximum(1.0 - ratio, 0.5))
        first = jnp.where(high, 0.0, 1.0 - 2.0 * ratio) * scale
        second = (1.0 + ratio) * scale
        return first * density + second * square - scale * cube, change

    def advance(carry):
        index, _, density = carry
        density, change = purify_step(density)
        return index + 1, change[0, 0], density

    def unsettled(carry):
        return (carry[0] < steps) & (carry[1] > SETTLED)

    return lax.while_loop(unsettled, advance, (0, jnp.float32(1.0), initial))[2]


def ritz(half_stiff, half_mass, wanted, steps, last):
    order = half_stiff.shape[0]
    eye = eye_of(order)
    gram_stiff = half_stiff + transposed(half_stiff)
    gram_mass = half_mass + transposed(half_mass)
    picked = jnp.where(eye, gram_mass, 0.0)
    scale_col = lax.rsqrt(jnp.sum(picked, axis=1, keepdims=True) + 1e-06)
    scale_row = lax.rsqrt(jnp.sum(picked, axis=0, keepdims=True) + 1e-06)
    stiff = scale_col * gram_stiff * scale_row
    mass = scale_col * gram_mass * scale_row
    ones = jnp.where(eye, 1.0, 0.0)
    if order == wanted:
        inverse_low = eliminate(mass, ones, 0)
    else:
        known = lane_of((1, LANES)) < wanted
        pivots = jnp.where(known, jnp.sum(jnp.where(eye, mass, 0.0), axis=0, keepdims=True), 1.0)
        ratio = jnp.where(known, mass[wanted:], 0.0) / pivots
        rest = jnp.where(known, 0.0, mass[wanted:] - mul_nn(ratio, mass[:wanted], 3))
        inverse_low = jnp.concatenate(
            [ones[:wanted] * lax.rsqrt(pivots), eliminate(rest, ones[wanted:] - ratio, wanted)], axis=0
        )
    reduced = mul_nt(mul_nn(inverse_low, stiff, 3), inverse_low, 3)
    reduced = 0.5 * (reduced + transposed(reduced))
    if order == wanted:
        return inverse_low * scale_row, reduced, gram_stiff, gram_mass
    columns = purify(reduced, wanted, steps)[:wanted]
    columns = eliminate(mul_nt(columns, columns, 3), columns, 0)
    coefficients = mul_nn(columns, inverse_low, 3) * scale_row
    if last:
        return coefficients, None, gram_stiff, gram_mass
    projected = mul_nt(mul_nn(columns, reduced, 3), columns, 3)
    return coefficients, 0.5 * (projected + transposed(projected)), gram_stiff, gram_mass


def halves_next(coefficients, projected, gram_stiff, gram_mass):
    order = gram_stiff.shape[0]
    wanted = coefficients.shape[0]
    lane = lane_of((wanted, LANES))
    first = lane < wanted
    stiff_top = jnp.where(first, 0.5 * projected, 0.0)
    mass_top = jnp.where(eye_of(wanted), 0.5, 0.0)
    blank = jnp.zeros((wanted, LANES), F32)
    if order == wanted:
        return jnp.concatenate([stiff_top, blank], axis=0), jnp.concatenate([mass_top, blank], axis=0)
    later = jnp.where(first, 0.0, coefficients)
    both = jnp.concatenate([mul_nn(later, gram_stiff, 3), mul_nn(later, gram_mass, 3)], axis=0)
    crossed = mul_nt(both, jnp.concatenate([coefficients, later], axis=0), 3)
    moved = pltpu.roll(crossed, wanted, 1)
    lane = lane_of((2 * wanted, LANES))
    tail = jnp.where((lane >= 2 * wanted) & (lane < 3 * wanted), 0.5 * moved, 0.0)
    crossed = jnp.where(lane < wanted, crossed, tail)
    return (
        jnp.concatenate([stiff_top, blank, crossed[:wanted]], axis=0),
        jnp.concatenate([mass_top, blank, crossed[wanted:]], axis=0),
    )


def odd_lanes(rows):
    return (lane_of((rows, LANES)) // MODES) % 2 == 1


def pack_gram(gram):
    rows = gram.shape[0]
    gram = jnp.where(odd_lanes(rows), gram, 0.0)
    if rows <= 2 * MODES:
        return gram
    top = gram[:MODES] + pltpu.roll(gram[2 * MODES :], MODES, 1)
    return jnp.concatenate([top, gram[MODES : 2 * MODES]], axis=0)


def unpack_gram(packed, order):
    if order > 2 * MODES:
        packed = jnp.concatenate([packed, pltpu.roll(packed[:MODES], LANES - MODES, 1)], axis=0)
    return jnp.where(odd_lanes(order), packed, 0.0)


def halves_now(parts, known, order):
    total = parts[0][...]
    for part in parts[1:]:
        total = total + part[...]
    total = unpack_gram(total, order)
    if order == MODES:
        first = lane_of((MODES, LANES)) < MODES
        stiff = jnp.where(first, 0.5 * pltpu.roll(total, LANES - MODES, 1), 0.0)
        mass = jnp.where(first, 0.5 * pltpu.roll(total, MODES, 1), 0.0)
        return stiff, mass
    row = row_of((order, LANES))
    lane = lane_of((order, LANES))
    total = total * jnp.where((row >= MODES) & (row < 2 * MODES), 0.5, 1.0)
    inside = (lane >= MODES) & (lane < 2 * MODES)
    stiff = known[0][...] + jnp.where(inside, total, 0.0)
    mass = known[1][...] + jnp.where(inside, pltpu.roll(total, LANES // 2, 1), 0.0)
    return stiff, mass


def stiffness_apply(split_ref, out_ref, offsets_ref, first, last, pairs_of):
    width = split_ref.shape[1] // (offsets_ref.shape[0] + REACH)
    slots = offsets_ref.shape[1]

    def block_step(block, carry):
        here = pl.ds(pl.multiple_of((block + REACH) * width, width), width)
        mine = split_ref[:, here]
        pairs = pairs_of(block)
        own = fold(dot_nn(mine, jnp.concatenate(pairs[0], axis=1)))
        spread = []
        for slot in range(slots):
            back = block + REACH - offsets_ref[block, slot]
            there = pl.ds(pl.multiple_of(back * width, width), width)
            across, down = pairs[2 * slot + 1], pairs[2 * slot + 2]
            own = own + fold(dot_nn(split_ref[:, there], jnp.concatenate(down, axis=1)))
            spread.append((there, fold(dot_nn(mine, jnp.concatenate(across, axis=1)))))
        out_ref[:, here] += own
        for there, product in spread:
            out_ref[:, there] += product
        return carry

    lax.fori_loop(first, last, block_step, 0)


def loaded_pairs(pairs_ref):
    slots = pairs_ref.shape[1]
    return lambda block: [[pairs_ref[block, slot, 0], pairs_ref[block, slot, 1]] for slot in range(slots)]


def stacked(value, width):
    count = value.shape[1] // width
    return jnp.concatenate([value[:, width * i : width * (i + 1)] for i in range(count)], axis=0)


def unstacked(value, count):
    rows = value.shape[0] // count
    return jnp.concatenate([value[rows * i : rows * (i + 1)] for i in range(count)], axis=1)


def send_edges(gram, behind, ahead, even, gram_ref, near_ref, far_ref):
    behind, ahead = stacked(behind, LANES), stacked(ahead, LANES)
    rows = gram.shape[0]
    gram_ref[...] = gram
    near_ref[:rows, :] = gram
    near_ref[rows:, :] = jnp.where(even, ahead, behind)
    far_ref[...] = jnp.where(even, behind, ahead)


def received_edges(near_ref, far_ref, even):
    far = far_ref[...]
    near = near_ref[near_ref.shape[0] - far.shape[0] :, :]
    ahead, behind = jnp.where(even, far, near), jnp.where(even, near, far)
    return unstacked(ahead, REACH), unstacked(behind, REACH)


def split_store(split_ref, at, value):
    rows = value.shape[0]
    high, low = pieces(value, 2)
    split_ref[:rows, at] = high
    split_ref[rows:, at] = low


def gram_of(basis_refs, vectors_ref, stiff_ref, mass):
    halo = stiff_ref.shape[1] - mass.shape[1]
    weighted = jnp.concatenate(
        [jnp.zeros((MODES, halo), F32), vectors_ref[:, halo:] * mass], axis=1
    )
    stiff_high, stiff_low = pieces(stiff_ref[...], 2)
    mass_high, mass_low = pieces(weighted, 2)
    right = jnp.concatenate([stiff_low, stiff_high, mass_low, mass_high], axis=0)
    basis = [pieces(ref[...], 2) for ref in basis_refs]
    left = jnp.concatenate([pair[0] for pair in basis] + [pair[1] for pair in basis], axis=0)
    out = dot_nt(left, right)
    rows = left.shape[0] // 2
    out = out[:rows] + out[rows:]
    return pack_gram(out + pltpu.roll(out, MODES, 1))


def first_kernel(
    modes_hbm, diag_hbm, coupling_hbm, edge_ref, mass_ref, parity_ref, offsets_ref,
    basis_ref, stiff_ref, gram_ref, near_ref, far_ref, inverse_ref, pairs_ref,
    split_ref, modes_ref, diag_ref, coupling_ref, semaphores,
):
    halo = edge_ref.shape[1]
    count, width = diag_ref.shape[0], diag_ref.shape[1]
    groups = semaphores.shape[0] // 2
    size = count // groups
    copies = [pltpu.make_async_copy(modes_hbm, modes_ref, semaphores.at[2 * groups])]
    for group in range(groups):
        at = pl.ds(group * size, size)
        copies.append(pltpu.make_async_copy(diag_hbm.at[at], diag_ref.at[at], semaphores.at[2 * group]))
        copies.append(
            pltpu.make_async_copy(coupling_hbm.at[at], coupling_ref.at[at], semaphores.at[2 * group + 1])
        )
    for copy in copies:
        copy.start()
    diagonal = lax.broadcasted_iota(jnp.int32, (width, width), 0) == lax.broadcasted_iota(
        jnp.int32, (width, width), 1
    )

    def pairs_of(block):
        pairs = [pieces(jnp.where(diagonal, 0.0, diag_ref[block]), 2)]
        for slot in range(coupling_ref.shape[1]):
            pair = pieces(coupling_ref[block, slot], 2)
            pairs += [pair, [part.T for part in pair]]
        for index, pair in enumerate(pairs):
            pairs_ref[block, index, 0] = pair[0]
            pairs_ref[block, index, 1] = pair[1]
        return pairs

    copies[0].wait()
    basis_ref[:, :halo] = edge_ref[...]
    basis_ref[:, halo:] = modes_ref[...]
    split_store(split_ref, slice(None), basis_ref[...])
    stiff_ref[...] = jnp.zeros(stiff_ref.shape, F32)
    for group in range(groups):
        copies[2 * group + 1].wait()
        copies[2 * group + 2].wait()
        for block in range(group * size, (group + 1) * size):
            at = slice(block * width, (block + 1) * width)
            picked = jnp.sum(jnp.where(diagonal, diag_ref[block], 0.0), axis=0, keepdims=True)
            inverse_ref[:, at] = 1.0 / picked
            stiff_ref[:, halo + block * width : halo + (block + 1) * width] += modes_ref[:, at] * picked
        stiffness_apply(split_ref, stiff_ref, offsets_ref, group * size, (group + 1) * size, pairs_of)
    gram = gram_of([basis_ref], basis_ref, stiff_ref, mass_ref[...])
    extra = near_ref.shape[0] // REACH - MODES - gram.shape[0] // REACH
    start = inverse_ref.shape[1] - halo
    tail = jnp.where(
        row_of((extra, halo)) == 0,
        jnp.broadcast_to(inverse_ref[:, start:], (extra, halo)),
        jnp.broadcast_to(mass_ref[:, start:], (extra, halo)),
    )
    behind = jnp.concatenate([stiff_ref[:, :halo], tail], axis=0)
    ahead = jnp.concatenate([stiff_ref[:, stiff_ref.shape[1] - halo :], tail], axis=0)
    send_edges(gram, behind, ahead, parity_ref[0] == 0, gram_ref, near_ref, far_ref)


def combine(left, right):
    high, low = pieces(right, 2)
    pair = jnp.concatenate(pieces(left, 2), axis=0)
    rows = left.shape[0]
    out = dot_nn(pair, high)
    return out[:rows] + (out[rows:] + dot_nn(left.astype(BF16), low))


def middle_kernel(order, parts_count, *refs):
    refs = list(refs)
    take = lambda count: [refs.pop(0) for _ in range(count)]
    parts = take(parts_count)
    known = take(2) if order > MODES else []
    blocks = order // MODES
    basis = take(blocks)
    stiff = take(blocks)
    near_in, far_in, mass_in, inverse_in, pairs_ref, parity_ref, offsets_ref = take(7)
    out_blocks = min(blocks + 1, 3)
    basis_out = take(out_blocks)
    stiff_out = take(out_blocks)
    gram_ref, near_ref, far_ref, half_stiff_ref, half_mass_ref = take(5)
    mass_ref, inverse_ref = take(2) if order == MODES else (mass_in, inverse_in)
    (split_ref,) = take(1)

    even = parity_ref[0] == 0
    coefficients, projected, gram_stiff, gram_mass = ritz(
        *halves_now(parts, known, order), MODES, PURIFY, False
    )
    halves = halves_next(coefficients, projected, gram_stiff, gram_mass)
    half_stiff_ref[...] = halves[0]
    half_mass_ref[...] = halves[1]
    ahead, behind = received_edges(near_in, far_in, even)
    halo = ahead.shape[1]
    extent = basis[0].shape[1]
    if order == MODES:
        inverse_ref[:, :halo] = ahead[MODES : MODES + 1]
        inverse_ref[:, halo:] = inverse_in[...]
        mass_ref[:, :halo] = ahead[MODES + 1 : MODES + 2]
        mass_ref[:, halo:] = mass_in[...]
    mixing = coefficients[:, :order]
    if order > MODES:
        later = jnp.where(lane_of((MODES, LANES)) < MODES, 0.0, coefficients)
        mixing = jnp.concatenate([mixing, later[:, :order]], axis=0)
    newest = 0 if order == MODES else 1
    for start in range(0, extent, halo):
        at = slice(start, start + halo)
        current = [ref[:, at] for ref in stiff]
        if start == 0:
            current[newest] = current[newest] + ahead[:MODES]
        if start + halo == extent:
            current[newest] = current[newest] + behind[:MODES]
        vectors = combine(mixing, jnp.concatenate([ref[:, at] for ref in basis], axis=0))
        images = combine(mixing, jnp.concatenate(current, axis=0))
        modes, stiff_modes = vectors[:MODES], images[:MODES]
        basis_out[0][:, at] = modes
        stiff_out[0][:, at] = stiff_modes
        if order > MODES:
            basis_out[2][:, at] = vectors[MODES:]
            stiff_out[2][:, at] = images[MODES:]
        residual = stiff_modes - combine(projected[:, :MODES], modes * mass_ref[:, at])
        precond = residual * inverse_ref[:, at]
        basis_out[1][:, at] = precond
        split_store(split_ref, at, precond)
        stiff_out[1][:, at] = jnp.zeros((MODES, halo), F32) if start == 0 else residual
    stiffness_apply(split_ref, stiff_out[1], offsets_ref, 0, offsets_ref.shape[0], loaded_pairs(pairs_ref))
    gram = gram_of(basis_out, basis_out[1], stiff_out[1], mass_ref[:, halo:])
    newest = stiff_out[1]
    send_edges(gram, newest[:, :halo], newest[:, extent - halo :], even, gram_ref, near_ref, far_ref)


def last_kernel(order, parts_count, weight, *refs):
    refs = list(refs)
    take = lambda count: [refs.pop(0) for _ in range(count)]
    parts = take(parts_count)
    known = take(2)
    blocks = order // MODES
    basis = take(blocks)
    stiff = take(blocks)
    near_in, far_in, mass_ref, parity_ref = take(4)
    mass_out, energy_out = take(2)
    coefficients = ritz(*halves_now(parts, known, order), MODES, PURIFY, True)[0]
    behind = received_edges(near_in, far_in, parity_ref[0] == 0)[1]
    halo = behind.shape[1]
    extent = mass_ref.shape[1]
    mixing = coefficients[:, :order]
    for start in range(halo, extent, halo):
        at = slice(start, start + halo)
        to = slice(start - halo, start)
        current = [ref[:, at] for ref in stiff]
        if start + halo == extent:
            current[1] = current[1] + behind
        vectors = combine(mixing, jnp.concatenate([ref[:, at] for ref in basis], axis=0))
        images = combine(mixing, jnp.concatenate(current, axis=0))
        mass_out[:, to] = weight * mass_ref[:, at] * jnp.sum(vectors * vectors, axis=0, keepdims=True)
        energy_out[:, to] = weight * jnp.sum(vectors * images, axis=0, keepdims=True)


def call(kernel, args, outs, scratch, flops, spaces=()):
    spaces = list(spaces) + [pltpu.VMEM] * (len(args) - len(spaces))
    spaces = [pltpu.SMEM if arg.dtype == jnp.int32 else space for arg, space in zip(args, spaces)]
    return pl.pallas_call(
        kernel,
        out_shape=[
            jax.ShapeDtypeStruct(shape, BF16 if len(shape) > 2 else F32) for shape in outs
        ],
        in_specs=[pl.BlockSpec(memory_space=space) for space in spaces],
        out_specs=[pl.BlockSpec(memory_space=pltpu.VMEM)] * len(outs),
        scratch_shapes=scratch,
        compiler_params=pltpu.CompilerParams(vmem_limit_bytes=24 << 20),
        cost_estimate=pl.CostEstimate(flops=flops, bytes_accessed=1 << 20, transcendentals=0),
    )(*args)


def hbm(value):
    return pltpu.with_memory_space_constraint(value, pltpu.HBM)


def exchange(gram, near, far, axis):
    count = lax.axis_size(axis)
    across = lambda value, mask: lax.ppermute(
        value, axis, [(at, at ^ mask) for at in range(count) if at ^ mask < count]
    )
    near = across(near, 1)
    if count & (count - 1):
        parts = [lax.psum(gram, axis)]
    else:
        parts, stride = [gram], 1
        while stride < count:
            if len(parts) > 1:
                gram = sum(parts[1:], parts[0])
            masks = [stride, 2 * stride, 3 * stride] if 4 * stride <= count else [stride]
            parts = [gram] + [
                near[: gram.shape[0]] if mask == 1 else across(gram, mask) for mask in masks
            ]
            stride *= 1 << len(masks).bit_length()
    hops = [(at, at + 1 if at % 2 else at - 1) for at in range(count)]
    far = lax.ppermute(far, axis, [hop for hop in hops if 0 <= hop[1] < count])
    return parts, near, far


def local(diag_blocks, coupling, offsets, mass, initial_modes):
    count, width = diag_blocks.shape[0], diag_blocks.shape[1]
    slots = coupling.shape[1]
    own = count * width
    halo = REACH * width
    extent = own + halo
    split = [pltpu.VMEM((2 * MODES, extent), BF16)]
    parity = (lax.axis_index("row") % 2).astype(jnp.int32).reshape(1)
    mass = mass.reshape(1, own)
    spare = 8
    ranks = lax.axis_size("row")
    edge = lax.ppermute(initial_modes[:, own - halo :], "row", [(at, at + 1) for at in range(ranks - 1)])
    edge_rows = REACH * (MODES + spare)
    groups = 4 if count % 4 == 0 else 1
    vectors, stiff, gram, near, far, inverse, pairs = call(
        first_kernel,
        [hbm(initial_modes), hbm(diag_blocks), hbm(coupling), edge, mass, parity, offsets],
        [
            (MODES, extent), (MODES, extent), (MODES, LANES), (MODES + edge_rows, LANES),
            (edge_rows, LANES), (1, own), (count, 2 * slots + 1, 2, width, width),
        ],
        split
        + [
            pltpu.VMEM((MODES, own), F32),
            pltpu.VMEM((count, width, width), F32),
            pltpu.VMEM((count, slots, width, width), F32),
            pltpu.SemaphoreType.DMA((2 * groups + 1,)),
        ],
        1 << 30,
        [pltpu.HBM] * 3,
    )
    edge_rows = REACH * MODES
    basis, images, known = [vectors], [stiff], []
    for iteration in range(ITERS):
        parts, near, far = exchange(gram, near, far, "row")
        order = MODES * len(basis)
        out_blocks = min(len(basis) + 1, 3)
        wide = [(MODES, extent)] * out_blocks
        packed = min(out_blocks, 2) * MODES
        halves = [(out_blocks * MODES, LANES)] * 2
        outs = call(
            functools.partial(middle_kernel, order, len(parts)),
            [*parts, *known, *basis, *images, near, far, mass, inverse, pairs, parity, offsets],
            [
                *wide, *wide, (packed, LANES), (packed + edge_rows, LANES), (edge_rows, LANES), *halves,
                *([(1, extent)] * 2 if order == MODES else []),
            ],
            split,
            1 << 31,
        )
        basis = outs[:out_blocks]
        images = outs[out_blocks : 2 * out_blocks]
        gram, near, far = outs[2 * out_blocks : 2 * out_blocks + 3]
        known = outs[2 * out_blocks + 3 : 2 * out_blocks + 5]
        if order == MODES:
            mass, inverse = outs[-2:]
    parts, near, far = exchange(gram, near, far, "row")
    weight = own * ranks / MODES
    outs = call(
        functools.partial(last_kernel, MODES * len(basis), len(parts), weight),
        [*parts, *known, *basis, *images, near, far, mass, parity],
        [(1, own), (1, own)],
        [],
        1 << 31,
    )
    return outs[0].reshape(own), outs[1].reshape(own)


def solution(mesh):
    placed = (
        P(("sub", "row"), None, None),
        P(("sub", "row"), None, None, None),
        P(("sub", "row"), None),
        P(("sub", "row")),
        P(None, ("sub", "row")),
    )
    return jax.shard_map(
        local,
        mesh=mesh,
        in_specs=placed,
        out_specs=(P(("sub", "row")), P(("sub", "row"))),
        check_vma=False,
    )
```

```python
import functools

import jax
import jax.numpy as jnp
from jax import lax
from jax.experimental import pallas as pl
from jax.experimental.pallas import tpu as pltpu
from jax.sharding import PartitionSpec as P

MODES = 32
REACH = 4
ITERS = 3
PURIFY = 28
LANES = 128
SETTLED = 1e-8
PANEL = 16
F32 = jnp.float32
BF16 = jnp.bfloat16


def pieces(value, count):
    parts = []
    for index in range(count):
        part = value.astype(BF16)
        parts.append(part)
        if index + 1 < count:
            value = value - part.astype(F32)
    return parts


def dot_nn(left, right):
    return lax.dot_general(left, right, (((1,), (0,)), ((), ())), preferred_element_type=F32)


def dot_nt(left, right):
    return lax.dot_general(left, right, (((1,), (1,)), ((), ())), preferred_element_type=F32)


def pad_rows(value):
    short = LANES - value.shape[0]
    if short == 0:
        return value
    return jnp.concatenate([value, jnp.zeros((short, value.shape[1]), value.dtype)], axis=0)


def transposed(value):
    return pad_rows(value).T[: value.shape[0]]


def fold(out):
    rows, width = out.shape[0] // 2, out.shape[1] // 2
    out = out[:rows] + out[rows:]
    return out[:, :width] + out[:, width:]


def mul_nn(left, right):
    right = [pad_rows(part) for part in pieces(right, 2)]
    return fold(dot_nn(jnp.concatenate(pieces(left, 2), axis=0), jnp.concatenate(right, axis=1)))


def mul_nt(left, right):
    right = [pad_rows(part) for part in pieces(right, 2)]
    return fold(dot_nt(jnp.concatenate(pieces(left, 2), axis=0), jnp.concatenate(right, axis=0)))


def lane_of(shape):
    return lax.broadcasted_iota(jnp.int32, shape, 1)


def row_of(shape):
    return lax.broadcasted_iota(jnp.int32, shape, 0)


def eye_of(rows, lead=0):
    shape = (rows, LANES)
    return lane_of(shape) == row_of(shape) + lead


def eliminate(matrix, other, lead):
    order = matrix.shape[0]
    tiles = order // 8
    a = [matrix[8 * i : 8 * i + 8] for i in range(tiles)]
    e = [other[8 * i : 8 * i + 8] for i in range(tiles)]
    sub = row_of((8, LANES))
    for start in range(0, order, PANEL):
        columns = [
            {
                i: jnp.broadcast_to(a[i][:, lead + start + k : lead + start + k + 1], (8, LANES))
                for i in range(start // 8, tiles)
            }
            for k in range(PANEL)
        ]
        for step in range(PANEL):
            kt, k = (start + step) // 8, step % 8
            below = range(kt, tiles)
            head = lambda tile: jnp.broadcast_to(tile[k : k + 1, :], (8, LANES))
            pivot = head(columns[step][kt])
            inverse = 1.0 / pivot
            ratios = {i: columns[step][i] * inverse for i in below}
            ratios[kt] = jnp.where(sub > k, ratios[kt], 0.0)
            for later in range(step + 1, PANEL):
                top = head(columns[later][kt])
                for i in below:
                    columns[later][i] = columns[later][i] - ratios[i] * top
            row_a, row_e = head(a[kt]), head(e[kt])
            for i in below:
                a[i] = a[i] - ratios[i] * row_a
                e[i] = e[i] - ratios[i] * row_e
            e[kt] = jnp.where(sub == k, e[kt] * lax.rsqrt(pivot), e[kt])
    return jnp.concatenate(e, axis=0)


def total_of(value):
    return jnp.sum(jnp.sum(value, axis=0, keepdims=True), axis=1, keepdims=True)


def purify(matrix, wanted, steps):
    order = matrix.shape[0]
    eye = eye_of(order)
    valid = lane_of((1, LANES)) < order
    diagonal = jnp.sum(jnp.where(eye, matrix, 0.0), axis=0, keepdims=True)
    center = jnp.sum(diagonal, axis=1, keepdims=True) / order
    radius = jnp.sum(jnp.where(eye, 0.0, jnp.abs(matrix)), axis=0, keepdims=True)
    highest = jnp.max(jnp.where(valid, diagonal + radius, -jnp.inf), axis=1, keepdims=True)
    lowest = jnp.min(jnp.where(valid, diagonal - radius, jnp.inf), axis=1, keepdims=True)
    factor = jnp.minimum(
        wanted / jnp.maximum(highest - center, 1e-06),
        (order - wanted) / jnp.maximum(center - lowest, 1e-06),
    )
    ones = jnp.where(eye, 1.0, 0.0)
    initial = factor / order * (center * ones - matrix) + wanted / order * ones

    def purify_step(density):
        square = mul_nn(density, density)
        cube = mul_nn(square, density)
        gap = density - square
        below = total_of(jnp.where(eye, density, 0.0) - density * density)
        above = total_of(density * gap)
        change = total_of(gap * gap)
        safe = jnp.where(jnp.abs(below) > 1e-12, below, 1.0)
        ratio = jnp.clip(above / safe, 0.0, 1.0)
        high = ratio >= 0.5
        scale = 1.0 / jnp.where(high, jnp.maximum(ratio, 0.5), jnp.maximum(1.0 - ratio, 0.5))
        first = jnp.where(high, 0.0, 1.0 - 2.0 * ratio) * scale
        second = (1.0 + ratio) * scale
        return first * density + second * square - scale * cube, change

    def advance(carry):
        index, _, density = carry
        density, change = purify_step(density)
        return index + 1, change[0, 0], density

    def unsettled(carry):
        return (carry[0] < steps) & (carry[1] > SETTLED)

    return lax.while_loop(unsettled, advance, (0, jnp.float32(1.0), initial))[2]


def ritz(half_stiff, half_mass, wanted, steps, last):
    order = half_stiff.shape[0]
    eye = eye_of(order)
    gram_stiff = half_stiff + transposed(half_stiff)
    gram_mass = half_mass + transposed(half_mass)
    picked = jnp.where(eye, gram_mass, 0.0)
    scale_col = lax.rsqrt(jnp.sum(picked, axis=1, keepdims=True) + 1e-06)
    scale_row = lax.rsqrt(jnp.sum(picked, axis=0, keepdims=True) + 1e-06)
    stiff = scale_col * gram_stiff * scale_row
    mass = scale_col * gram_mass * scale_row
    ones = jnp.where(eye, 1.0, 0.0)
    if order == wanted:
        inverse_low = eliminate(mass, ones, 0)
    else:
        known = lane_of((1, LANES)) < wanted
        pivots = jnp.where(known, jnp.sum(jnp.where(eye, mass, 0.0), axis=0, keepdims=True), 1.0)
        ratio = jnp.where(known, mass[wanted:], 0.0) / pivots
        rest = jnp.where(known, 0.0, mass[wanted:] - mul_nn(ratio, mass[:wanted]))
        inverse_low = jnp.concatenate(
            [ones[:wanted] * lax.rsqrt(pivots), eliminate(rest, ones[wanted:] - ratio, wanted)], axis=0
        )
    reduced = mul_nt(mul_nn(inverse_low, stiff), inverse_low)
    reduced = 0.5 * (reduced + transposed(reduced))
    if order == wanted:
        return inverse_low * scale_row, reduced, gram_stiff, gram_mass
    columns = purify(reduced, wanted, steps)[:wanted]
    columns = eliminate(mul_nt(columns, columns), columns, 0)
    coefficients = mul_nn(columns, inverse_low) * scale_row
    if last:
        return coefficients, None, gram_stiff, gram_mass
    projected = mul_nt(mul_nn(columns, reduced), columns)
    return coefficients, 0.5 * (projected + transposed(projected)), gram_stiff, gram_mass


def halves_next(coefficients, projected, gram_stiff, gram_mass):
    order = gram_stiff.shape[0]
    wanted = coefficients.shape[0]
    lane = lane_of((wanted, LANES))
    first = lane < wanted
    stiff_top = jnp.where(first, 0.5 * projected, 0.0)
    mass_top = jnp.where(eye_of(wanted), 0.5, 0.0)
    blank = jnp.zeros((wanted, LANES), F32)
    if order == wanted:
        return jnp.concatenate([stiff_top, blank], axis=0), jnp.concatenate([mass_top, blank], axis=0)
    later = jnp.where(first, 0.0, coefficients)
    both = jnp.concatenate([mul_nn(later, gram_stiff), mul_nn(later, gram_mass)], axis=0)
    crossed = mul_nt(both, jnp.concatenate([coefficients, later], axis=0))
    moved = pltpu.roll(crossed, wanted, 1)
    lane = lane_of((2 * wanted, LANES))
    tail = jnp.where((lane >= 2 * wanted) & (lane < 3 * wanted), 0.5 * moved, 0.0)
    crossed = jnp.where(lane < wanted, crossed, tail)
    return (
        jnp.concatenate([stiff_top, blank, crossed[:wanted]], axis=0),
        jnp.concatenate([mass_top, blank, crossed[wanted:]], axis=0),
    )


def odd_lanes(rows):
    return (lane_of((rows, LANES)) // MODES) % 2 == 1


def pack_gram(gram):
    rows = gram.shape[0]
    gram = jnp.where(odd_lanes(rows), gram, 0.0)
    if rows <= 2 * MODES:
        return gram
    top = gram[:MODES] + pltpu.roll(gram[2 * MODES :], MODES, 1)
    return jnp.concatenate([top, gram[MODES : 2 * MODES]], axis=0)


def unpack_gram(packed, order):
    if order > 2 * MODES:
        packed = jnp.concatenate([packed, pltpu.roll(packed[:MODES], LANES - MODES, 1)], axis=0)
    return jnp.where(odd_lanes(order), packed, 0.0)


def halves_now(parts, known, order):
    total = parts[0][...]
    for part in parts[1:]:
        total = total + part[...]
    total = unpack_gram(total, order)
    if order == MODES:
        first = lane_of((MODES, LANES)) < MODES
        stiff = jnp.where(first, 0.5 * pltpu.roll(total, LANES - MODES, 1), 0.0)
        mass = jnp.where(first, 0.5 * pltpu.roll(total, MODES, 1), 0.0)
        return stiff, mass
    row = row_of((order, LANES))
    lane = lane_of((order, LANES))
    total = total * jnp.where((row >= MODES) & (row < 2 * MODES), 0.5, 1.0)
    inside = (lane >= MODES) & (lane < 2 * MODES)
    stiff = known[0][...] + jnp.where(inside, total, 0.0)
    mass = known[1][...] + jnp.where(inside, pltpu.roll(total, LANES // 2, 1), 0.0)
    return stiff, mass


def stiffness_apply(split_ref, out_ref, offsets_ref, first, last, pairs_of):
    width = split_ref.shape[1] // (offsets_ref.shape[0] + REACH)
    slots = offsets_ref.shape[1]

    def block_step(block, carry):
        here = pl.ds(pl.multiple_of((block + REACH) * width, width), width)
        mine = split_ref[:, here]
        pairs = pairs_of(block)
        own = fold(dot_nn(mine, jnp.concatenate(pairs[0], axis=1)))
        spread = []
        for slot in range(slots):
            back = block + REACH - offsets_ref[block, slot]
            there = pl.ds(pl.multiple_of(back * width, width), width)
            across, down = pairs[2 * slot + 1], pairs[2 * slot + 2]
            own = own + fold(dot_nn(split_ref[:, there], jnp.concatenate(down, axis=1)))
            spread.append((there, fold(dot_nn(mine, jnp.concatenate(across, axis=1)))))
        out_ref[:, here] += own
        for there, product in spread:
            out_ref[:, there] += product
        return carry

    lax.fori_loop(first, last, block_step, 0)


def loaded_pairs(pairs_ref):
    slots = pairs_ref.shape[1]
    return lambda block: [[pairs_ref[block, slot, 0], pairs_ref[block, slot, 1]] for slot in range(slots)]


def stacked(value, width):
    count = value.shape[1] // width
    return jnp.concatenate([value[:, width * i : width * (i + 1)] for i in range(count)], axis=0)


def unstacked(value, count):
    rows = value.shape[0] // count
    return jnp.concatenate([value[rows * i : rows * (i + 1)] for i in range(count)], axis=1)


def send_edges(gram, behind, ahead, even, gram_ref, near_ref, far_ref):
    behind, ahead = stacked(behind, LANES), stacked(ahead, LANES)
    rows = gram.shape[0]
    gram_ref[...] = gram
    near_ref[:rows, :] = gram
    near_ref[rows:, :] = jnp.where(even, ahead, behind)
    far_ref[...] = jnp.where(even, behind, ahead)


def received_edges(near_ref, far_ref, even):
    far = far_ref[...]
    near = near_ref[near_ref.shape[0] - far.shape[0] :, :]
    ahead, behind = jnp.where(even, far, near), jnp.where(even, near, far)
    return unstacked(ahead, REACH), unstacked(behind, REACH)


def split_store(split_ref, at, value):
    rows = value.shape[0]
    high, low = pieces(value, 2)
    split_ref[:rows, at] = high
    split_ref[rows:, at] = low


def gram_of(basis_refs, vectors_ref, stiff_ref, mass):
    halo = stiff_ref.shape[1] - mass.shape[1]
    weighted = jnp.concatenate(
        [jnp.zeros((MODES, halo), F32), vectors_ref[:, halo:] * mass], axis=1
    )
    stiff_high, stiff_low = pieces(stiff_ref[...], 2)
    mass_high, mass_low = pieces(weighted, 2)
    right = jnp.concatenate([stiff_low, stiff_high, mass_low, mass_high], axis=0)
    basis = [pieces(ref[...], 2) for ref in basis_refs]
    left = jnp.concatenate([pair[0] for pair in basis] + [pair[1] for pair in basis], axis=0)
    out = dot_nt(left, right)
    rows = left.shape[0] // 2
    out = out[:rows] + out[rows:]
    return pack_gram(out + pltpu.roll(out, MODES, 1))


def first_kernel(
    modes_hbm, diag_hbm, coupling_hbm, edge_ref, mass_ref, parity_ref, offsets_ref,
    basis_ref, stiff_ref, gram_ref, near_ref, far_ref, inverse_ref, pairs_ref,
    split_ref, modes_ref, diag_ref, coupling_ref, semaphores,
):
    halo = edge_ref.shape[1]
    count, width = diag_ref.shape[0], diag_ref.shape[1]
    groups = semaphores.shape[0] // 2
    size = count // groups
    copies = [pltpu.make_async_copy(modes_hbm, modes_ref, semaphores.at[2 * groups])]
    for group in range(groups):
        at = pl.ds(group * size, size)
        copies.append(pltpu.make_async_copy(diag_hbm.at[at], diag_ref.at[at], semaphores.at[2 * group]))
        copies.append(
            pltpu.make_async_copy(coupling_hbm.at[at], coupling_ref.at[at], semaphores.at[2 * group + 1])
        )
    for copy in copies:
        copy.start()
    diagonal = lax.broadcasted_iota(jnp.int32, (width, width), 0) == lax.broadcasted_iota(
        jnp.int32, (width, width), 1
    )

    def pairs_of(block):
        pairs = [pieces(jnp.where(diagonal, 0.0, diag_ref[block]), 2)]
        for slot in range(coupling_ref.shape[1]):
            pair = pieces(coupling_ref[block, slot], 2)
            pairs += [pair, [part.T for part in pair]]
        for index, pair in enumerate(pairs):
            pairs_ref[block, index, 0] = pair[0]
            pairs_ref[block, index, 1] = pair[1]
        return pairs

    copies[0].wait()
    basis_ref[:, :halo] = edge_ref[...]
    basis_ref[:, halo:] = modes_ref[...]
    split_store(split_ref, slice(None), basis_ref[...])
    stiff_ref[...] = jnp.zeros(stiff_ref.shape, F32)
    for group in range(groups):
        copies[2 * group + 1].wait()
        copies[2 * group + 2].wait()
        for block in range(group * size, (group + 1) * size):
            at = slice(block * width, (block + 1) * width)
            picked = jnp.sum(jnp.where(diagonal, diag_ref[block], 0.0), axis=0, keepdims=True)
            inverse_ref[:, at] = 1.0 / picked
            stiff_ref[:, halo + block * width : halo + (block + 1) * width] += modes_ref[:, at] * picked
        stiffness_apply(split_ref, stiff_ref, offsets_ref, group * size, (group + 1) * size, pairs_of)
    gram = gram_of([basis_ref], basis_ref, stiff_ref, mass_ref[...])
    extra = near_ref.shape[0] // REACH - MODES - gram.shape[0] // REACH
    start = inverse_ref.shape[1] - halo
    tail = jnp.where(
        row_of((extra, halo)) == 0,
        jnp.broadcast_to(inverse_ref[:, start:], (extra, halo)),
        jnp.broadcast_to(mass_ref[:, start:], (extra, halo)),
    )
    behind = jnp.concatenate([stiff_ref[:, :halo], tail], axis=0)
    ahead = jnp.concatenate([stiff_ref[:, stiff_ref.shape[1] - halo :], tail], axis=0)
    send_edges(gram, behind, ahead, parity_ref[0] == 0, gram_ref, near_ref, far_ref)


def doubled(left):
    return jnp.concatenate([jnp.concatenate([part, part], axis=1) for part in pieces(left, 2)], axis=0)


def combine(left, right):
    out = dot_nn(left, jnp.concatenate(pieces(right, 2), axis=0))
    rows = left.shape[0] // 2
    return out[:rows] + out[rows:]


def middle_kernel(order, parts_count, *refs):
    refs = list(refs)
    take = lambda count: [refs.pop(0) for _ in range(count)]
    parts = take(parts_count)
    known = take(2) if order > MODES else []
    blocks = order // MODES
    basis = take(blocks)
    stiff = take(blocks)
    near_in, far_in, mass_in, inverse_in, pairs_ref, parity_ref, offsets_ref = take(7)
    out_blocks = min(blocks + 1, 3)
    basis_out = take(out_blocks)
    stiff_out = take(out_blocks)
    gram_ref, near_ref, far_ref, half_stiff_ref, half_mass_ref = take(5)
    mass_ref, inverse_ref = take(2) if order == MODES else (mass_in, inverse_in)
    (split_ref,) = take(1)

    even = parity_ref[0] == 0
    coefficients, projected, gram_stiff, gram_mass = ritz(
        *halves_now(parts, known, order), MODES, PURIFY, False
    )
    halves = halves_next(coefficients, projected, gram_stiff, gram_mass)
    half_stiff_ref[...] = halves[0]
    half_mass_ref[...] = halves[1]
    ahead, behind = received_edges(near_in, far_in, even)
    halo = ahead.shape[1]
    extent = basis[0].shape[1]
    if order == MODES:
        inverse_ref[:, :halo] = ahead[MODES : MODES + 1]
        inverse_ref[:, halo:] = inverse_in[...]
        mass_ref[:, :halo] = ahead[MODES + 1 : MODES + 2]
        mass_ref[:, halo:] = mass_in[...]
    mixing = coefficients[:, :order]
    if order > MODES:
        later = jnp.where(lane_of((MODES, LANES)) < MODES, 0.0, coefficients)
        mixing = jnp.concatenate([mixing, later[:, :order]], axis=0)
    mixing = doubled(mixing)
    pulling = doubled(projected[:, :MODES])
    newest = 0 if order == MODES else 1
    for start in range(0, extent, halo):
        at = slice(start, start + halo)
        current = [ref[:, at] for ref in stiff]
        if start == 0:
            current[newest] = current[newest] + ahead[:MODES]
        if start + halo == extent:
            current[newest] = current[newest] + behind[:MODES]
        vectors = combine(mixing, jnp.concatenate([ref[:, at] for ref in basis], axis=0))
        images = combine(mixing, jnp.concatenate(current, axis=0))
        modes, stiff_modes = vectors[:MODES], images[:MODES]
        basis_out[0][:, at] = modes
        stiff_out[0][:, at] = stiff_modes
        if order > MODES:
            basis_out[2][:, at] = vectors[MODES:]
            stiff_out[2][:, at] = images[MODES:]
        residual = stiff_modes - combine(pulling, modes * mass_ref[:, at])
        precond = residual * inverse_ref[:, at]
        basis_out[1][:, at] = precond
        split_store(split_ref, at, precond)
        stiff_out[1][:, at] = jnp.zeros((MODES, halo), F32) if start == 0 else residual
    stiffness_apply(split_ref, stiff_out[1], offsets_ref, 0, offsets_ref.shape[0], loaded_pairs(pairs_ref))
    gram = gram_of(basis_out, basis_out[1], stiff_out[1], mass_ref[:, halo:])
    newest = stiff_out[1]
    send_edges(gram, newest[:, :halo], newest[:, extent - halo :], even, gram_ref, near_ref, far_ref)


def last_kernel(order, parts_count, weight, *refs):
    refs = list(refs)
    take = lambda count: [refs.pop(0) for _ in range(count)]
    parts = take(parts_count)
    known = take(2)
    blocks = order // MODES
    basis = take(blocks)
    stiff = take(blocks)
    near_in, far_in, mass_ref, parity_ref = take(4)
    mass_out, energy_out = take(2)
    coefficients = ritz(*halves_now(parts, known, order), MODES, PURIFY, True)[0]
    behind = received_edges(near_in, far_in, parity_ref[0] == 0)[1]
    halo = behind.shape[1]
    extent = mass_ref.shape[1]
    mixing = doubled(coefficients[:, :order])
    for start in range(halo, extent, halo):
        at = slice(start, start + halo)
        to = slice(start - halo, start)
        current = [ref[:, at] for ref in stiff]
        if start + halo == extent:
            current[1] = current[1] + behind
        vectors = combine(mixing, jnp.concatenate([ref[:, at] for ref in basis], axis=0))
        images = combine(mixing, jnp.concatenate(current, axis=0))
        mass_out[:, to] = weight * mass_ref[:, at] * jnp.sum(vectors * vectors, axis=0, keepdims=True)
        energy_out[:, to] = weight * jnp.sum(vectors * images, axis=0, keepdims=True)


def call(kernel, args, outs, scratch, flops, spaces=()):
    spaces = list(spaces) + [pltpu.VMEM] * (len(args) - len(spaces))
    spaces = [pltpu.SMEM if arg.dtype == jnp.int32 else space for arg, space in zip(args, spaces)]
    return pl.pallas_call(
        kernel,
        out_shape=[
            jax.ShapeDtypeStruct(shape, BF16 if len(shape) > 2 else F32) for shape in outs
        ],
        in_specs=[pl.BlockSpec(memory_space=space) for space in spaces],
        out_specs=[pl.BlockSpec(memory_space=pltpu.VMEM)] * len(outs),
        scratch_shapes=scratch,
        compiler_params=pltpu.CompilerParams(vmem_limit_bytes=24 << 20),
        cost_estimate=pl.CostEstimate(flops=flops, bytes_accessed=1 << 20, transcendentals=0),
    )(*args)


def hbm(value):
    return pltpu.with_memory_space_constraint(value, pltpu.HBM)


def exchange(gram, near, far, axis):
    count = lax.axis_size(axis)
    across = lambda value, mask: lax.ppermute(
        value, axis, [(at, at ^ mask) for at in range(count) if at ^ mask < count]
    )
    near = across(near, 1)
    if count & (count - 1):
        parts = [lax.psum(gram, axis)]
    else:
        parts, stride = [gram], 1
        while stride < count:
            if len(parts) > 1:
                gram = sum(parts[1:], parts[0])
            masks = [stride, 2 * stride, 3 * stride] if 4 * stride <= count else [stride]
            parts = [gram] + [
                near[: gram.shape[0]] if mask == 1 else across(gram, mask) for mask in masks
            ]
            stride *= 1 << len(masks).bit_length()
    hops = [(at, at + 1 if at % 2 else at - 1) for at in range(count)]
    far = lax.ppermute(far, axis, [hop for hop in hops if 0 <= hop[1] < count])
    return parts, near, far


def local(diag_blocks, coupling, offsets, mass, initial_modes):
    count, width = diag_blocks.shape[0], diag_blocks.shape[1]
    slots = coupling.shape[1]
    own = count * width
    halo = REACH * width
    extent = own + halo
    split = [pltpu.VMEM((2 * MODES, extent), BF16)]
    parity = (lax.axis_index("row") % 2).astype(jnp.int32).reshape(1)
    mass = mass.reshape(1, own)
    spare = 8
    ranks = lax.axis_size("row")
    edge = lax.ppermute(initial_modes[:, own - halo :], "row", [(at, at + 1) for at in range(ranks - 1)])
    edge_rows = REACH * (MODES + spare)
    groups = 4 if count % 4 == 0 else 1
    vectors, stiff, gram, near, far, inverse, pairs = call(
        first_kernel,
        [hbm(initial_modes), hbm(diag_blocks), hbm(coupling), edge, mass, parity, offsets],
        [
            (MODES, extent), (MODES, extent), (MODES, LANES), (MODES + edge_rows, LANES),
            (edge_rows, LANES), (1, own), (count, 2 * slots + 1, 2, width, width),
        ],
        split
        + [
            pltpu.VMEM((MODES, own), F32),
            pltpu.VMEM((count, width, width), F32),
            pltpu.VMEM((count, slots, width, width), F32),
            pltpu.SemaphoreType.DMA((2 * groups + 1,)),
        ],
        1 << 30,
        [pltpu.HBM] * 3,
    )
    edge_rows = REACH * MODES
    basis, images, known = [vectors], [stiff], []
    for iteration in range(ITERS):
        parts, near, far = exchange(gram, near, far, "row")
        order = MODES * len(basis)
        out_blocks = min(len(basis) + 1, 3)
        wide = [(MODES, extent)] * out_blocks
        packed = min(out_blocks, 2) * MODES
        halves = [(out_blocks * MODES, LANES)] * 2
        outs = call(
            functools.partial(middle_kernel, order, len(parts)),
            [*parts, *known, *basis, *images, near, far, mass, inverse, pairs, parity, offsets],
            [
                *wide, *wide, (packed, LANES), (packed + edge_rows, LANES), (edge_rows, LANES), *halves,
                *([(1, extent)] * 2 if order == MODES else []),
            ],
            split,
            1 << 31,
        )
        basis = outs[:out_blocks]
        images = outs[out_blocks : 2 * out_blocks]
        gram, near, far = outs[2 * out_blocks : 2 * out_blocks + 3]
        known = outs[2 * out_blocks + 3 : 2 * out_blocks + 5]
        if order == MODES:
            mass, inverse = outs[-2:]
    parts, near, far = exchange(gram, near, far, "row")
    weight = own * ranks / MODES
    outs = call(
        functools.partial(last_kernel, MODES * len(basis), len(parts), weight),
        [*parts, *known, *basis, *images, near, far, mass, parity],
        [(1, own), (1, own)],
        [],
        1 << 31,
    )
    return outs[0].reshape(own), outs[1].reshape(own)


def solution(mesh):
    placed = (
        P(("sub", "row"), None, None),
        P(("sub", "row"), None, None, None),
        P(("sub", "row"), None),
        P(("sub", "row")),
        P(None, ("sub", "row")),
    )
    return jax.shard_map(
        local,
        mesh=mesh,
        in_specs=placed,
        out_specs=(P(("sub", "row")), P(("sub", "row"))),
        check_vma=False,
    )
```

```python
import functools

import jax
import jax.numpy as jnp
from jax import lax
from jax.experimental import pallas as pl
from jax.experimental.pallas import tpu as pltpu
from jax.sharding import PartitionSpec as P

MODES = 32
REACH = 4
ITERS = 3
PURIFY = 28
LANES = 128
SETTLED = 1e-8
PANEL = 16
TOGETHER = (1, 2, 4, 8)
F32 = jnp.float32
BF16 = jnp.bfloat16


def pieces(value, count):
    parts = []
    for index in range(count):
        part = value.astype(BF16)
        parts.append(part)
        if index + 1 < count:
            value = value - part.astype(F32)
    return parts


def dot_nn(left, right):
    return lax.dot_general(left, right, (((1,), (0,)), ((), ())), preferred_element_type=F32)


def dot_nt(left, right):
    return lax.dot_general(left, right, (((1,), (1,)), ((), ())), preferred_element_type=F32)


def pad_rows(value):
    short = LANES - value.shape[0]
    if short == 0:
        return value
    return jnp.concatenate([value, jnp.zeros((short, value.shape[1]), value.dtype)], axis=0)


def transposed(value):
    return pad_rows(value).T[: value.shape[0]]


def fold(out):
    rows, width = out.shape[0] // 2, out.shape[1] // 2
    out = out[:rows] + out[rows:]
    return out[:, :width] + out[:, width:]


def mul_nn(left, right):
    right = [pad_rows(part) for part in pieces(right, 2)]
    return fold(dot_nn(jnp.concatenate(pieces(left, 2), axis=0), jnp.concatenate(right, axis=1)))


def mul_nt(left, right):
    right = [pad_rows(part) for part in pieces(right, 2)]
    return fold(dot_nt(jnp.concatenate(pieces(left, 2), axis=0), jnp.concatenate(right, axis=0)))


def lane_of(shape):
    return lax.broadcasted_iota(jnp.int32, shape, 1)


def row_of(shape):
    return lax.broadcasted_iota(jnp.int32, shape, 0)


def eye_of(rows, lead=0):
    shape = (rows, LANES)
    return lane_of(shape) == row_of(shape) + lead


def eliminate(matrix, other, lead):
    order = matrix.shape[0]
    tiles = order // 8
    a = [matrix[8 * i : 8 * i + 8] for i in range(tiles)]
    e = [other[8 * i : 8 * i + 8] for i in range(tiles)]
    sub = row_of((8, LANES))
    for start in range(0, order, PANEL):
        columns = [
            {
                i: jnp.broadcast_to(a[i][:, lead + start + k : lead + start + k + 1], (8, LANES))
                for i in range(start // 8, tiles)
            }
            for k in range(PANEL)
        ]
        for step in range(PANEL):
            kt, k = (start + step) // 8, step % 8
            below = range(kt, tiles)
            head = lambda tile: jnp.broadcast_to(tile[k : k + 1, :], (8, LANES))
            pivot = head(columns[step][kt])
            inverse = 1.0 / pivot
            ratios = {i: columns[step][i] * inverse for i in below}
            ratios[kt] = jnp.where(sub > k, ratios[kt], 0.0)
            for later in range(step + 1, PANEL):
                top = head(columns[later][kt])
                for i in below:
                    columns[later][i] = columns[later][i] - ratios[i] * top
            row_a, row_e = head(a[kt]), head(e[kt])
            for i in below:
                a[i] = a[i] - ratios[i] * row_a
                e[i] = e[i] - ratios[i] * row_e
            e[kt] = jnp.where(sub == k, e[kt] * lax.rsqrt(pivot), e[kt])
    return jnp.concatenate(e, axis=0)


def total_of(value):
    return jnp.sum(jnp.sum(value, axis=0, keepdims=True), axis=1, keepdims=True)


def purify(matrix, wanted, steps):
    order = matrix.shape[0]
    eye = eye_of(order)
    valid = lane_of((1, LANES)) < order
    diagonal = jnp.sum(jnp.where(eye, matrix, 0.0), axis=0, keepdims=True)
    center = jnp.sum(diagonal, axis=1, keepdims=True) / order
    radius = jnp.sum(jnp.where(eye, 0.0, jnp.abs(matrix)), axis=0, keepdims=True)
    highest = jnp.max(jnp.where(valid, diagonal + radius, -jnp.inf), axis=1, keepdims=True)
    lowest = jnp.min(jnp.where(valid, diagonal - radius, jnp.inf), axis=1, keepdims=True)
    factor = jnp.minimum(
        wanted / jnp.maximum(highest - center, 1e-06),
        (order - wanted) / jnp.maximum(center - lowest, 1e-06),
    )
    ones = jnp.where(eye, 1.0, 0.0)
    initial = factor / order * (center * ones - matrix) + wanted / order * ones

    def purify_step(density):
        square = mul_nn(density, density)
        cube = mul_nn(square, density)
        gap = density - square
        below = total_of(jnp.where(eye, density, 0.0) - density * density)
        above = total_of(density * gap)
        change = total_of(gap * gap)
        safe = jnp.where(jnp.abs(below) > 1e-12, below, 1.0)
        ratio = jnp.clip(above / safe, 0.0, 1.0)
        high = ratio >= 0.5
        scale = 1.0 / jnp.where(high, jnp.maximum(ratio, 0.5), jnp.maximum(1.0 - ratio, 0.5))
        first = jnp.where(high, 0.0, 1.0 - 2.0 * ratio) * scale
        second = (1.0 + ratio) * scale
        return first * density + second * square - scale * cube, change

    def advance(carry):
        index, _, density = carry
        density, change = purify_step(density)
        return index + 1, change[0, 0], density

    def unsettled(carry):
        return (carry[0] < steps) & (carry[1] > SETTLED)

    return lax.while_loop(unsettled, advance, (0, jnp.float32(1.0), initial))[2]


def ritz(half_stiff, half_mass, wanted, steps, last):
    order = half_stiff.shape[0]
    eye = eye_of(order)
    gram_stiff = half_stiff + transposed(half_stiff)
    gram_mass = half_mass + transposed(half_mass)
    picked = jnp.where(eye, gram_mass, 0.0)
    scale_col = lax.rsqrt(jnp.sum(picked, axis=1, keepdims=True) + 1e-06)
    scale_row = lax.rsqrt(jnp.sum(picked, axis=0, keepdims=True) + 1e-06)
    stiff = scale_col * gram_stiff * scale_row
    mass = scale_col * gram_mass * scale_row
    ones = jnp.where(eye, 1.0, 0.0)
    if order == wanted:
        inverse_low = eliminate(mass, ones, 0)
    else:
        known = lane_of((1, LANES)) < wanted
        pivots = jnp.where(known, jnp.sum(jnp.where(eye, mass, 0.0), axis=0, keepdims=True), 1.0)
        ratio = jnp.where(known, mass[wanted:], 0.0) / pivots
        rest = jnp.where(known, 0.0, mass[wanted:] - mul_nn(ratio, mass[:wanted]))
        inverse_low = jnp.concatenate(
            [ones[:wanted] * lax.rsqrt(pivots), eliminate(rest, ones[wanted:] - ratio, wanted)], axis=0
        )
    reduced = mul_nt(mul_nn(inverse_low, stiff), inverse_low)
    reduced = 0.5 * (reduced + transposed(reduced))
    if order == wanted:
        return inverse_low * scale_row, reduced, gram_stiff, gram_mass
    columns = purify(reduced, wanted, steps)[:wanted]
    columns = eliminate(mul_nt(columns, columns), columns, 0)
    coefficients = mul_nn(columns, inverse_low) * scale_row
    if last:
        return coefficients, None, gram_stiff, gram_mass
    projected = mul_nt(mul_nn(columns, reduced), columns)
    return coefficients, 0.5 * (projected + transposed(projected)), gram_stiff, gram_mass


def halves_next(coefficients, projected, gram_stiff, gram_mass):
    order = gram_stiff.shape[0]
    wanted = coefficients.shape[0]
    lane = lane_of((wanted, LANES))
    first = lane < wanted
    stiff_top = jnp.where(first, 0.5 * projected, 0.0)
    mass_top = jnp.where(eye_of(wanted), 0.5, 0.0)
    blank = jnp.zeros((wanted, LANES), F32)
    if order == wanted:
        return jnp.concatenate([stiff_top, blank], axis=0), jnp.concatenate([mass_top, blank], axis=0)
    later = jnp.where(first, 0.0, coefficients)
    both = jnp.concatenate([mul_nn(later, gram_stiff), mul_nn(later, gram_mass)], axis=0)
    crossed = mul_nt(both, jnp.concatenate([coefficients, later], axis=0))
    moved = pltpu.roll(crossed, wanted, 1)
    lane = lane_of((2 * wanted, LANES))
    tail = jnp.where((lane >= 2 * wanted) & (lane < 3 * wanted), 0.5 * moved, 0.0)
    crossed = jnp.where(lane < wanted, crossed, tail)
    return (
        jnp.concatenate([stiff_top, blank, crossed[:wanted]], axis=0),
        jnp.concatenate([mass_top, blank, crossed[wanted:]], axis=0),
    )


def odd_lanes(rows):
    return (lane_of((rows, LANES)) // MODES) % 2 == 1


def pack_gram(gram):
    rows = gram.shape[0]
    gram = jnp.where(odd_lanes(rows), gram, 0.0)
    if rows <= 2 * MODES:
        return gram
    top = gram[:MODES] + pltpu.roll(gram[2 * MODES :], MODES, 1)
    return jnp.concatenate([top, gram[MODES : 2 * MODES]], axis=0)


def unpack_gram(packed, order):
    if order > 2 * MODES:
        packed = jnp.concatenate([packed, pltpu.roll(packed[:MODES], LANES - MODES, 1)], axis=0)
    return jnp.where(odd_lanes(order), packed, 0.0)


def halves_now(parts, known, order):
    total = parts[0][...]
    for part in parts[1:]:
        total = total + part[...]
    total = unpack_gram(total, order)
    if order == MODES:
        first = lane_of((MODES, LANES)) < MODES
        stiff = jnp.where(first, 0.5 * pltpu.roll(total, LANES - MODES, 1), 0.0)
        mass = jnp.where(first, 0.5 * pltpu.roll(total, MODES, 1), 0.0)
        return stiff, mass
    row = row_of((order, LANES))
    lane = lane_of((order, LANES))
    total = total * jnp.where((row >= MODES) & (row < 2 * MODES), 0.5, 1.0)
    inside = (lane >= MODES) & (lane < 2 * MODES)
    stiff = known[0][...] + jnp.where(inside, total, 0.0)
    mass = known[1][...] + jnp.where(inside, pltpu.roll(total, LANES // 2, 1), 0.0)
    return stiff, mass


def stiffness_apply(split_ref, out_ref, offsets_ref, first, last, pairs_of):
    width = split_ref.shape[1] // (offsets_ref.shape[0] + REACH)
    slots = offsets_ref.shape[1]

    def products(block):
        here = pl.ds(pl.multiple_of((block + REACH) * width, width), width)
        mine = split_ref[:, here]
        pairs = pairs_of(block)
        own = dot_nn(mine, jnp.concatenate(pairs[0], axis=1))
        spread = []
        for slot in range(slots):
            back = block + REACH - offsets_ref[block, slot]
            there = pl.ds(pl.multiple_of(back * width, width), width)
            across, down = pairs[2 * slot + 1], pairs[2 * slot + 2]
            own = own + dot_nn(split_ref[:, there], jnp.concatenate(down, axis=1))
            spread.append((there, fold(dot_nn(mine, jnp.concatenate(across, axis=1)))))
        return [(here, fold(own)), *spread]

    together = max(size for size in TOGETHER if (last - first) % size == 0)

    def group_step(group, carry):
        found = []
        for index in range(together):
            found += products(first + group * together + index)
        for at, product in found:
            out_ref[:, at] += product
        return carry

    lax.fori_loop(0, (last - first) // together, group_step, 0)


def loaded_pairs(pairs_ref):
    slots = pairs_ref.shape[1]
    return lambda block: [[pairs_ref[block, slot, 0], pairs_ref[block, slot, 1]] for slot in range(slots)]


def stacked(value, width):
    count = value.shape[1] // width
    return jnp.concatenate([value[:, width * i : width * (i + 1)] for i in range(count)], axis=0)


def unstacked(value, count):
    rows = value.shape[0] // count
    return jnp.concatenate([value[rows * i : rows * (i + 1)] for i in range(count)], axis=1)


def send_edges(gram, behind, ahead, even, gram_ref, near_ref, far_ref):
    behind, ahead = stacked(behind, LANES), stacked(ahead, LANES)
    rows = gram.shape[0]
    gram_ref[...] = gram
    near_ref[:rows, :] = gram
    near_ref[rows:, :] = jnp.where(even, ahead, behind)
    far_ref[...] = jnp.where(even, behind, ahead)


def received_edges(near_ref, far_ref, even):
    far = far_ref[...]
    near = near_ref[near_ref.shape[0] - far.shape[0] :, :]
    ahead, behind = jnp.where(even, far, near), jnp.where(even, near, far)
    return unstacked(ahead, REACH), unstacked(behind, REACH)


def split_store(split_ref, at, value):
    rows = value.shape[0]
    high, low = pieces(value, 2)
    split_ref[:rows, at] = high
    split_ref[rows:, at] = low


def gram_of(basis_refs, vectors_ref, stiff_ref, mass):
    halo = stiff_ref.shape[1] - mass.shape[1]
    weighted = jnp.concatenate(
        [jnp.zeros((MODES, halo), F32), vectors_ref[:, halo:] * mass], axis=1
    )
    stiff_high, stiff_low = pieces(stiff_ref[...], 2)
    mass_high, mass_low = pieces(weighted, 2)
    right = jnp.concatenate([stiff_low, stiff_high, mass_low, mass_high], axis=0)
    basis = [pieces(ref[...], 2) for ref in basis_refs]
    left = jnp.concatenate([pair[0] for pair in basis] + [pair[1] for pair in basis], axis=0)
    out = dot_nt(left, right)
    rows = left.shape[0] // 2
    out = out[:rows] + out[rows:]
    return pack_gram(out + pltpu.roll(out, MODES, 1))


def first_kernel(
    modes_hbm, diag_hbm, coupling_hbm, edge_ref, mass_ref, parity_ref, offsets_ref,
    basis_ref, stiff_ref, gram_ref, near_ref, far_ref, inverse_ref, pairs_ref,
    split_ref, modes_ref, diag_ref, coupling_ref, semaphores,
):
    halo = edge_ref.shape[1]
    count, width = diag_ref.shape[0], diag_ref.shape[1]
    groups = semaphores.shape[0] // 2
    size = count // groups
    copies = [pltpu.make_async_copy(modes_hbm, modes_ref, semaphores.at[2 * groups])]
    for group in range(groups):
        at = pl.ds(group * size, size)
        copies.append(pltpu.make_async_copy(diag_hbm.at[at], diag_ref.at[at], semaphores.at[2 * group]))
        copies.append(
            pltpu.make_async_copy(coupling_hbm.at[at], coupling_ref.at[at], semaphores.at[2 * group + 1])
        )
    for copy in copies:
        copy.start()
    diagonal = lax.broadcasted_iota(jnp.int32, (width, width), 0) == lax.broadcasted_iota(
        jnp.int32, (width, width), 1
    )

    def pairs_of(block):
        pairs = [pieces(jnp.where(diagonal, 0.0, diag_ref[block]), 2)]
        for slot in range(coupling_ref.shape[1]):
            pair = pieces(coupling_ref[block, slot], 2)
            pairs += [pair, [part.T for part in pair]]
        for index, pair in enumerate(pairs):
            pairs_ref[block, index, 0] = pair[0]
            pairs_ref[block, index, 1] = pair[1]
        return pairs

    copies[0].wait()
    basis_ref[:, :halo] = edge_ref[...]
    basis_ref[:, halo:] = modes_ref[...]
    split_store(split_ref, slice(None), basis_ref[...])
    stiff_ref[...] = jnp.zeros(stiff_ref.shape, F32)
    for group in range(groups):
        copies[2 * group + 1].wait()
        copies[2 * group + 2].wait()
        for block in range(group * size, (group + 1) * size):
            at = slice(block * width, (block + 1) * width)
            picked = jnp.sum(jnp.where(diagonal, diag_ref[block], 0.0), axis=0, keepdims=True)
            inverse_ref[:, at] = 1.0 / picked
            stiff_ref[:, halo + block * width : halo + (block + 1) * width] += modes_ref[:, at] * picked
        stiffness_apply(split_ref, stiff_ref, offsets_ref, group * size, (group + 1) * size, pairs_of)
    gram = gram_of([basis_ref], basis_ref, stiff_ref, mass_ref[...])
    extra = near_ref.shape[0] // REACH - MODES - gram.shape[0] // REACH
    start = inverse_ref.shape[1] - halo
    tail = jnp.where(
        row_of((extra, halo)) == 0,
        jnp.broadcast_to(inverse_ref[:, start:], (extra, halo)),
        jnp.broadcast_to(mass_ref[:, start:], (extra, halo)),
    )
    behind = jnp.concatenate([stiff_ref[:, :halo], tail], axis=0)
    ahead = jnp.concatenate([stiff_ref[:, stiff_ref.shape[1] - halo :], tail], axis=0)
    send_edges(gram, behind, ahead, parity_ref[0] == 0, gram_ref, near_ref, far_ref)


def doubled(left):
    return jnp.concatenate([jnp.concatenate([part, part], axis=1) for part in pieces(left, 2)], axis=0)


def combine(left, right):
    out = dot_nn(left, jnp.concatenate(pieces(right, 2), axis=0))
    rows = left.shape[0] // 2
    return out[:rows] + out[rows:]


def middle_kernel(order, parts_count, *refs):
    refs = list(refs)
    take = lambda count: [refs.pop(0) for _ in range(count)]
    parts = take(parts_count)
    known = take(2) if order > MODES else []
    blocks = order // MODES
    basis = take(blocks)
    stiff = take(blocks)
    near_in, far_in, mass_in, inverse_in, pairs_ref, parity_ref, offsets_ref = take(7)
    out_blocks = min(blocks + 1, 3)
    basis_out = take(out_blocks)
    stiff_out = take(out_blocks)
    gram_ref, near_ref, far_ref, half_stiff_ref, half_mass_ref = take(5)
    mass_ref, inverse_ref = take(2) if order == MODES else (mass_in, inverse_in)
    (split_ref,) = take(1)

    even = parity_ref[0] == 0
    coefficients, projected, gram_stiff, gram_mass = ritz(
        *halves_now(parts, known, order), MODES, PURIFY, False
    )
    halves = halves_next(coefficients, projected, gram_stiff, gram_mass)
    half_stiff_ref[...] = halves[0]
    half_mass_ref[...] = halves[1]
    ahead, behind = received_edges(near_in, far_in, even)
    halo = ahead.shape[1]
    extent = basis[0].shape[1]
    if order == MODES:
        inverse_ref[:, :halo] = ahead[MODES : MODES + 1]
        inverse_ref[:, halo:] = inverse_in[...]
        mass_ref[:, :halo] = ahead[MODES + 1 : MODES + 2]
        mass_ref[:, halo:] = mass_in[...]
    mixing = coefficients[:, :order]
    if order > MODES:
        later = jnp.where(lane_of((MODES, LANES)) < MODES, 0.0, coefficients)
        mixing = jnp.concatenate([mixing, later[:, :order]], axis=0)
    mixing = doubled(mixing)
    pulling = doubled(projected[:, :MODES])
    newest = 0 if order == MODES else 1
    for start in range(0, extent, halo):
        at = slice(start, start + halo)
        current = [ref[:, at] for ref in stiff]
        if start == 0:
            current[newest] = current[newest] + ahead[:MODES]
        if start + halo == extent:
            current[newest] = current[newest] + behind[:MODES]
        vectors = combine(mixing, jnp.concatenate([ref[:, at] for ref in basis], axis=0))
        images = combine(mixing, jnp.concatenate(current, axis=0))
        modes, stiff_modes = vectors[:MODES], images[:MODES]
        basis_out[0][:, at] = modes
        stiff_out[0][:, at] = stiff_modes
        if order > MODES:
            basis_out[2][:, at] = vectors[MODES:]
            stiff_out[2][:, at] = images[MODES:]
        residual = stiff_modes - combine(pulling, modes * mass_ref[:, at])
        precond = residual * inverse_ref[:, at]
        basis_out[1][:, at] = precond
        split_store(split_ref, at, precond)
        stiff_out[1][:, at] = jnp.zeros((MODES, halo), F32) if start == 0 else residual
    stiffness_apply(split_ref, stiff_out[1], offsets_ref, 0, offsets_ref.shape[0], loaded_pairs(pairs_ref))
    gram = gram_of(basis_out, basis_out[1], stiff_out[1], mass_ref[:, halo:])
    newest = stiff_out[1]
    send_edges(gram, newest[:, :halo], newest[:, extent - halo :], even, gram_ref, near_ref, far_ref)


def last_kernel(order, parts_count, weight, *refs):
    refs = list(refs)
    take = lambda count: [refs.pop(0) for _ in range(count)]
    parts = take(parts_count)
    known = take(2)
    blocks = order // MODES
    basis = take(blocks)
    stiff = take(blocks)
    near_in, far_in, mass_ref, parity_ref = take(4)
    mass_out, energy_out = take(2)
    coefficients = ritz(*halves_now(parts, known, order), MODES, PURIFY, True)[0]
    behind = received_edges(near_in, far_in, parity_ref[0] == 0)[1]
    halo = behind.shape[1]
    extent = mass_ref.shape[1]
    mixing = doubled(coefficients[:, :order])
    for start in range(halo, extent, halo):
        at = slice(start, start + halo)
        to = slice(start - halo, start)
        current = [ref[:, at] for ref in stiff]
        if start + halo == extent:
            current[1] = current[1] + behind
        vectors = combine(mixing, jnp.concatenate([ref[:, at] for ref in basis], axis=0))
        images = combine(mixing, jnp.concatenate(current, axis=0))
        mass_out[:, to] = weight * mass_ref[:, at] * jnp.sum(vectors * vectors, axis=0, keepdims=True)
        energy_out[:, to] = weight * jnp.sum(vectors * images, axis=0, keepdims=True)


def call(kernel, args, outs, scratch, flops, spaces=()):
    spaces = list(spaces) + [pltpu.VMEM] * (len(args) - len(spaces))
    spaces = [pltpu.SMEM if arg.dtype == jnp.int32 else space for arg, space in zip(args, spaces)]
    return pl.pallas_call(
        kernel,
        out_shape=[
            jax.ShapeDtypeStruct(shape, BF16 if len(shape) > 2 else F32) for shape in outs
        ],
        in_specs=[pl.BlockSpec(memory_space=space) for space in spaces],
        out_specs=[pl.BlockSpec(memory_space=pltpu.VMEM)] * len(outs),
        scratch_shapes=scratch,
        compiler_params=pltpu.CompilerParams(vmem_limit_bytes=24 << 20),
        cost_estimate=pl.CostEstimate(flops=flops, bytes_accessed=1 << 20, transcendentals=0),
    )(*args)


def hbm(value):
    return pltpu.with_memory_space_constraint(value, pltpu.HBM)


def exchange(gram, near, far, axis):
    count = lax.axis_size(axis)
    across = lambda value, mask: lax.ppermute(
        value, axis, [(at, at ^ mask) for at in range(count) if at ^ mask < count]
    )
    near = across(near, 1)
    if count & (count - 1):
        parts = [lax.psum(gram, axis)]
    else:
        parts, stride = [gram], 1
        while stride < count:
            if len(parts) > 1:
                gram = sum(parts[1:], parts[0])
            masks = [stride, 2 * stride, 3 * stride] if 4 * stride <= count else [stride]
            parts = [gram] + [
                near[: gram.shape[0]] if mask == 1 else across(gram, mask) for mask in masks
            ]
            stride *= 1 << len(masks).bit_length()
    hops = [(at, at + 1 if at % 2 else at - 1) for at in range(count)]
    far = lax.ppermute(far, axis, [hop for hop in hops if 0 <= hop[1] < count])
    return parts, near, far


def local(diag_blocks, coupling, offsets, mass, initial_modes):
    count, width = diag_blocks.shape[0], diag_blocks.shape[1]
    slots = coupling.shape[1]
    own = count * width
    halo = REACH * width
    extent = own + halo
    split = [pltpu.VMEM((2 * MODES, extent), BF16)]
    parity = (lax.axis_index("row") % 2).astype(jnp.int32).reshape(1)
    mass = mass.reshape(1, own)
    spare = 8
    ranks = lax.axis_size("row")
    edge = lax.ppermute(initial_modes[:, own - halo :], "row", [(at, at + 1) for at in range(ranks - 1)])
    edge_rows = REACH * (MODES + spare)
    groups = 4 if count % 4 == 0 else 1
    vectors, stiff, gram, near, far, inverse, pairs = call(
        first_kernel,
        [hbm(initial_modes), hbm(diag_blocks), hbm(coupling), edge, mass, parity, offsets],
        [
            (MODES, extent), (MODES, extent), (MODES, LANES), (MODES + edge_rows, LANES),
            (edge_rows, LANES), (1, own), (count, 2 * slots + 1, 2, width, width),
        ],
        split
        + [
            pltpu.VMEM((MODES, own), F32),
            pltpu.VMEM((count, width, width), F32),
            pltpu.VMEM((count, slots, width, width), F32),
            pltpu.SemaphoreType.DMA((2 * groups + 1,)),
        ],
        1 << 30,
        [pltpu.HBM] * 3,
    )
    edge_rows = REACH * MODES
    basis, images, known = [vectors], [stiff], []
    for iteration in range(ITERS):
        parts, near, far = exchange(gram, near, far, "row")
        order = MODES * len(basis)
        out_blocks = min(len(basis) + 1, 3)
        wide = [(MODES, extent)] * out_blocks
        packed = min(out_blocks, 2) * MODES
        halves = [(out_blocks * MODES, LANES)] * 2
        outs = call(
            functools.partial(middle_kernel, order, len(parts)),
            [*parts, *known, *basis, *images, near, far, mass, inverse, pairs, parity, offsets],
            [
                *wide, *wide, (packed, LANES), (packed + edge_rows, LANES), (edge_rows, LANES), *halves,
                *([(1, extent)] * 2 if order == MODES else []),
            ],
            split,
            1 << 31,
        )
        basis = outs[:out_blocks]
        images = outs[out_blocks : 2 * out_blocks]
        gram, near, far = outs[2 * out_blocks : 2 * out_blocks + 3]
        known = outs[2 * out_blocks + 3 : 2 * out_blocks + 5]
        if order == MODES:
            mass, inverse = outs[-2:]
    parts, near, far = exchange(gram, near, far, "row")
    weight = own * ranks / MODES
    outs = call(
        functools.partial(last_kernel, MODES * len(basis), len(parts), weight),
        [*parts, *known, *basis, *images, near, far, mass, parity],
        [(1, own), (1, own)],
        [],
        1 << 31,
    )
    return outs[0].reshape(own), outs[1].reshape(own)


def solution(mesh):
    placed = (
        P(("sub", "row"), None, None),
        P(("sub", "row"), None, None, None),
        P(("sub", "row"), None),
        P(("sub", "row")),
        P(None, ("sub", "row")),
    )
    return jax.shard_map(
        local,
        mesh=mesh,
        in_specs=placed,
        out_specs=(P(("sub", "row")), P(("sub", "row"))),
        check_vma=False,
    )
```

```python
import functools

import jax
import jax.numpy as jnp
from jax import lax
from jax.experimental import pallas as pl
from jax.experimental.pallas import tpu as pltpu
from jax.sharding import PartitionSpec as P

MODES = 32
REACH = 4
ITERS = 3
PURIFY = 28
LANES = 128
SETTLED = 1e-7
PANEL = 16
TOGETHER = (1, 2, 4, 8)
F32 = jnp.float32
BF16 = jnp.bfloat16


def pieces(value, count):
    parts = []
    for index in range(count):
        part = value.astype(BF16)
        parts.append(part)
        if index + 1 < count:
            value = value - part.astype(F32)
    return parts


def dot_nn(left, right):
    return lax.dot_general(left, right, (((1,), (0,)), ((), ())), preferred_element_type=F32)


def dot_nt(left, right):
    return lax.dot_general(left, right, (((1,), (1,)), ((), ())), preferred_element_type=F32)


def pad_rows(value):
    short = LANES - value.shape[0]
    if short == 0:
        return value
    return jnp.concatenate([value, jnp.zeros((short, value.shape[1]), value.dtype)], axis=0)


def transposed(value):
    return pad_rows(value).T[: value.shape[0]]


def fold(out):
    rows, width = out.shape[0] // 2, out.shape[1] // 2
    out = out[:rows] + out[rows:]
    return out[:, :width] + out[:, width:]


def mul_nn(left, right):
    right = [pad_rows(part) for part in pieces(right, 2)]
    return fold(dot_nn(jnp.concatenate(pieces(left, 2), axis=0), jnp.concatenate(right, axis=1)))


def mul_nt(left, right):
    right = [pad_rows(part) for part in pieces(right, 2)]
    return fold(dot_nt(jnp.concatenate(pieces(left, 2), axis=0), jnp.concatenate(right, axis=0)))


def lane_of(shape):
    return lax.broadcasted_iota(jnp.int32, shape, 1)


def row_of(shape):
    return lax.broadcasted_iota(jnp.int32, shape, 0)


def eye_of(rows, lead=0):
    shape = (rows, LANES)
    return lane_of(shape) == row_of(shape) + lead


def eliminate(matrix, other, lead):
    order = matrix.shape[0]
    tiles = order // 8
    a = [matrix[8 * i : 8 * i + 8] for i in range(tiles)]
    e = [other[8 * i : 8 * i + 8] for i in range(tiles)]
    sub = row_of((8, LANES))
    for start in range(0, order, PANEL):
        columns = [
            {
                i: jnp.broadcast_to(a[i][:, lead + start + k : lead + start + k + 1], (8, LANES))
                for i in range(start // 8, tiles)
            }
            for k in range(PANEL)
        ]
        for step in range(PANEL):
            kt, k = (start + step) // 8, step % 8
            below = range(kt, tiles)
            head = lambda tile: jnp.broadcast_to(tile[k : k + 1, :], (8, LANES))
            pivot = head(columns[step][kt])
            inverse = 1.0 / pivot
            ratios = {i: columns[step][i] * inverse for i in below}
            ratios[kt] = jnp.where(sub > k, ratios[kt], 0.0)
            for later in range(step + 1, PANEL):
                top = head(columns[later][kt])
                for i in below:
                    columns[later][i] = columns[later][i] - ratios[i] * top
            row_a, row_e = head(a[kt]), head(e[kt])
            for i in below:
                a[i] = a[i] - ratios[i] * row_a
                e[i] = e[i] - ratios[i] * row_e
            e[kt] = jnp.where(sub == k, e[kt] * lax.rsqrt(pivot), e[kt])
    return jnp.concatenate(e, axis=0)


def total_of(value):
    return jnp.sum(jnp.sum(value, axis=0, keepdims=True), axis=1, keepdims=True)


def purify(matrix, wanted, steps):
    order = matrix.shape[0]
    eye = eye_of(order)
    valid = lane_of((1, LANES)) < order
    diagonal = jnp.sum(jnp.where(eye, matrix, 0.0), axis=0, keepdims=True)
    center = jnp.sum(diagonal, axis=1, keepdims=True) / order
    radius = jnp.sum(jnp.where(eye, 0.0, jnp.abs(matrix)), axis=0, keepdims=True)
    highest = jnp.max(jnp.where(valid, diagonal + radius, -jnp.inf), axis=1, keepdims=True)
    lowest = jnp.min(jnp.where(valid, diagonal - radius, jnp.inf), axis=1, keepdims=True)
    factor = jnp.minimum(
        wanted / jnp.maximum(highest - center, 1e-06),
        (order - wanted) / jnp.maximum(center - lowest, 1e-06),
    )
    ones = jnp.where(eye, 1.0, 0.0)
    initial = factor / order * (center * ones - matrix) + wanted / order * ones

    def purify_step(density):
        square = mul_nn(density, density)
        cube = mul_nn(square, density)
        gap = density - square
        below = total_of(jnp.where(eye, density, 0.0) - density * density)
        above = total_of(density * gap)
        change = total_of(gap * gap)
        safe = jnp.where(jnp.abs(below) > 1e-12, below, 1.0)
        ratio = jnp.clip(above / safe, 0.0, 1.0)
        high = ratio >= 0.5
        scale = 1.0 / jnp.where(high, jnp.maximum(ratio, 0.5), jnp.maximum(1.0 - ratio, 0.5))
        first = jnp.where(high, 0.0, 1.0 - 2.0 * ratio) * scale
        second = (1.0 + ratio) * scale
        return first * density + second * square - scale * cube, change

    def advance(carry):
        index, _, density = carry
        density, change = purify_step(density)
        return index + 1, change[0, 0], density

    def unsettled(carry):
        return (carry[0] < steps) & (carry[1] > SETTLED)

    return lax.while_loop(unsettled, advance, (0, jnp.float32(1.0), initial))[2]


def ritz(half_stiff, half_mass, wanted, steps, last):
    order = half_stiff.shape[0]
    eye = eye_of(order)
    gram_stiff = half_stiff + transposed(half_stiff)
    gram_mass = half_mass + transposed(half_mass)
    picked = jnp.where(eye, gram_mass, 0.0)
    scale_col = lax.rsqrt(jnp.sum(picked, axis=1, keepdims=True) + 1e-06)
    scale_row = lax.rsqrt(jnp.sum(picked, axis=0, keepdims=True) + 1e-06)
    stiff = scale_col * gram_stiff * scale_row
    mass = scale_col * gram_mass * scale_row
    ones = jnp.where(eye, 1.0, 0.0)
    if order == wanted:
        inverse_low = eliminate(mass, ones, 0)
    else:
        known = lane_of((1, LANES)) < wanted
        pivots = jnp.where(known, jnp.sum(jnp.where(eye, mass, 0.0), axis=0, keepdims=True), 1.0)
        ratio = jnp.where(known, mass[wanted:], 0.0) / pivots
        rest = jnp.where(known, 0.0, mass[wanted:] - mul_nn(ratio, mass[:wanted]))
        inverse_low = jnp.concatenate(
            [ones[:wanted] * lax.rsqrt(pivots), eliminate(rest, ones[wanted:] - ratio, wanted)], axis=0
        )
    reduced = mul_nt(mul_nn(inverse_low, stiff), inverse_low)
    if order == wanted:
        return inverse_low * scale_row, reduced, gram_stiff, gram_mass
    columns = purify(reduced, wanted, steps)[:wanted]
    columns = eliminate(mul_nt(columns, columns), columns, 0)
    coefficients = mul_nn(columns, inverse_low) * scale_row
    if last:
        return coefficients, None, gram_stiff, gram_mass
    projected = mul_nt(mul_nn(columns, reduced), columns)
    return coefficients, projected, gram_stiff, gram_mass


def halves_next(coefficients, projected, gram_stiff, gram_mass):
    order = gram_stiff.shape[0]
    wanted = coefficients.shape[0]
    lane = lane_of((wanted, LANES))
    first = lane < wanted
    stiff_top = jnp.where(first, 0.5 * projected, 0.0)
    mass_top = jnp.where(eye_of(wanted), 0.5, 0.0)
    blank = jnp.zeros((wanted, LANES), F32)
    if order == wanted:
        return jnp.concatenate([stiff_top, blank], axis=0), jnp.concatenate([mass_top, blank], axis=0)
    later = jnp.where(first, 0.0, coefficients)
    both = jnp.concatenate([mul_nn(later, gram_stiff), mul_nn(later, gram_mass)], axis=0)
    crossed = mul_nt(both, jnp.concatenate([coefficients, later], axis=0))
    moved = pltpu.roll(crossed, wanted, 1)
    lane = lane_of((2 * wanted, LANES))
    tail = jnp.where((lane >= 2 * wanted) & (lane < 3 * wanted), 0.5 * moved, 0.0)
    crossed = jnp.where(lane < wanted, crossed, tail)
    return (
        jnp.concatenate([stiff_top, blank, crossed[:wanted]], axis=0),
        jnp.concatenate([mass_top, blank, crossed[wanted:]], axis=0),
    )


def odd_lanes(rows):
    return (lane_of((rows, LANES)) // MODES) % 2 == 1


def pack_gram(gram):
    rows = gram.shape[0]
    gram = jnp.where(odd_lanes(rows), gram, 0.0)
    if rows <= 2 * MODES:
        return gram
    top = gram[:MODES] + pltpu.roll(gram[2 * MODES :], MODES, 1)
    return jnp.concatenate([top, gram[MODES : 2 * MODES]], axis=0)


def unpack_gram(packed, order):
    if order > 2 * MODES:
        packed = jnp.concatenate([packed, pltpu.roll(packed[:MODES], LANES - MODES, 1)], axis=0)
    return jnp.where(odd_lanes(order), packed, 0.0)


def halves_now(parts, known, order):
    total = parts[0][...]
    for part in parts[1:]:
        total = total + part[...]
    total = unpack_gram(total, order)
    if order == MODES:
        first = lane_of((MODES, LANES)) < MODES
        stiff = jnp.where(first, 0.5 * pltpu.roll(total, LANES - MODES, 1), 0.0)
        mass = jnp.where(first, 0.5 * pltpu.roll(total, MODES, 1), 0.0)
        return stiff, mass
    row = row_of((order, LANES))
    lane = lane_of((order, LANES))
    total = total * jnp.where((row >= MODES) & (row < 2 * MODES), 0.5, 1.0)
    inside = (lane >= MODES) & (lane < 2 * MODES)
    stiff = known[0][...] + jnp.where(inside, total, 0.0)
    mass = known[1][...] + jnp.where(inside, pltpu.roll(total, LANES // 2, 1), 0.0)
    return stiff, mass


def stiffness_apply(split_ref, out_ref, offsets_ref, first, last, pairs_of):
    width = split_ref.shape[1] // (offsets_ref.shape[0] + REACH)
    slots = offsets_ref.shape[1]

    def products(block):
        here = pl.ds(pl.multiple_of((block + REACH) * width, width), width)
        mine = split_ref[:, here]
        pairs = pairs_of(block)
        own = dot_nn(mine, jnp.concatenate(pairs[0], axis=1))
        spread = []
        for slot in range(slots):
            back = block + REACH - offsets_ref[block, slot]
            there = pl.ds(pl.multiple_of(back * width, width), width)
            across, down = pairs[2 * slot + 1], pairs[2 * slot + 2]
            own = own + dot_nn(split_ref[:, there], jnp.concatenate(down, axis=1))
            spread.append((there, fold(dot_nn(mine, jnp.concatenate(across, axis=1)))))
        return [(here, fold(own)), *spread]

    together = max(size for size in TOGETHER if (last - first) % size == 0)

    def group_step(group, carry):
        found = []
        for index in range(together):
            found += products(first + group * together + index)
        for at, product in found:
            out_ref[:, at] += product
        return carry

    lax.fori_loop(0, (last - first) // together, group_step, 0)


def loaded_pairs(pairs_ref):
    slots = pairs_ref.shape[1]
    return lambda block: [[pairs_ref[block, slot, 0], pairs_ref[block, slot, 1]] for slot in range(slots)]


def stacked(value, width):
    count = value.shape[1] // width
    return jnp.concatenate([value[:, width * i : width * (i + 1)] for i in range(count)], axis=0)


def unstacked(value, count):
    rows = value.shape[0] // count
    return jnp.concatenate([value[rows * i : rows * (i + 1)] for i in range(count)], axis=1)


def send_edges(gram, behind, ahead, even, gram_ref, near_ref, far_ref):
    behind, ahead = stacked(behind, LANES), stacked(ahead, LANES)
    rows = gram.shape[0]
    gram_ref[...] = gram
    near_ref[:rows, :] = gram
    near_ref[rows:, :] = jnp.where(even, ahead, behind)
    far_ref[...] = jnp.where(even, behind, ahead)


def received_edges(near_ref, far_ref, even):
    far = far_ref[...]
    near = near_ref[near_ref.shape[0] - far.shape[0] :, :]
    ahead, behind = jnp.where(even, far, near), jnp.where(even, near, far)
    return unstacked(ahead, REACH), unstacked(behind, REACH)


def split_store(split_ref, at, value):
    rows = value.shape[0]
    high, low = pieces(value, 2)
    split_ref[:rows, at] = high
    split_ref[rows:, at] = low


def gram_of(basis_refs, vectors_ref, stiff_ref, mass):
    halo = stiff_ref.shape[1] - mass.shape[1]
    weighted = jnp.concatenate(
        [jnp.zeros((MODES, halo), F32), vectors_ref[:, halo:] * mass], axis=1
    )
    stiff_high, stiff_low = pieces(stiff_ref[...], 2)
    mass_high, mass_low = pieces(weighted, 2)
    right = jnp.concatenate([stiff_low, stiff_high, mass_low, mass_high], axis=0)
    basis = [pieces(ref[...], 2) for ref in basis_refs]
    left = jnp.concatenate([pair[0] for pair in basis] + [pair[1] for pair in basis], axis=0)
    out = dot_nt(left, right)
    rows = left.shape[0] // 2
    out = out[:rows] + out[rows:]
    return pack_gram(out + pltpu.roll(out, MODES, 1))


def first_kernel(
    modes_hbm, diag_hbm, coupling_hbm, edge_ref, mass_ref, parity_ref, offsets_ref,
    basis_ref, stiff_ref, gram_ref, near_ref, far_ref, inverse_ref, pairs_ref,
    split_ref, modes_ref, diag_ref, coupling_ref, semaphores,
):
    halo = edge_ref.shape[1]
    count, width = diag_ref.shape[0], diag_ref.shape[1]
    groups = semaphores.shape[0] // 2
    size = count // groups
    copies = [pltpu.make_async_copy(modes_hbm, modes_ref, semaphores.at[2 * groups])]
    for group in range(groups):
        at = pl.ds(group * size, size)
        copies.append(pltpu.make_async_copy(diag_hbm.at[at], diag_ref.at[at], semaphores.at[2 * group]))
        copies.append(
            pltpu.make_async_copy(coupling_hbm.at[at], coupling_ref.at[at], semaphores.at[2 * group + 1])
        )
    for copy in copies:
        copy.start()
    diagonal = lax.broadcasted_iota(jnp.int32, (width, width), 0) == lax.broadcasted_iota(
        jnp.int32, (width, width), 1
    )

    def pairs_of(block):
        pairs = [pieces(jnp.where(diagonal, 0.0, diag_ref[block]), 2)]
        for slot in range(coupling_ref.shape[1]):
            pair = pieces(coupling_ref[block, slot], 2)
            pairs += [pair, [part.T for part in pair]]
        for index, pair in enumerate(pairs):
            pairs_ref[block, index, 0] = pair[0]
            pairs_ref[block, index, 1] = pair[1]
        return pairs

    copies[0].wait()
    basis_ref[:, :halo] = edge_ref[...]
    basis_ref[:, halo:] = modes_ref[...]
    split_store(split_ref, slice(None), basis_ref[...])
    stiff_ref[...] = jnp.zeros(stiff_ref.shape, F32)
    for group in range(groups):
        copies[2 * group + 1].wait()
        copies[2 * group + 2].wait()
        for block in range(group * size, (group + 1) * size):
            at = slice(block * width, (block + 1) * width)
            picked = jnp.sum(jnp.where(diagonal, diag_ref[block], 0.0), axis=0, keepdims=True)
            inverse_ref[:, at] = 1.0 / picked
            stiff_ref[:, halo + block * width : halo + (block + 1) * width] += modes_ref[:, at] * picked
        stiffness_apply(split_ref, stiff_ref, offsets_ref, group * size, (group + 1) * size, pairs_of)
    gram = gram_of([basis_ref], basis_ref, stiff_ref, mass_ref[...])
    extra = near_ref.shape[0] // REACH - MODES - gram.shape[0] // REACH
    start = inverse_ref.shape[1] - halo
    tail = jnp.where(
        row_of((extra, halo)) == 0,
        jnp.broadcast_to(inverse_ref[:, start:], (extra, halo)),
        jnp.broadcast_to(mass_ref[:, start:], (extra, halo)),
    )
    behind = jnp.concatenate([stiff_ref[:, :halo], tail], axis=0)
    ahead = jnp.concatenate([stiff_ref[:, stiff_ref.shape[1] - halo :], tail], axis=0)
    send_edges(gram, behind, ahead, parity_ref[0] == 0, gram_ref, near_ref, far_ref)


def doubled(left):
    return jnp.concatenate([jnp.concatenate([part, part], axis=1) for part in pieces(left, 2)], axis=0)


def combine(left, right):
    out = dot_nn(left, jnp.concatenate(pieces(right, 2), axis=0))
    rows = left.shape[0] // 2
    return out[:rows] + out[rows:]


def middle_kernel(order, parts_count, *refs):
    refs = list(refs)
    take = lambda count: [refs.pop(0) for _ in range(count)]
    parts = take(parts_count)
    known = take(2) if order > MODES else []
    blocks = order // MODES
    basis = take(blocks)
    stiff = take(blocks)
    near_in, far_in, mass_in, inverse_in, pairs_ref, parity_ref, offsets_ref = take(7)
    out_blocks = min(blocks + 1, 3)
    basis_out = take(out_blocks)
    stiff_out = take(out_blocks)
    gram_ref, near_ref, far_ref, half_stiff_ref, half_mass_ref = take(5)
    mass_ref, inverse_ref = take(2) if order == MODES else (mass_in, inverse_in)
    (split_ref,) = take(1)

    even = parity_ref[0] == 0
    coefficients, projected, gram_stiff, gram_mass = ritz(
        *halves_now(parts, known, order), MODES, PURIFY, False
    )
    halves = halves_next(coefficients, projected, gram_stiff, gram_mass)
    half_stiff_ref[...] = halves[0]
    half_mass_ref[...] = halves[1]
    ahead, behind = received_edges(near_in, far_in, even)
    halo = ahead.shape[1]
    extent = basis[0].shape[1]
    if order == MODES:
        inverse_ref[:, :halo] = ahead[MODES : MODES + 1]
        inverse_ref[:, halo:] = inverse_in[...]
        mass_ref[:, :halo] = ahead[MODES + 1 : MODES + 2]
        mass_ref[:, halo:] = mass_in[...]
    mixing = coefficients[:, :order]
    if order > MODES:
        later = jnp.where(lane_of((MODES, LANES)) < MODES, 0.0, coefficients)
        mixing = jnp.concatenate([mixing, later[:, :order]], axis=0)
    mixing = doubled(mixing)
    pulling = doubled(projected[:, :MODES])
    newest = 0 if order == MODES else 1
    current = [ref[...] for ref in stiff]
    completion = jnp.concatenate(
        [ahead[:MODES], jnp.zeros((MODES, extent - 2 * halo), F32), behind[:MODES]], axis=1
    )
    current[newest] = current[newest] + completion
    vectors = combine(mixing, jnp.concatenate([ref[...] for ref in basis], axis=0))
    images = combine(mixing, jnp.concatenate(current, axis=0))
    modes, stiff_modes = vectors[:MODES], images[:MODES]
    residual = stiff_modes - combine(pulling, modes * mass_ref[...])
    precond = residual * inverse_ref[...]
    split_store(split_ref, slice(None), precond)
    basis_out[0][...] = modes
    stiff_out[0][...] = stiff_modes
    if order > MODES:
        basis_out[2][...] = vectors[MODES:]
        stiff_out[2][...] = images[MODES:]
    basis_out[1][...] = precond
    stiff_out[1][:, :halo] = jnp.zeros((MODES, halo), F32)
    stiff_out[1][:, halo:] = residual[:, halo:]
    stiffness_apply(split_ref, stiff_out[1], offsets_ref, 0, offsets_ref.shape[0], loaded_pairs(pairs_ref))
    gram = gram_of(basis_out, basis_out[1], stiff_out[1], mass_ref[:, halo:])
    newest = stiff_out[1]
    send_edges(gram, newest[:, :halo], newest[:, extent - halo :], even, gram_ref, near_ref, far_ref)


def last_kernel(order, parts_count, weight, *refs):
    refs = list(refs)
    take = lambda count: [refs.pop(0) for _ in range(count)]
    parts = take(parts_count)
    known = take(2)
    blocks = order // MODES
    basis = take(blocks)
    stiff = take(blocks)
    near_in, far_in, mass_ref, parity_ref = take(4)
    mass_out, energy_out = take(2)
    coefficients = ritz(*halves_now(parts, known, order), MODES, PURIFY, True)[0]
    behind = received_edges(near_in, far_in, parity_ref[0] == 0)[1]
    halo = behind.shape[1]
    extent = mass_ref.shape[1]
    mixing = doubled(coefficients[:, :order])
    for start in range(halo, extent, halo):
        at = slice(start, start + halo)
        to = slice(start - halo, start)
        current = [ref[:, at] for ref in stiff]
        if start + halo == extent:
            current[1] = current[1] + behind
        vectors = combine(mixing, jnp.concatenate([ref[:, at] for ref in basis], axis=0))
        images = combine(mixing, jnp.concatenate(current, axis=0))
        mass_out[:, to] = weight * mass_ref[:, at] * jnp.sum(vectors * vectors, axis=0, keepdims=True)
        energy_out[:, to] = weight * jnp.sum(vectors * images, axis=0, keepdims=True)


def call(kernel, args, outs, scratch, flops, spaces=()):
    spaces = list(spaces) + [pltpu.VMEM] * (len(args) - len(spaces))
    spaces = [pltpu.SMEM if arg.dtype == jnp.int32 else space for arg, space in zip(args, spaces)]
    return pl.pallas_call(
        kernel,
        out_shape=[
            jax.ShapeDtypeStruct(shape, BF16 if len(shape) > 2 else F32) for shape in outs
        ],
        in_specs=[pl.BlockSpec(memory_space=space) for space in spaces],
        out_specs=[pl.BlockSpec(memory_space=pltpu.VMEM)] * len(outs),
        scratch_shapes=scratch,
        compiler_params=pltpu.CompilerParams(vmem_limit_bytes=24 << 20),
        cost_estimate=pl.CostEstimate(flops=flops, bytes_accessed=1 << 20, transcendentals=0),
    )(*args)


def hbm(value):
    return pltpu.with_memory_space_constraint(value, pltpu.HBM)


def exchange(gram, near, far, axis):
    count = lax.axis_size(axis)
    across = lambda value, mask: lax.ppermute(
        value, axis, [(at, at ^ mask) for at in range(count) if at ^ mask < count]
    )
    near = across(near, 1)
    if count & (count - 1):
        parts = [lax.psum(gram, axis)]
    else:
        parts, stride = [gram], 1
        while stride < count:
            if len(parts) > 1:
                gram = sum(parts[1:], parts[0])
            masks = [stride, 2 * stride, 3 * stride] if 4 * stride <= count else [stride]
            parts = [gram] + [
                near[: gram.shape[0]] if mask == 1 else across(gram, mask) for mask in masks
            ]
            stride *= 1 << len(masks).bit_length()
    hops = [(at, at + 1 if at % 2 else at - 1) for at in range(count)]
    far = lax.ppermute(far, axis, [hop for hop in hops if 0 <= hop[1] < count])
    return parts, near, far


def local(diag_blocks, coupling, offsets, mass, initial_modes):
    count, width = diag_blocks.shape[0], diag_blocks.shape[1]
    slots = coupling.shape[1]
    own = count * width
    halo = REACH * width
    extent = own + halo
    split = [pltpu.VMEM((2 * MODES, extent), BF16)]
    parity = (lax.axis_index("row") % 2).astype(jnp.int32).reshape(1)
    mass = mass.reshape(1, own)
    spare = 8
    ranks = lax.axis_size("row")
    edge = lax.ppermute(initial_modes[:, own - halo :], "row", [(at, at + 1) for at in range(ranks - 1)])
    edge_rows = REACH * (MODES + spare)
    groups = 4 if count % 4 == 0 else 1
    vectors, stiff, gram, near, far, inverse, pairs = call(
        first_kernel,
        [hbm(initial_modes), hbm(diag_blocks), hbm(coupling), edge, mass, parity, offsets],
        [
            (MODES, extent), (MODES, extent), (MODES, LANES), (MODES + edge_rows, LANES),
            (edge_rows, LANES), (1, own), (count, 2 * slots + 1, 2, width, width),
        ],
        split
        + [
            pltpu.VMEM((MODES, own), F32),
            pltpu.VMEM((count, width, width), F32),
            pltpu.VMEM((count, slots, width, width), F32),
            pltpu.SemaphoreType.DMA((2 * groups + 1,)),
        ],
        1 << 30,
        [pltpu.HBM] * 3,
    )
    edge_rows = REACH * MODES
    basis, images, known = [vectors], [stiff], []
    for iteration in range(ITERS):
        parts, near, far = exchange(gram, near, far, "row")
        order = MODES * len(basis)
        out_blocks = min(len(basis) + 1, 3)
        wide = [(MODES, extent)] * out_blocks
        packed = min(out_blocks, 2) * MODES
        halves = [(out_blocks * MODES, LANES)] * 2
        outs = call(
            functools.partial(middle_kernel, order, len(parts)),
            [*parts, *known, *basis, *images, near, far, mass, inverse, pairs, parity, offsets],
            [
                *wide, *wide, (packed, LANES), (packed + edge_rows, LANES), (edge_rows, LANES), *halves,
                *([(1, extent)] * 2 if order == MODES else []),
            ],
            split,
            1 << 31,
        )
        basis = outs[:out_blocks]
        images = outs[out_blocks : 2 * out_blocks]
        gram, near, far = outs[2 * out_blocks : 2 * out_blocks + 3]
        known = outs[2 * out_blocks + 3 : 2 * out_blocks + 5]
        if order == MODES:
            mass, inverse = outs[-2:]
    parts, near, far = exchange(gram, near, far, "row")
    weight = own * ranks / MODES
    outs = call(
        functools.partial(last_kernel, MODES * len(basis), len(parts), weight),
        [*parts, *known, *basis, *images, near, far, mass, parity],
        [(1, own), (1, own)],
        [],
        1 << 31,
    )
    return outs[0].reshape(own), outs[1].reshape(own)


def solution(mesh):
    placed = (
        P(("sub", "row"), None, None),
        P(("sub", "row"), None, None, None),
        P(("sub", "row"), None),
        P(("sub", "row")),
        P(None, ("sub", "row")),
    )
    return jax.shard_map(
        local,
        mesh=mesh,
        in_specs=placed,
        out_specs=(P(("sub", "row")), P(("sub", "row"))),
        check_vma=False,
    )
```

```python
import functools

import jax
import jax.numpy as jnp
from jax import lax
from jax.experimental import pallas as pl
from jax.experimental.pallas import tpu as pltpu
from jax.sharding import PartitionSpec as P

MODES = 32
REACH = 4
ITERS = 3
PURIFY = 28
LANES = 128
SETTLED = 1e-7
PANEL = 16
TOGETHER = (1, 2, 4, 8, 16)
F32 = jnp.float32
BF16 = jnp.bfloat16


def pieces(value, count):
    parts = []
    for index in range(count):
        part = value.astype(BF16)
        parts.append(part)
        if index + 1 < count:
            value = value - part.astype(F32)
    return parts


def dot_nn(left, right):
    return lax.dot_general(left, right, (((1,), (0,)), ((), ())), preferred_element_type=F32)


def dot_nt(left, right):
    return lax.dot_general(left, right, (((1,), (1,)), ((), ())), preferred_element_type=F32)


def pad_rows(value):
    short = LANES - value.shape[0]
    if short == 0:
        return value
    return jnp.concatenate([value, jnp.zeros((short, value.shape[1]), value.dtype)], axis=0)


def transposed(value):
    return pad_rows(value).T[: value.shape[0]]


def fold(out):
    rows, width = out.shape[0] // 2, out.shape[1] // 2
    out = out[:rows] + out[rows:]
    return out[:, :width] + out[:, width:]


def mul_nn(left, right):
    right = [pad_rows(part) for part in pieces(right, 2)]
    return fold(dot_nn(jnp.concatenate(pieces(left, 2), axis=0), jnp.concatenate(right, axis=1)))


def mul_nt(left, right):
    right = [pad_rows(part) for part in pieces(right, 2)]
    return fold(dot_nt(jnp.concatenate(pieces(left, 2), axis=0), jnp.concatenate(right, axis=0)))


def lane_of(shape):
    return lax.broadcasted_iota(jnp.int32, shape, 1)


def row_of(shape):
    return lax.broadcasted_iota(jnp.int32, shape, 0)


def eye_of(rows, lead=0):
    shape = (rows, LANES)
    return lane_of(shape) == row_of(shape) + lead


def eliminate(matrix, other, lead):
    order = matrix.shape[0]
    tiles = order // 8
    a = [matrix[8 * i : 8 * i + 8] for i in range(tiles)]
    e = [other[8 * i : 8 * i + 8] for i in range(tiles)]
    sub = row_of((8, LANES))
    for start in range(0, order, PANEL):
        columns = [
            {
                i: jnp.broadcast_to(a[i][:, lead + start + k : lead + start + k + 1], (8, LANES))
                for i in range(start // 8, tiles)
            }
            for k in range(PANEL)
        ]
        for step in range(PANEL):
            kt, k = (start + step) // 8, step % 8
            below = range(kt, tiles)
            head = lambda tile: jnp.broadcast_to(tile[k : k + 1, :], (8, LANES))
            pivot = head(columns[step][kt])
            inverse = 1.0 / pivot
            ratios = {i: columns[step][i] * inverse for i in below}
            ratios[kt] = jnp.where(sub > k, ratios[kt], 0.0)
            for later in range(step + 1, PANEL):
                top = head(columns[later][kt])
                for i in below:
                    columns[later][i] = columns[later][i] - ratios[i] * top
            row_a, row_e = head(a[kt]), head(e[kt])
            for i in below:
                a[i] = a[i] - ratios[i] * row_a
                e[i] = e[i] - ratios[i] * row_e
            e[kt] = jnp.where(sub == k, e[kt] * lax.rsqrt(pivot), e[kt])
    return jnp.concatenate(e, axis=0)


def total_of(value):
    return jnp.sum(jnp.sum(value, axis=0, keepdims=True), axis=1, keepdims=True)


def purify(matrix, wanted, steps):
    order = matrix.shape[0]
    eye = eye_of(order)
    valid = lane_of((1, LANES)) < order
    diagonal = jnp.sum(jnp.where(eye, matrix, 0.0), axis=0, keepdims=True)
    center = jnp.sum(diagonal, axis=1, keepdims=True) / order
    radius = jnp.sum(jnp.where(eye, 0.0, jnp.abs(matrix)), axis=0, keepdims=True)
    highest = jnp.max(jnp.where(valid, diagonal + radius, -jnp.inf), axis=1, keepdims=True)
    lowest = jnp.min(jnp.where(valid, diagonal - radius, jnp.inf), axis=1, keepdims=True)
    factor = jnp.minimum(
        wanted / jnp.maximum(highest - center, 1e-06),
        (order - wanted) / jnp.maximum(center - lowest, 1e-06),
    )
    ones = jnp.where(eye, 1.0, 0.0)
    initial = factor / order * (center * ones - matrix) + wanted / order * ones

    def purify_step(density):
        square = mul_nn(density, density)
        cube = mul_nn(square, density)
        gap = density - square
        below = total_of(jnp.where(eye, density, 0.0) - density * density)
        above = total_of(density * gap)
        change = total_of(gap * gap)
        safe = jnp.where(jnp.abs(below) > 1e-12, below, 1.0)
        ratio = jnp.clip(above / safe, 0.0, 1.0)
        high = ratio >= 0.5
        scale = 1.0 / jnp.where(high, jnp.maximum(ratio, 0.5), jnp.maximum(1.0 - ratio, 0.5))
        first = jnp.where(high, 0.0, 1.0 - 2.0 * ratio) * scale
        second = (1.0 + ratio) * scale
        return first * density + second * square - scale * cube, change

    def advance(carry):
        index, _, density = carry
        density, change = purify_step(density)
        return index + 1, change[0, 0], density

    def unsettled(carry):
        return (carry[0] < steps) & (carry[1] > SETTLED)

    return lax.while_loop(unsettled, advance, (0, jnp.float32(1.0), initial))[2]


def ritz(half_stiff, half_mass, wanted, steps, last):
    order = half_stiff.shape[0]
    eye = eye_of(order)
    gram_stiff = half_stiff + transposed(half_stiff)
    gram_mass = half_mass + transposed(half_mass)
    picked = jnp.where(eye, gram_mass, 0.0)
    scale_col = lax.rsqrt(jnp.sum(picked, axis=1, keepdims=True) + 1e-06)
    scale_row = lax.rsqrt(jnp.sum(picked, axis=0, keepdims=True) + 1e-06)
    stiff = scale_col * gram_stiff * scale_row
    mass = scale_col * gram_mass * scale_row
    ones = jnp.where(eye, 1.0, 0.0)
    if order == wanted:
        inverse_low = eliminate(mass, ones, 0)
    else:
        known = lane_of((1, LANES)) < wanted
        pivots = jnp.where(known, jnp.sum(jnp.where(eye, mass, 0.0), axis=0, keepdims=True), 1.0)
        ratio = jnp.where(known, mass[wanted:], 0.0) / pivots
        rest = jnp.where(known, 0.0, mass[wanted:] - mul_nn(ratio, mass[:wanted]))
        inverse_low = jnp.concatenate(
            [ones[:wanted] * lax.rsqrt(pivots), eliminate(rest, ones[wanted:] - ratio, wanted)], axis=0
        )
    reduced = mul_nt(mul_nn(inverse_low, stiff), inverse_low)
    if order == wanted:
        return inverse_low * scale_row, reduced, gram_stiff, gram_mass
    columns = purify(reduced, wanted, steps)[:wanted]
    columns = eliminate(mul_nt(columns, columns), columns, 0)
    coefficients = mul_nn(columns, inverse_low) * scale_row
    if last:
        return coefficients, None, gram_stiff, gram_mass
    projected = mul_nt(mul_nn(columns, reduced), columns)
    return coefficients, projected, gram_stiff, gram_mass


def halves_next(coefficients, projected, gram_stiff, gram_mass):
    order = gram_stiff.shape[0]
    wanted = coefficients.shape[0]
    lane = lane_of((wanted, LANES))
    first = lane < wanted
    stiff_top = jnp.where(first, 0.5 * projected, 0.0)
    mass_top = jnp.where(eye_of(wanted), 0.5, 0.0)
    blank = jnp.zeros((wanted, LANES), F32)
    if order == wanted:
        return jnp.concatenate([stiff_top, blank], axis=0), jnp.concatenate([mass_top, blank], axis=0)
    later = jnp.where(first, 0.0, coefficients)
    both = jnp.concatenate([mul_nn(later, gram_stiff), mul_nn(later, gram_mass)], axis=0)
    crossed = mul_nt(both, jnp.concatenate([coefficients, later], axis=0))
    moved = pltpu.roll(crossed, wanted, 1)
    lane = lane_of((2 * wanted, LANES))
    tail = jnp.where((lane >= 2 * wanted) & (lane < 3 * wanted), 0.5 * moved, 0.0)
    crossed = jnp.where(lane < wanted, crossed, tail)
    return (
        jnp.concatenate([stiff_top, blank, crossed[:wanted]], axis=0),
        jnp.concatenate([mass_top, blank, crossed[wanted:]], axis=0),
    )


def odd_lanes(rows):
    return (lane_of((rows, LANES)) // MODES) % 2 == 1


def pack_gram(gram):
    rows = gram.shape[0]
    gram = jnp.where(odd_lanes(rows), gram, 0.0)
    if rows <= 2 * MODES:
        return gram
    top = gram[:MODES] + pltpu.roll(gram[2 * MODES :], MODES, 1)
    return jnp.concatenate([top, gram[MODES : 2 * MODES]], axis=0)


def unpack_gram(packed, order):
    if order > 2 * MODES:
        packed = jnp.concatenate([packed, pltpu.roll(packed[:MODES], LANES - MODES, 1)], axis=0)
    return jnp.where(odd_lanes(order), packed, 0.0)


def halves_now(parts, known, order):
    total = parts[0][...]
    for part in parts[1:]:
        total = total + part[...]
    total = unpack_gram(total, order)
    if order == MODES:
        first = lane_of((MODES, LANES)) < MODES
        stiff = jnp.where(first, 0.5 * pltpu.roll(total, LANES - MODES, 1), 0.0)
        mass = jnp.where(first, 0.5 * pltpu.roll(total, MODES, 1), 0.0)
        return stiff, mass
    row = row_of((order, LANES))
    lane = lane_of((order, LANES))
    total = total * jnp.where((row >= MODES) & (row < 2 * MODES), 0.5, 1.0)
    inside = (lane >= MODES) & (lane < 2 * MODES)
    stiff = known[0][...] + jnp.where(inside, total, 0.0)
    mass = known[1][...] + jnp.where(inside, pltpu.roll(total, LANES // 2, 1), 0.0)
    return stiff, mass


def stiffness_apply(split_ref, out_ref, offsets_ref, first, last, pairs_of):
    width = split_ref.shape[1] // (offsets_ref.shape[0] + REACH)
    slots = offsets_ref.shape[1]

    def products(block):
        here = pl.ds(pl.multiple_of((block + REACH) * width, width), width)
        mine = split_ref[:, here]
        pairs = pairs_of(block)
        own = dot_nn(mine, jnp.concatenate(pairs[0], axis=1))
        spread = []
        for slot in range(slots):
            back = block + REACH - offsets_ref[block, slot]
            there = pl.ds(pl.multiple_of(back * width, width), width)
            across, down = pairs[2 * slot + 1], pairs[2 * slot + 2]
            own = own + dot_nn(split_ref[:, there], jnp.concatenate(down, axis=1))
            spread.append((there, fold(dot_nn(mine, jnp.concatenate(across, axis=1)))))
        return [(here, fold(own)), *spread]

    together = max(size for size in TOGETHER if (last - first) % size == 0)

    def group_step(group, carry):
        found = []
        for index in range(together):
            found += products(first + group * together + index)
        for at, product in found:
            out_ref[:, at] += product
        return carry

    lax.fori_loop(0, (last - first) // together, group_step, 0)


def loaded_pairs(pairs_ref):
    slots = pairs_ref.shape[1]
    return lambda block: [[pairs_ref[block, slot, 0], pairs_ref[block, slot, 1]] for slot in range(slots)]


def stacked(value, width):
    count = value.shape[1] // width
    return jnp.concatenate([value[:, width * i : width * (i + 1)] for i in range(count)], axis=0)


def unstacked(value, count):
    rows = value.shape[0] // count
    return jnp.concatenate([value[rows * i : rows * (i + 1)] for i in range(count)], axis=1)


def send_edges(gram, behind, ahead, even, gram_ref, near_ref, far_ref):
    behind, ahead = stacked(behind, LANES), stacked(ahead, LANES)
    rows = gram.shape[0]
    gram_ref[...] = gram
    near_ref[:rows, :] = gram
    near_ref[rows:, :] = jnp.where(even, ahead, behind)
    far_ref[...] = jnp.where(even, behind, ahead)


def received_edges(near_ref, far_ref, even):
    far = far_ref[...]
    near = near_ref[near_ref.shape[0] - far.shape[0] :, :]
    ahead, behind = jnp.where(even, far, near), jnp.where(even, near, far)
    return unstacked(ahead, REACH), unstacked(behind, REACH)


def split_store(split_ref, at, value):
    rows = value.shape[0]
    high, low = pieces(value, 2)
    split_ref[:rows, at] = high
    split_ref[rows:, at] = low


def gram_of(basis_refs, vectors_ref, stiff_ref, mass):
    halo = stiff_ref.shape[1] - mass.shape[1]
    weighted = jnp.concatenate(
        [jnp.zeros((MODES, halo), F32), vectors_ref[:, halo:] * mass], axis=1
    )
    stiff_high, stiff_low = pieces(stiff_ref[...], 2)
    mass_high, mass_low = pieces(weighted, 2)
    right = jnp.concatenate([stiff_low, stiff_high, mass_low, mass_high], axis=0)
    basis = [pieces(ref[...], 2) for ref in basis_refs]
    left = jnp.concatenate([pair[0] for pair in basis] + [pair[1] for pair in basis], axis=0)
    out = dot_nt(left, right)
    rows = left.shape[0] // 2
    out = out[:rows] + out[rows:]
    return pack_gram(out + pltpu.roll(out, MODES, 1))


def first_kernel(
    modes_hbm, diag_hbm, coupling_hbm, edge_ref, mass_ref, parity_ref, offsets_ref,
    basis_ref, stiff_ref, gram_ref, near_ref, far_ref, inverse_ref, pairs_ref,
    split_ref, modes_ref, diag_ref, coupling_ref, semaphores,
):
    halo = edge_ref.shape[1]
    count, width = diag_ref.shape[0], diag_ref.shape[1]
    groups = semaphores.shape[0] // 2
    size = count // groups
    copies = [pltpu.make_async_copy(modes_hbm, modes_ref, semaphores.at[2 * groups])]
    for group in range(groups):
        at = pl.ds(group * size, size)
        copies.append(pltpu.make_async_copy(diag_hbm.at[at], diag_ref.at[at], semaphores.at[2 * group]))
        copies.append(
            pltpu.make_async_copy(coupling_hbm.at[at], coupling_ref.at[at], semaphores.at[2 * group + 1])
        )
    for copy in copies:
        copy.start()
    diagonal = lax.broadcasted_iota(jnp.int32, (width, width), 0) == lax.broadcasted_iota(
        jnp.int32, (width, width), 1
    )

    def pairs_of(block):
        pairs = [pieces(jnp.where(diagonal, 0.0, diag_ref[block]), 2)]
        for slot in range(coupling_ref.shape[1]):
            pair = pieces(coupling_ref[block, slot], 2)
            pairs += [pair, [part.T for part in pair]]
        for index, pair in enumerate(pairs):
            pairs_ref[block, index, 0] = pair[0]
            pairs_ref[block, index, 1] = pair[1]
        return pairs

    copies[0].wait()
    basis_ref[:, :halo] = edge_ref[...]
    basis_ref[:, halo:] = modes_ref[...]
    split_store(split_ref, slice(None), basis_ref[...])
    stiff_ref[...] = jnp.zeros(stiff_ref.shape, F32)
    for group in range(groups):
        copies[2 * group + 1].wait()
        copies[2 * group + 2].wait()
        for block in range(group * size, (group + 1) * size):
            at = slice(block * width, (block + 1) * width)
            picked = jnp.sum(jnp.where(diagonal, diag_ref[block], 0.0), axis=0, keepdims=True)
            inverse_ref[:, at] = 1.0 / picked
            stiff_ref[:, halo + block * width : halo + (block + 1) * width] += modes_ref[:, at] * picked
        stiffness_apply(split_ref, stiff_ref, offsets_ref, group * size, (group + 1) * size, pairs_of)
    gram = gram_of([basis_ref], basis_ref, stiff_ref, mass_ref[...])
    extra = near_ref.shape[0] // REACH - MODES - gram.shape[0] // REACH
    start = inverse_ref.shape[1] - halo
    tail = jnp.where(
        row_of((extra, halo)) == 0,
        jnp.broadcast_to(inverse_ref[:, start:], (extra, halo)),
        jnp.broadcast_to(mass_ref[:, start:], (extra, halo)),
    )
    behind = jnp.concatenate([stiff_ref[:, :halo], tail], axis=0)
    ahead = jnp.concatenate([stiff_ref[:, stiff_ref.shape[1] - halo :], tail], axis=0)
    send_edges(gram, behind, ahead, parity_ref[0] == 0, gram_ref, near_ref, far_ref)


def doubled(left):
    return jnp.concatenate([jnp.concatenate([part, part], axis=1) for part in pieces(left, 2)], axis=0)


def combine(left, right):
    out = dot_nn(left, jnp.concatenate(pieces(right, 2), axis=0))
    rows = left.shape[0] // 2
    return out[:rows] + out[rows:]


def middle_kernel(order, parts_count, *refs):
    refs = list(refs)
    take = lambda count: [refs.pop(0) for _ in range(count)]
    parts = take(parts_count)
    known = take(2) if order > MODES else []
    blocks = order // MODES
    basis = take(blocks)
    stiff = take(blocks)
    near_in, far_in, mass_in, inverse_in, pairs_ref, parity_ref, offsets_ref = take(7)
    out_blocks = min(blocks + 1, 3)
    basis_out = take(out_blocks)
    stiff_out = take(out_blocks)
    gram_ref, near_ref, far_ref, half_stiff_ref, half_mass_ref = take(5)
    mass_ref, inverse_ref = take(2) if order == MODES else (mass_in, inverse_in)
    (split_ref,) = take(1)

    even = parity_ref[0] == 0
    coefficients, projected, gram_stiff, gram_mass = ritz(
        *halves_now(parts, known, order), MODES, PURIFY, False
    )
    halves = halves_next(coefficients, projected, gram_stiff, gram_mass)
    half_stiff_ref[...] = halves[0]
    half_mass_ref[...] = halves[1]
    ahead, behind = received_edges(near_in, far_in, even)
    halo = ahead.shape[1]
    extent = basis[0].shape[1]
    if order == MODES:
        inverse_ref[:, :halo] = ahead[MODES : MODES + 1]
        inverse_ref[:, halo:] = inverse_in[...]
        mass_ref[:, :halo] = ahead[MODES + 1 : MODES + 2]
        mass_ref[:, halo:] = mass_in[...]
    mixing = coefficients[:, :order]
    if order > MODES:
        later = jnp.where(lane_of((MODES, LANES)) < MODES, 0.0, coefficients)
        mixing = jnp.concatenate([mixing, later[:, :order]], axis=0)
    mixing = doubled(mixing)
    pulling = doubled(projected[:, :MODES])
    newest = 0 if order == MODES else 1
    current = [ref[...] for ref in stiff]
    completion = jnp.concatenate(
        [ahead[:MODES], jnp.zeros((MODES, extent - 2 * halo), F32), behind[:MODES]], axis=1
    )
    current[newest] = current[newest] + completion
    vectors = combine(mixing, jnp.concatenate([ref[...] for ref in basis], axis=0))
    images = combine(mixing, jnp.concatenate(current, axis=0))
    modes, stiff_modes = vectors[:MODES], images[:MODES]
    residual = stiff_modes - combine(pulling, modes * mass_ref[...])
    precond = residual * inverse_ref[...]
    split_store(split_ref, slice(None), precond)
    basis_out[0][...] = modes
    stiff_out[0][...] = stiff_modes
    if order > MODES:
        basis_out[2][...] = vectors[MODES:]
        stiff_out[2][...] = images[MODES:]
    basis_out[1][...] = precond
    stiff_out[1][:, :halo] = jnp.zeros((MODES, halo), F32)
    stiff_out[1][:, halo:] = residual[:, halo:]
    stiffness_apply(split_ref, stiff_out[1], offsets_ref, 0, offsets_ref.shape[0], loaded_pairs(pairs_ref))
    gram = gram_of(basis_out, basis_out[1], stiff_out[1], mass_ref[:, halo:])
    newest = stiff_out[1]
    send_edges(gram, newest[:, :halo], newest[:, extent - halo :], even, gram_ref, near_ref, far_ref)


def last_kernel(order, parts_count, weight, *refs):
    refs = list(refs)
    take = lambda count: [refs.pop(0) for _ in range(count)]
    parts = take(parts_count)
    known = take(2)
    blocks = order // MODES
    basis = take(blocks)
    stiff = take(blocks)
    near_in, far_in, mass_ref, parity_ref = take(4)
    mass_out, energy_out = take(2)
    coefficients = ritz(*halves_now(parts, known, order), MODES, PURIFY, True)[0]
    behind = received_edges(near_in, far_in, parity_ref[0] == 0)[1]
    halo = behind.shape[1]
    extent = mass_ref.shape[1]
    mixing = doubled(coefficients[:, :order])
    for start in range(halo, extent, halo):
        at = slice(start, start + halo)
        to = slice(start - halo, start)
        current = [ref[:, at] for ref in stiff]
        if start + halo == extent:
            current[1] = current[1] + behind
        vectors = combine(mixing, jnp.concatenate([ref[:, at] for ref in basis], axis=0))
        images = combine(mixing, jnp.concatenate(current, axis=0))
        mass_out[:, to] = weight * mass_ref[:, at] * jnp.sum(vectors * vectors, axis=0, keepdims=True)
        energy_out[:, to] = weight * jnp.sum(vectors * images, axis=0, keepdims=True)


def call(kernel, args, outs, scratch, flops, spaces=()):
    spaces = list(spaces) + [pltpu.VMEM] * (len(args) - len(spaces))
    spaces = [pltpu.SMEM if arg.dtype == jnp.int32 else space for arg, space in zip(args, spaces)]
    return pl.pallas_call(
        kernel,
        out_shape=[
            jax.ShapeDtypeStruct(shape, BF16 if len(shape) > 2 else F32) for shape in outs
        ],
        in_specs=[pl.BlockSpec(memory_space=space) for space in spaces],
        out_specs=[pl.BlockSpec(memory_space=pltpu.VMEM)] * len(outs),
        scratch_shapes=scratch,
        compiler_params=pltpu.CompilerParams(vmem_limit_bytes=24 << 20),
        cost_estimate=pl.CostEstimate(flops=flops, bytes_accessed=1 << 20, transcendentals=0),
    )(*args)


def hbm(value):
    return pltpu.with_memory_space_constraint(value, pltpu.HBM)


def exchange(gram, near, far, axis):
    count = lax.axis_size(axis)
    across = lambda value, mask: lax.ppermute(
        value, axis, [(at, at ^ mask) for at in range(count) if at ^ mask < count]
    )
    near = across(near, 1)
    if count & (count - 1):
        parts = [lax.psum(gram, axis)]
    else:
        parts, stride = [gram], 1
        while stride < count:
            if len(parts) > 1:
                gram = sum(parts[1:], parts[0])
            masks = ([stride, 3 * stride, 2 * stride] if stride == 1 else [stride, 2 * stride, 3 * stride]) if 4 * stride <= count else [stride]
            parts = [gram] + [
                near[: gram.shape[0]] if mask == 1 else across(gram, mask) for mask in masks
            ]
            stride *= 1 << len(masks).bit_length()
    hops = [(at, at + 1 if at % 2 else at - 1) for at in range(count)]
    far = lax.ppermute(far, axis, [hop for hop in hops if 0 <= hop[1] < count])
    return parts, near, far


def local(diag_blocks, coupling, offsets, mass, initial_modes):
    count, width = diag_blocks.shape[0], diag_blocks.shape[1]
    slots = coupling.shape[1]
    own = count * width
    halo = REACH * width
    extent = own + halo
    split = [pltpu.VMEM((2 * MODES, extent), BF16)]
    parity = (lax.axis_index("row") % 2).astype(jnp.int32).reshape(1)
    mass = mass.reshape(1, own)
    spare = 8
    ranks = lax.axis_size("row")
    edge = lax.ppermute(initial_modes[:, own - halo :], "row", [(at, at + 1) for at in range(ranks - 1)])
    edge_rows = REACH * (MODES + spare)
    groups = 4 if count % 4 == 0 else 1
    vectors, stiff, gram, near, far, inverse, pairs = call(
        first_kernel,
        [hbm(initial_modes), hbm(diag_blocks), hbm(coupling), edge, mass, parity, offsets],
        [
            (MODES, extent), (MODES, extent), (MODES, LANES), (MODES + edge_rows, LANES),
            (edge_rows, LANES), (1, own), (count, 2 * slots + 1, 2, width, width),
        ],
        split
        + [
            pltpu.VMEM((MODES, own), F32),
            pltpu.VMEM((count, width, width), F32),
            pltpu.VMEM((count, slots, width, width), F32),
            pltpu.SemaphoreType.DMA((2 * groups + 1,)),
        ],
        1 << 30,
        [pltpu.HBM] * 3,
    )
    edge_rows = REACH * MODES
    basis, images, known = [vectors], [stiff], []
    for iteration in range(ITERS):
        parts, near, far = exchange(gram, near, far, "row")
        order = MODES * len(basis)
        out_blocks = min(len(basis) + 1, 3)
        wide = [(MODES, extent)] * out_blocks
        packed = min(out_blocks, 2) * MODES
        halves = [(out_blocks * MODES, LANES)] * 2
        outs = call(
            functools.partial(middle_kernel, order, len(parts)),
            [*parts, *known, *basis, *images, near, far, mass, inverse, pairs, parity, offsets],
            [
                *wide, *wide, (packed, LANES), (packed + edge_rows, LANES), (edge_rows, LANES), *halves,
                *([(1, extent)] * 2 if order == MODES else []),
            ],
            split,
            1 << 31,
        )
        basis = outs[:out_blocks]
        images = outs[out_blocks : 2 * out_blocks]
        gram, near, far = outs[2 * out_blocks : 2 * out_blocks + 3]
        known = outs[2 * out_blocks + 3 : 2 * out_blocks + 5]
        if order == MODES:
            mass, inverse = outs[-2:]
    parts, near, far = exchange(gram, near, far, "row")
    weight = own * ranks / MODES
    outs = call(
        functools.partial(last_kernel, MODES * len(basis), len(parts), weight),
        [*parts, *known, *basis, *images, near, far, mass, parity],
        [(1, own), (1, own)],
        [],
        1 << 31,
    )
    return outs[0].reshape(own), outs[1].reshape(own)


def solution(mesh):
    placed = (
        P(("sub", "row"), None, None),
        P(("sub", "row"), None, None, None),
        P(("sub", "row"), None),
        P(("sub", "row")),
        P(None, ("sub", "row")),
    )
    return jax.shard_map(
        local,
        mesh=mesh,
        in_specs=placed,
        out_specs=(P(("sub", "row")), P(("sub", "row"))),
        check_vma=False,
    )
```

```python
import functools

import jax
import jax.numpy as jnp
from jax import lax
from jax.experimental import pallas as pl
from jax.experimental.pallas import tpu as pltpu
from jax.sharding import PartitionSpec as P

MODES = 32
REACH = 4
ITERS = 3
PURIFY = 28
LANES = 128
SETTLED = 1e-7
PANEL = 16
TOGETHER = (1, 2, 4, 8, 16)
F32 = jnp.float32
BF16 = jnp.bfloat16


def pieces(value, count):
    parts = []
    for index in range(count):
        part = value.astype(BF16)
        parts.append(part)
        if index + 1 < count:
            value = value - part.astype(F32)
    return parts


def dot_nn(left, right):
    return lax.dot_general(left, right, (((1,), (0,)), ((), ())), preferred_element_type=F32)


def dot_nt(left, right):
    return lax.dot_general(left, right, (((1,), (1,)), ((), ())), preferred_element_type=F32)


def pad_rows(value):
    short = LANES - value.shape[0]
    if short == 0:
        return value
    return jnp.concatenate([value, jnp.zeros((short, value.shape[1]), value.dtype)], axis=0)


def transposed(value):
    return pad_rows(value).T[: value.shape[0]]


def fold(out):
    rows, width = out.shape[0] // 2, out.shape[1] // 2
    out = out[:rows] + out[rows:]
    return out[:, :width] + out[:, width:]


def mul_nn(left, right):
    right = [pad_rows(part) for part in pieces(right, 2)]
    return fold(dot_nn(jnp.concatenate(pieces(left, 2), axis=0), jnp.concatenate(right, axis=1)))


def mul_nt(left, right):
    right = [pad_rows(part) for part in pieces(right, 2)]
    return fold(dot_nt(jnp.concatenate(pieces(left, 2), axis=0), jnp.concatenate(right, axis=0)))


def lane_of(shape):
    return lax.broadcasted_iota(jnp.int32, shape, 1)


def row_of(shape):
    return lax.broadcasted_iota(jnp.int32, shape, 0)


def eye_of(rows, lead=0):
    shape = (rows, LANES)
    return lane_of(shape) == row_of(shape) + lead


def eliminate(matrix, other, lead):
    order = matrix.shape[0]
    tiles = order // 8
    a = [matrix[8 * i : 8 * i + 8] for i in range(tiles)]
    e = [other[8 * i : 8 * i + 8] for i in range(tiles)]
    sub = row_of((8, LANES))
    for start in range(0, order, PANEL):
        columns = [
            {
                i: jnp.broadcast_to(a[i][:, lead + start + k : lead + start + k + 1], (8, LANES))
                for i in range(start // 8, tiles)
            }
            for k in range(PANEL)
        ]
        for step in range(PANEL):
            kt, k = (start + step) // 8, step % 8
            below = range(kt, tiles)
            head = lambda tile: jnp.broadcast_to(tile[k : k + 1, :], (8, LANES))
            pivot = head(columns[step][kt])
            inverse = 1.0 / pivot
            ratios = {i: columns[step][i] * inverse for i in below}
            ratios[kt] = jnp.where(sub > k, ratios[kt], 0.0)
            for later in range(step + 1, PANEL):
                top = head(columns[later][kt])
                for i in below:
                    columns[later][i] = columns[later][i] - ratios[i] * top
            row_a, row_e = head(a[kt]), head(e[kt])
            for i in below:
                a[i] = a[i] - ratios[i] * row_a
                e[i] = e[i] - ratios[i] * row_e
            e[kt] = jnp.where(sub == k, e[kt] * lax.rsqrt(pivot), e[kt])
    return jnp.concatenate(e, axis=0)


def total_of(value):
    return jnp.sum(jnp.sum(value, axis=0, keepdims=True), axis=1, keepdims=True)


def purify(matrix, wanted, steps):
    order = matrix.shape[0]
    eye = eye_of(order)
    valid = lane_of((1, LANES)) < order
    diagonal = jnp.sum(jnp.where(eye, matrix, 0.0), axis=0, keepdims=True)
    center = jnp.sum(diagonal, axis=1, keepdims=True) / order
    radius = jnp.sum(jnp.where(eye, 0.0, jnp.abs(matrix)), axis=0, keepdims=True)
    highest = jnp.max(jnp.where(valid, diagonal + radius, -jnp.inf), axis=1, keepdims=True)
    lowest = jnp.min(jnp.where(valid, diagonal - radius, jnp.inf), axis=1, keepdims=True)
    factor = jnp.minimum(
        wanted / jnp.maximum(highest - center, 1e-06),
        (order - wanted) / jnp.maximum(center - lowest, 1e-06),
    )
    ones = jnp.where(eye, 1.0, 0.0)
    initial = factor / order * (center * ones - matrix) + wanted / order * ones

    def purify_step(density):
        square = mul_nn(density, density)
        cube = mul_nn(square, density)
        gap = density - square
        below = total_of(jnp.where(eye, density, 0.0) - density * density)
        above = total_of(density * gap)
        change = total_of(gap * gap)
        safe = jnp.where(jnp.abs(below) > 1e-12, below, 1.0)
        ratio = jnp.clip(above / safe, 0.0, 1.0)
        high = ratio >= 0.5
        scale = 1.0 / jnp.where(high, jnp.maximum(ratio, 0.5), jnp.maximum(1.0 - ratio, 0.5))
        first = jnp.where(high, 0.0, 1.0 - 2.0 * ratio) * scale
        second = (1.0 + ratio) * scale
        return first * density + second * square - scale * cube, change

    def advance(carry):
        index, _, density = carry
        density, change = purify_step(density)
        return index + 1, change[0, 0], density

    def unsettled(carry):
        return (carry[0] < steps) & (carry[1] > SETTLED)

    return lax.while_loop(unsettled, advance, (0, jnp.float32(1.0), initial))[2]


def ritz(half_stiff, half_mass, wanted, steps, last):
    order = half_stiff.shape[0]
    eye = eye_of(order)
    gram_stiff = half_stiff + transposed(half_stiff)
    gram_mass = half_mass + transposed(half_mass)
    picked = jnp.where(eye, gram_mass, 0.0)
    scale_col = lax.rsqrt(jnp.sum(picked, axis=1, keepdims=True) + 1e-06)
    scale_row = lax.rsqrt(jnp.sum(picked, axis=0, keepdims=True) + 1e-06)
    stiff = scale_col * gram_stiff * scale_row
    mass = scale_col * gram_mass * scale_row
    ones = jnp.where(eye, 1.0, 0.0)
    if order == wanted:
        inverse_low = eliminate(mass, ones, 0)
    else:
        known = lane_of((1, LANES)) < wanted
        pivots = jnp.where(known, jnp.sum(jnp.where(eye, mass, 0.0), axis=0, keepdims=True), 1.0)
        ratio = jnp.where(known, mass[wanted:], 0.0) / pivots
        rest = jnp.where(known, 0.0, mass[wanted:] - mul_nn(ratio, mass[:wanted]))
        inverse_low = jnp.concatenate(
            [ones[:wanted] * lax.rsqrt(pivots), eliminate(rest, ones[wanted:] - ratio, wanted)], axis=0
        )
    reduced = mul_nt(mul_nn(inverse_low, stiff), inverse_low)
    if order == wanted:
        return inverse_low * scale_row, reduced, gram_stiff, gram_mass
    columns = purify(reduced, wanted, steps)[:wanted]
    columns = eliminate(mul_nt(columns, columns), columns, 0)
    coefficients = mul_nn(columns, inverse_low) * scale_row
    if last:
        return coefficients, None, gram_stiff, gram_mass
    projected = mul_nt(mul_nn(columns, reduced), columns)
    return coefficients, projected, gram_stiff, gram_mass


def halves_next(coefficients, projected, gram_stiff, gram_mass):
    order = gram_stiff.shape[0]
    wanted = coefficients.shape[0]
    lane = lane_of((wanted, LANES))
    first = lane < wanted
    stiff_top = jnp.where(first, 0.5 * projected, 0.0)
    mass_top = jnp.where(eye_of(wanted), 0.5, 0.0)
    blank = jnp.zeros((wanted, LANES), F32)
    if order == wanted:
        return jnp.concatenate([stiff_top, blank], axis=0), jnp.concatenate([mass_top, blank], axis=0)
    later = jnp.where(first, 0.0, coefficients)
    both = jnp.concatenate([mul_nn(later, gram_stiff), mul_nn(later, gram_mass)], axis=0)
    crossed = mul_nt(both, jnp.concatenate([coefficients, later], axis=0))
    moved = pltpu.roll(crossed, wanted, 1)
    lane = lane_of((2 * wanted, LANES))
    tail = jnp.where((lane >= 2 * wanted) & (lane < 3 * wanted), 0.5 * moved, 0.0)
    crossed = jnp.where(lane < wanted, crossed, tail)
    return (
        jnp.concatenate([stiff_top, blank, crossed[:wanted]], axis=0),
        jnp.concatenate([mass_top, blank, crossed[wanted:]], axis=0),
    )


def odd_lanes(rows):
    return (lane_of((rows, LANES)) // MODES) % 2 == 1


def pack_gram(gram):
    rows = gram.shape[0]
    gram = jnp.where(odd_lanes(rows), gram, 0.0)
    if rows <= 2 * MODES:
        return gram
    top = gram[:MODES] + pltpu.roll(gram[2 * MODES :], MODES, 1)
    return jnp.concatenate([top, gram[MODES : 2 * MODES]], axis=0)


def unpack_gram(packed, order):
    if order > 2 * MODES:
        packed = jnp.concatenate([packed, pltpu.roll(packed[:MODES], LANES - MODES, 1)], axis=0)
    return jnp.where(odd_lanes(order), packed, 0.0)


def halves_now(parts, known, order):
    total = parts[0][...]
    for part in parts[1:]:
        total = total + part[...]
    total = unpack_gram(total, order)
    if order == MODES:
        first = lane_of((MODES, LANES)) < MODES
        stiff = jnp.where(first, 0.5 * pltpu.roll(total, LANES - MODES, 1), 0.0)
        mass = jnp.where(first, 0.5 * pltpu.roll(total, MODES, 1), 0.0)
        return stiff, mass
    row = row_of((order, LANES))
    lane = lane_of((order, LANES))
    total = total * jnp.where((row >= MODES) & (row < 2 * MODES), 0.5, 1.0)
    inside = (lane >= MODES) & (lane < 2 * MODES)
    stiff = known[0][...] + jnp.where(inside, total, 0.0)
    mass = known[1][...] + jnp.where(inside, pltpu.roll(total, LANES // 2, 1), 0.0)
    return stiff, mass


def stiffness_apply(split_ref, out_ref, offsets_ref, first, last, pairs_of):
    width = split_ref.shape[1] // (offsets_ref.shape[0] + REACH)
    slots = offsets_ref.shape[1]

    def products(block):
        here = pl.ds(pl.multiple_of((block + REACH) * width, width), width)
        mine = split_ref[:, here]
        pairs = pairs_of(block)
        own = dot_nn(mine, jnp.concatenate(pairs[0], axis=1))
        spread = []
        for slot in range(slots):
            back = block + REACH - offsets_ref[block, slot]
            there = pl.ds(pl.multiple_of(back * width, width), width)
            across, down = pairs[2 * slot + 1], pairs[2 * slot + 2]
            own = own + dot_nn(split_ref[:, there], jnp.concatenate(down, axis=1))
            spread.append((there, fold(dot_nn(mine, jnp.concatenate(across, axis=1)))))
        return [(here, fold(own)), *spread]

    together = max(size for size in TOGETHER if (last - first) % size == 0)

    def group_step(group, carry):
        found = []
        for index in range(together):
            found += products(first + group * together + index)
        for at, product in found:
            out_ref[:, at] += product
        return carry

    lax.fori_loop(0, (last - first) // together, group_step, 0)


def loaded_pairs(pairs_ref):
    slots = pairs_ref.shape[1]
    return lambda block: [[pairs_ref[block, slot, 0], pairs_ref[block, slot, 1]] for slot in range(slots)]


def stacked(value, width):
    count = value.shape[1] // width
    return jnp.concatenate([value[:, width * i : width * (i + 1)] for i in range(count)], axis=0)


def unstacked(value, count):
    rows = value.shape[0] // count
    return jnp.concatenate([value[rows * i : rows * (i + 1)] for i in range(count)], axis=1)


def send_edges(gram, behind, ahead, even, gram_ref, near_ref, far_ref):
    behind, ahead = stacked(behind, LANES), stacked(ahead, LANES)
    rows = gram.shape[0]
    gram_ref[...] = gram
    near_ref[:rows, :] = gram
    near_ref[rows:, :] = jnp.where(even, ahead, behind)
    far_ref[...] = jnp.where(even, behind, ahead)


def received_edges(near_ref, far_ref, even):
    far = far_ref[...]
    near = near_ref[near_ref.shape[0] - far.shape[0] :, :]
    ahead, behind = jnp.where(even, far, near), jnp.where(even, near, far)
    return unstacked(ahead, REACH), unstacked(behind, REACH)


def split_store(split_ref, at, value):
    rows = value.shape[0]
    high, low = pieces(value, 2)
    split_ref[:rows, at] = high
    split_ref[rows:, at] = low


def gram_of(basis_refs, vectors_ref, stiff_ref, mass):
    halo = stiff_ref.shape[1] - mass.shape[1]
    weighted = jnp.concatenate(
        [jnp.zeros((MODES, halo), F32), vectors_ref[:, halo:] * mass], axis=1
    )
    stiff_high, stiff_low = pieces(stiff_ref[...], 2)
    mass_high, mass_low = pieces(weighted, 2)
    right = jnp.concatenate([stiff_low, stiff_high, mass_low, mass_high], axis=0)
    basis = [pieces(ref[...], 2) for ref in basis_refs]
    left = jnp.concatenate([pair[0] for pair in basis] + [pair[1] for pair in basis], axis=0)
    out = dot_nt(left, right)
    rows = left.shape[0] // 2
    out = out[:rows] + out[rows:]
    return pack_gram(out + pltpu.roll(out, MODES, 1))


def first_kernel(
    modes_hbm, diag_hbm, coupling_hbm, edge_ref, mass_ref, parity_ref, offsets_ref,
    basis_ref, stiff_ref, gram_ref, near_ref, far_ref, inverse_ref, pairs_ref,
    split_ref, modes_ref, diag_ref, coupling_ref, semaphores,
):
    halo = edge_ref.shape[1]
    count, width = diag_ref.shape[0], diag_ref.shape[1]
    groups = semaphores.shape[0] // 2
    size = count // groups
    copies = [pltpu.make_async_copy(modes_hbm, modes_ref, semaphores.at[2 * groups])]
    for group in range(groups):
        at = pl.ds(group * size, size)
        copies.append(pltpu.make_async_copy(diag_hbm.at[at], diag_ref.at[at], semaphores.at[2 * group]))
        copies.append(
            pltpu.make_async_copy(coupling_hbm.at[at], coupling_ref.at[at], semaphores.at[2 * group + 1])
        )
    for copy in copies:
        copy.start()
    diagonal = lax.broadcasted_iota(jnp.int32, (width, width), 0) == lax.broadcasted_iota(
        jnp.int32, (width, width), 1
    )

    def pairs_of(block):
        pairs = [pieces(jnp.where(diagonal, 0.0, diag_ref[block]), 2)]
        for slot in range(coupling_ref.shape[1]):
            pair = pieces(coupling_ref[block, slot], 2)
            pairs += [pair, [part.T for part in pair]]
        for index, pair in enumerate(pairs):
            pairs_ref[block, index, 0] = pair[0]
            pairs_ref[block, index, 1] = pair[1]
        return pairs

    copies[0].wait()
    basis_ref[:, :halo] = edge_ref[...]
    basis_ref[:, halo:] = modes_ref[...]
    split_store(split_ref, slice(None), basis_ref[...])
    stiff_ref[...] = jnp.zeros(stiff_ref.shape, F32)
    for group in range(groups):
        copies[2 * group + 1].wait()
        copies[2 * group + 2].wait()
        for block in range(group * size, (group + 1) * size):
            at = slice(block * width, (block + 1) * width)
            picked = jnp.sum(jnp.where(diagonal, diag_ref[block], 0.0), axis=0, keepdims=True)
            inverse_ref[:, at] = 1.0 / picked
            stiff_ref[:, halo + block * width : halo + (block + 1) * width] += modes_ref[:, at] * picked
        stiffness_apply(split_ref, stiff_ref, offsets_ref, group * size, (group + 1) * size, pairs_of)
    gram = gram_of([basis_ref], basis_ref, stiff_ref, mass_ref[...])
    extra = near_ref.shape[0] // REACH - MODES - gram.shape[0] // REACH
    start = inverse_ref.shape[1] - halo
    tail = jnp.where(
        row_of((extra, halo)) == 0,
        jnp.broadcast_to(inverse_ref[:, start:], (extra, halo)),
        jnp.broadcast_to(mass_ref[:, start:], (extra, halo)),
    )
    behind = jnp.concatenate([stiff_ref[:, :halo], tail], axis=0)
    ahead = jnp.concatenate([stiff_ref[:, stiff_ref.shape[1] - halo :], tail], axis=0)
    send_edges(gram, behind, ahead, parity_ref[0] == 0, gram_ref, near_ref, far_ref)


def doubled(left):
    return jnp.concatenate([jnp.concatenate([part, part], axis=1) for part in pieces(left, 2)], axis=0)


def combine(left, right):
    out = dot_nn(left, jnp.concatenate(pieces(right, 2), axis=0))
    rows = left.shape[0] // 2
    return out[:rows] + out[rows:]


def middle_kernel(order, parts_count, *refs):
    refs = list(refs)
    take = lambda count: [refs.pop(0) for _ in range(count)]
    parts = take(parts_count)
    known = take(2) if order > MODES else []
    blocks = order // MODES
    basis = take(blocks)
    stiff = take(blocks)
    near_in, far_in, mass_in, inverse_in, pairs_ref, parity_ref, offsets_ref = take(7)
    out_blocks = min(blocks + 1, 3)
    basis_out = take(out_blocks)
    stiff_out = take(out_blocks)
    gram_ref, near_ref, far_ref, half_stiff_ref, half_mass_ref = take(5)
    mass_ref, inverse_ref = take(2) if order == MODES else (mass_in, inverse_in)
    (split_ref,) = take(1)

    even = parity_ref[0] == 0
    coefficients, projected, gram_stiff, gram_mass = ritz(
        *halves_now(parts, known, order), MODES, PURIFY, False
    )
    halves = halves_next(coefficients, projected, gram_stiff, gram_mass)
    half_stiff_ref[...] = halves[0]
    half_mass_ref[...] = halves[1]
    ahead, behind = received_edges(near_in, far_in, even)
    halo = ahead.shape[1]
    extent = basis[0].shape[1]
    if order == MODES:
        inverse_ref[:, :halo] = ahead[MODES : MODES + 1]
        inverse_ref[:, halo:] = inverse_in[...]
        mass_ref[:, :halo] = ahead[MODES + 1 : MODES + 2]
        mass_ref[:, halo:] = mass_in[...]
    mixing = coefficients[:, :order]
    if order > MODES:
        later = jnp.where(lane_of((MODES, LANES)) < MODES, 0.0, coefficients)
        mixing = jnp.concatenate([mixing, later[:, :order]], axis=0)
    mixing = doubled(mixing)
    pulling = doubled(projected[:, :MODES])
    newest = 0 if order == MODES else 1
    current = [ref[...] for ref in stiff]
    completion = jnp.concatenate(
        [ahead[:MODES], jnp.zeros((MODES, extent - 2 * halo), F32), behind[:MODES]], axis=1
    )
    current[newest] = current[newest] + completion
    vectors = combine(mixing, jnp.concatenate([ref[...] for ref in basis], axis=0))
    images = combine(mixing, jnp.concatenate(current, axis=0))
    modes, stiff_modes = vectors[:MODES], images[:MODES]
    residual = stiff_modes - combine(pulling, modes * mass_ref[...])
    precond = residual * inverse_ref[...]
    split_store(split_ref, slice(None), precond)
    basis_out[0][...] = modes
    stiff_out[0][...] = stiff_modes
    if order > MODES:
        basis_out[2][...] = vectors[MODES:]
        stiff_out[2][...] = images[MODES:]
    basis_out[1][...] = precond
    stiff_out[1][:, :halo] = jnp.zeros((MODES, halo), F32)
    stiff_out[1][:, halo:] = residual[:, halo:]
    stiffness_apply(split_ref, stiff_out[1], offsets_ref, 0, offsets_ref.shape[0], loaded_pairs(pairs_ref))
    gram = gram_of(basis_out, basis_out[1], stiff_out[1], mass_ref[:, halo:])
    newest = stiff_out[1]
    send_edges(gram, newest[:, :halo], newest[:, extent - halo :], even, gram_ref, near_ref, far_ref)


def last_kernel(order, parts_count, weight, *refs):
    refs = list(refs)
    take = lambda count: [refs.pop(0) for _ in range(count)]
    parts = take(parts_count)
    known = take(2)
    blocks = order // MODES
    basis = take(blocks)
    stiff = take(blocks)
    near_in, far_in, mass_ref, parity_ref = take(4)
    mass_out, energy_out = take(2)
    coefficients = ritz(*halves_now(parts, known, order), MODES, PURIFY, True)[0]
    behind = received_edges(near_in, far_in, parity_ref[0] == 0)[1]
    halo = behind.shape[1]
    extent = mass_ref.shape[1]
    mixing = doubled(coefficients[:, :order])
    for start in range(halo, extent, halo):
        at = slice(start, start + halo)
        to = slice(start - halo, start)
        current = [ref[:, at] for ref in stiff]
        if start + halo == extent:
            current[1] = current[1] + behind
        vectors = combine(mixing, jnp.concatenate([ref[:, at] for ref in basis], axis=0))
        images = combine(mixing, jnp.concatenate(current, axis=0))
        mass_out[:, to] = weight * mass_ref[:, at] * jnp.sum(vectors * vectors, axis=0, keepdims=True)
        energy_out[:, to] = weight * jnp.sum(vectors * images, axis=0, keepdims=True)


def call(kernel, args, outs, scratch, flops, spaces=()):
    spaces = list(spaces) + [pltpu.VMEM] * (len(args) - len(spaces))
    spaces = [pltpu.SMEM if arg.dtype == jnp.int32 else space for arg, space in zip(args, spaces)]
    return pl.pallas_call(
        kernel,
        out_shape=[
            jax.ShapeDtypeStruct(shape, BF16 if len(shape) > 2 else F32) for shape in outs
        ],
        in_specs=[pl.BlockSpec(memory_space=space) for space in spaces],
        out_specs=[pl.BlockSpec(memory_space=pltpu.VMEM)] * len(outs),
        scratch_shapes=scratch,
        compiler_params=pltpu.CompilerParams(vmem_limit_bytes=24 << 20),
        cost_estimate=pl.CostEstimate(flops=flops, bytes_accessed=1 << 20, transcendentals=0),
    )(*args)


def hbm(value):
    return pltpu.with_memory_space_constraint(value, pltpu.HBM)


def exchange(gram, near, far, axis, senders=2):
    count = lax.axis_size(axis)
    across = lambda value, mask: lax.ppermute(
        value, axis, [(at, at ^ mask) for at in range(count) if at ^ mask < count]
    )
    near = across(near, 1)
    if count & (count - 1):
        parts = [lax.psum(gram, axis)]
    else:
        parts, stride = [gram], 1
        while stride < count:
            if len(parts) > 1:
                gram = sum(parts[1:], parts[0])
            masks = ([stride, 3 * stride, 2 * stride] if stride == 1 else [stride, 2 * stride, 3 * stride]) if 4 * stride <= count else [stride]
            parts = [gram] + [
                near[: gram.shape[0]] if mask == 1 else across(gram, mask) for mask in masks
            ]
            stride *= 1 << len(masks).bit_length()
    hops = [(at, at + 1 if at % 2 else at - 1) for at in range(count) if at % 2 < senders]
    far = lax.ppermute(far, axis, [hop for hop in hops if 0 <= hop[1] < count])
    return parts, near, far


def local(diag_blocks, coupling, offsets, mass, initial_modes):
    count, width = diag_blocks.shape[0], diag_blocks.shape[1]
    slots = coupling.shape[1]
    own = count * width
    halo = REACH * width
    extent = own + halo
    split = [pltpu.VMEM((2 * MODES, extent), BF16)]
    parity = (lax.axis_index("row") % 2).astype(jnp.int32).reshape(1)
    mass = mass.reshape(1, own)
    spare = 8
    ranks = lax.axis_size("row")
    edge = lax.ppermute(initial_modes[:, own - halo :], "row", [(at, at + 1) for at in range(ranks - 1)])
    edge_rows = REACH * (MODES + spare)
    groups = 4 if count % 4 == 0 else 1
    vectors, stiff, gram, near, far, inverse, pairs = call(
        first_kernel,
        [hbm(initial_modes), hbm(diag_blocks), hbm(coupling), edge, mass, parity, offsets],
        [
            (MODES, extent), (MODES, extent), (MODES, LANES), (MODES + edge_rows, LANES),
            (edge_rows, LANES), (1, own), (count, 2 * slots + 1, 2, width, width),
        ],
        split
        + [
            pltpu.VMEM((MODES, own), F32),
            pltpu.VMEM((count, width, width), F32),
            pltpu.VMEM((count, slots, width, width), F32),
            pltpu.SemaphoreType.DMA((2 * groups + 1,)),
        ],
        1 << 30,
        [pltpu.HBM] * 3,
    )
    edge_rows = REACH * MODES
    basis, images, known = [vectors], [stiff], []
    for iteration in range(ITERS):
        parts, near, far = exchange(gram, near, far, "row")
        order = MODES * len(basis)
        out_blocks = min(len(basis) + 1, 3)
        wide = [(MODES, extent)] * out_blocks
        packed = min(out_blocks, 2) * MODES
        halves = [(out_blocks * MODES, LANES)] * 2
        outs = call(
            functools.partial(middle_kernel, order, len(parts)),
            [*parts, *known, *basis, *images, near, far, mass, inverse, pairs, parity, offsets],
            [
                *wide, *wide, (packed, LANES), (packed + edge_rows, LANES), (edge_rows, LANES), *halves,
                *([(1, extent)] * 2 if order == MODES else []),
            ],
            split,
            1 << 31,
        )
        basis = outs[:out_blocks]
        images = outs[out_blocks : 2 * out_blocks]
        gram, near, far = outs[2 * out_blocks : 2 * out_blocks + 3]
        known = outs[2 * out_blocks + 3 : 2 * out_blocks + 5]
        if order == MODES:
            mass, inverse = outs[-2:]
    parts, near, far = exchange(gram, near, far, "row", 1)
    weight = own * ranks / MODES
    outs = call(
        functools.partial(last_kernel, MODES * len(basis), len(parts), weight),
        [*parts, *known, *basis, *images, near, far, mass, parity],
        [(1, own), (1, own)],
        [],
        1 << 31,
    )
    return outs[0].reshape(own), outs[1].reshape(own)


def solution(mesh):
    placed = (
        P(("sub", "row"), None, None),
        P(("sub", "row"), None, None, None),
        P(("sub", "row"), None),
        P(("sub", "row")),
        P(None, ("sub", "row")),
    )
    return jax.shard_map(
        local,
        mesh=mesh,
        in_specs=placed,
        out_specs=(P(("sub", "row")), P(("sub", "row"))),
        check_vma=False,
    )
```
